32 devices in a mesh: ctx: 4 (over z), fsdp: 8 (over y, x, core).
Axes of the slice: x: 2, y: 2, z: 4, core: 2. Of those that a mesh axis runs over, the one named last changes fastest.
Arguments:
- tokens_in: bfloat16 [8, 4096, 768], P('fsdp', 'ctx'), may hold values from -6 to 6
- out_grad: bfloat16 [8, 4096, 768], P('fsdp', 'ctx'), may hold values from -6 to 6
- gain_attn: bfloat16 [768], P('fsdp'), may hold values from 0.5 to 1.5
- gain_mlp: bfloat16 [768], P('fsdp'), may hold values from 0.5 to 1.5
- w_qkv: bfloat16 [768, 2304], P('fsdp'), may hold values from -0.21875 to 0.21875
- w_out: bfloat16 [768, 768], P('fsdp'), may hold values from -6 to 6
- w_up: bfloat16 [768, 3072], P('fsdp'), may hold values from -0.21875 to 0.21875
- w_down: bfloat16 [3072, 768], P('fsdp'), may hold values from -0.109375 to 0.109375
- lengths: int32 [8], P('fsdp'), may hold values from 1024 to 4096, as said below
- block_order: int32 [8, 8], P('fsdp'), may hold values from 0 to 7, as said below
Outputs:
- result: bfloat16 [8, 4096, 768], P('fsdp', 'ctx')
- grad_tokens: bfloat16 [8, 4096, 768], P('fsdp', 'ctx')
- grad_gain_attn: float32 [768], P('fsdp')
- grad_gain_mlp: float32 [768], P('fsdp')
- grad_w_qkv: float32 [768, 2304], P('fsdp')
- grad_w_out: float32 [768, 768], P('fsdp')
- grad_w_up: float32 [768, 3072], P('fsdp')
- grad_w_down: float32 [3072, 768], P('fsdp')
The draws below stay inside these ranges and needn't reach their ends.
Inputs may be any that keep to these rules, and one draw needn't show every extreme that they name: `lengths`: some sequence has exactly 4096 valid tokens and some exactly 1024. `block_order`: each row holds every block number once; stored blocks 2 c and 2 c + 1 of a row are block numbers p and 7 - p in some order, for some p.
All inputs are finite; a program needn't handle non-finite values.
Results may differ from the reference program's by a relative error of at most 0.015.
The reference program's roundings to bfloat16 on the way count: a program that leaves them out, or rounds other values in their place, can miss the bound.
Values may be sent and summed in bfloat16 or wider, within the bound.
A program may use at most 256 MiB of HBM per device.

```python
import jax
import jax.numpy as jnp
from jax import lax

D = 768
HEADS = 12
HEAD_DIM = 64
FF = 3072
BLK = 512
MIN_LEN = 1024
BLOCKS = 8
SLOTS = 4096
SEQS = 8


def draw_lengths(key, part):
    key_values = jax.random.fold_in(key, 11)
    key_long = jax.random.fold_in(key, 12)
    key_short = jax.random.fold_in(key, 13)
    values_drawn = jax.random.randint(key_values, (SEQS,), MIN_LEN, SLOTS + 1)
    longest = jax.random.randint(key_long, (), 0, SEQS)
    shortest = (longest + 1 + jax.random.randint(key_short, (), 0, SEQS - 1)) % SEQS
    indices = jnp.arange(SEQS)
    values_drawn = jnp.where(indices == longest, SLOTS, values_drawn)
    values_drawn = jnp.where(indices == shortest, MIN_LEN, values_drawn)
    return values_drawn.astype(jnp.int32)


def draw_block_order(key, part):
    halfway_count = BLOCKS // 2
    row_keys = jax.random.split(jax.random.fold_in(key, 21), SEQS)
    pair_ids = jax.vmap(lambda row_key: jax.random.permutation(row_key, halfway_count))(row_keys)
    flips = jax.random.randint(jax.random.fold_in(key, 22), (SEQS, halfway_count), 0, 2)
    first = jnp.where(flips == 1, BLOCKS - 1 - pair_ids, pair_ids)
    second = BLOCKS - 1 - first
    return jnp.stack([first, second], axis=-1).reshape(SEQS, BLOCKS).astype(jnp.int32)


def steps_of(key, shape, cuts, low, high):
    level, own = 1.0, jax.random.fold_in(key, 6)
    for dim, parts in cuts:
        heights = jnp.exp(jax.random.uniform(jax.random.fold_in(own, dim), (parts,), jnp.float32, low / len(cuts), high / len(cuts)))
        level = level * jnp.repeat(heights, shape[dim] // parts).reshape([-1 if axis == dim else 1 for axis in range(len(shape))])
    return level


def noise(rng, shape, deviation, most, shards=(), kind=jnp.bfloat16):
    entries = deviation * jax.random.normal(rng, shape, jnp.float32)
    if shards:
        entries = entries * steps_of(rng, shape, shards, -0.22, 0.18)
    return jnp.clip(entries, -most, most).astype(kind)


def setup_inputs(seed: int = 0) -> dict:
    keys = jax.random.split(jax.random.key(seed), 11)
    return {
        "tokens_in": noise(keys[0], (SEQS, SLOTS, D), 1.0, 6.0, ((0, 8), (1, 4))),
        "out_grad": noise(keys[1], (SEQS, SLOTS, D), 1.0, 6.0, ((0, 8), (1, 4))),
        "gain_attn": jnp.clip(1.0 + 0.1 * jax.random.normal(keys[2], (D,), jnp.float32), 0.5, 1.5).astype(jnp.bfloat16),
        "gain_mlp": jnp.clip(1.0 + 0.1 * jax.random.normal(keys[3], (D,), jnp.float32), 0.5, 1.5).astype(jnp.bfloat16),
        "w_qkv": noise(keys[4], (D, 3 * D), D ** -0.5, 0.21875, ((0, 8),)),
        "w_out": noise(keys[5], (D, D), (max(1, 4 * D // SLOTS)) ** -0.5, 6.0, ((0, 8),)),
        "w_up": noise(keys[6], (D, FF), D ** -0.5, 0.21875, ((0, 8),)),
        "w_down": noise(keys[7], (FF, D), FF ** -0.5, 0.109375, ((0, 8),)),
        "lengths": draw_lengths(jax.random.fold_in(keys[10], 71), 0),
        "block_order": draw_block_order(jax.random.fold_in(keys[10], 71), 0),
    }


@jax.custom_vjp
def low(v):
    return lax.optimization_barrier(v.astype(jnp.bfloat16)).astype(jnp.float32)

@jax.custom_vjp
def low_back(v):
    return v

def low_keep(v):
    return (low(v), None)

def low_pass(kept, grad):
    return (grad,)

def back_keep(v):
    return (v, None)

def back_low(kept, grad):
    return (low(grad),)
low.defvjp(low_keep, low_pass)
low_back.defvjp(back_keep, back_low)

def product(left_operand, right_operand):
    return jnp.dot(left_operand, right_operand, precision=lax.Precision.HIGHEST, preferred_element_type=jnp.float32)

def layer_norm(values, gain):
    centre = lax.optimization_barrier(jnp.mean(values, axis=-1, keepdims=True))
    centred = values - centre
    spread = lax.optimization_barrier(jnp.mean(centred * centred, axis=-1, keepdims=True))
    return centred * lax.rsqrt(spread + 1e-05) * gain

def sequence_forward(tokens, gain_one, gain_two, w_qkv, w_out, w_up, w_down, positions, length):
    score_scale = HEAD_DIM ** (-0.5)
    normed_one = low(layer_norm(tokens, gain_one))
    packed = low(low_back(product(normed_one, w_qkv)))
    allowed = (positions[None, :] <= positions[:, None]) & (positions[None, :] < length)

    def by_head(matrix):
        return matrix.reshape(SLOTS, HEADS, HEAD_DIM).transpose(1, 0, 2)

    def one_head(triple):
        head_query, head_key, head_value = triple
        scores = low_back(product(head_query, head_key.T) * score_scale)
        magnitude = jnp.abs(scores)
        row_top = lax.optimization_barrier(jnp.max(jnp.where(allowed, magnitude, -1e+30), axis=-1, keepdims=True))
        exponent = jnp.where(allowed, jnp.exp(magnitude - row_top), 0.0)
        positive = exponent / lax.optimization_barrier(jnp.sum(exponent, axis=-1, keepdims=True))
        signed = low(jnp.sign(scores) * positive)
        return product(signed, head_value)
    mixture = lax.map(jax.checkpoint(one_head), (by_head(packed[:, :D]), by_head(packed[:, D:2 * D]), by_head(packed[:, 2 * D:])))
    mixture = low(low_back(mixture.transpose(1, 0, 2).reshape(SLOTS, D)))
    middle = tokens + low_back(product(mixture, w_out))
    normed_two = low(layer_norm(middle, gain_two))
    pre_act = low_back(product(normed_two, w_up))
    activation = low(jax.nn.gelu(pre_act, approximate=True))
    return middle + low_back(product(activation, w_down))

def reference(tokens_in, out_grad, gain_attn, gain_mlp, w_qkv, w_out, w_up, w_down, lengths, block_order):
    params = (gain_attn.astype(jnp.float32), gain_mlp.astype(jnp.float32), w_qkv.astype(jnp.float32), w_out.astype(jnp.float32), w_up.astype(jnp.float32), w_down.astype(jnp.float32))
    offsets = jnp.arange(BLK, dtype=jnp.int32)
    positions_all = (block_order[:, :, None] * BLK + offsets[None, None, :]).reshape(SEQS, SLOTS).astype(jnp.int32)

    def per_sequence(totals, inputs_seq):
        tokens_seq, grad_seq, positions, length = inputs_seq

        def forward(tokens, gain_one, gain_two, weight_a, weight_b, weight_c, weight_d):
            return sequence_forward(tokens, gain_one, gain_two, weight_a, weight_b, weight_c, weight_d, positions, length)
        output, pullback = jax.vjp(forward, tokens_seq.astype(jnp.float32), *params)
        live_mask = (positions < length).astype(jnp.float32)
        gradient_list = pullback(grad_seq.astype(jnp.float32) * live_mask[:, None])
        totals = jax.tree.map(jnp.add, totals, tuple(gradient_list[1:]))
        return (totals, (output.astype(jnp.bfloat16), gradient_list[0].astype(jnp.bfloat16)))
    zeros = jax.tree.map(jnp.zeros_like, params)
    totals, stacked = lax.scan(per_sequence, zeros, (tokens_in, out_grad, positions_all, lengths))
    return (stacked[0], stacked[1], totals[0], totals[1], totals[2], totals[3], totals[4], totals[5])
```

```python
import functools

import jax
import jax.numpy as jnp
from jax import lax
from jax.experimental import pallas as pl
from jax.experimental.pallas import tpu as pltpu
from jax.sharding import PartitionSpec as P

HEAD_DIM = 64
BLK = 512
LOG2E = 1.4426950408889634
BIG = 3e38
LOW = -1e30


def nn(left, right):
    return lax.dot_general(left, right, (((1,), (0,)), ((), ())), preferred_element_type=jnp.float32)


def nt(left, right):
    return lax.dot_general(left, right, (((1,), (1,)), ((), ())), preferred_element_type=jnp.float32)


def sign_of(scores):
    return jnp.tanh(scores.astype(jnp.bfloat16) * jnp.bfloat16(BIG))


def block_mask(key_block, query_block, length):
    keys = key_block * BLK + lax.broadcasted_iota(jnp.int32, (BLK, BLK), 0)
    queries = query_block * BLK + lax.broadcasted_iota(jnp.int32, (BLK, BLK), 1)
    return keys <= jnp.minimum(queries, length - 1)


def split_queries(query_t, weight_ref):
    high = query_t.astype(jnp.bfloat16)
    rest = (query_t - high.astype(jnp.float32)).astype(jnp.bfloat16)
    zero = jnp.zeros((HEAD_DIM, BLK), jnp.bfloat16)
    for head in range(2):
        rows = slice(head * HEAD_DIM, (head + 1) * HEAD_DIM)
        parts = [zero, zero, zero, zero]
        parts[head] = high[rows]
        parts[2 + head] = rest[rows]
        weight_ref[head] = jnp.concatenate(parts, axis=0)


def forward_kernel(table, query_ref, key_ref, value_ref, out_ref, exact_ref, log_ref, value_t, weights):
    length = table[2]
    for part in range(value_ref.shape[0] // BLK):
        rows = slice(part * BLK, (part + 1) * BLK)
        value_t[:, rows] = value_ref[rows, :].T
    for block in range(query_ref.shape[0] // BLK):
        place = table[block]
        rows = slice(block * BLK, (block + 1) * BLK)
        query_t = query_ref[rows, :].astype(jnp.float32).T * (LOG2E * HEAD_DIM ** -0.5)
        split_queries(query_t, weights)
        count = jnp.minimum(place + 1, (length + BLK - 1) // BLK)

        def step(number, carry, masked):
            start = pl.multiple_of(table[4 + number] * BLK, BLK)
            keys = key_ref[pl.ds(start, BLK), :]
            keys = jnp.concatenate([keys, keys], axis=1)
            result = []
            scores_list = [nn(keys, weights[head]) for head in range(2)]
            for head in range(2):
                top, total, mixed = carry[head]
                scores = scores_list[head]
                size = jnp.abs(scores)
                if masked:
                    size = jnp.where(block_mask(number, place, length), size, LOW)
                new_top = jnp.maximum(top, jnp.max(size, axis=0, keepdims=True))
                fade = jnp.exp2(top - new_top)
                powers = jnp.exp2(size - new_top)
                new_total = total * fade + jnp.sum(powers, axis=0, keepdims=True)
                signed = powers.astype(jnp.bfloat16) * sign_of(scores)
                values = value_t[head * HEAD_DIM : (head + 1) * HEAD_DIM, pl.ds(start, BLK)]
                result.append((new_top, new_total, mixed * fade + nn(values, signed)))
            return tuple(result)

        begin = (
            jnp.full((1, BLK), LOW, jnp.float32),
            jnp.zeros((1, BLK), jnp.float32),
            jnp.zeros((HEAD_DIM, BLK), jnp.float32),
        )
        carry = lax.fori_loop(0, count - 1, functools.partial(step, masked=False), (begin, begin))
        carry = step(count - 1, carry, True)
        mixed = jnp.concatenate([c[2] / c[1] for c in carry], axis=0)
        exact_ref[:, rows] = mixed
        out_ref[rows, :] = mixed.T.astype(jnp.bfloat16)
        for head in range(2):
            log_ref[0, head : head + 1, rows] = carry[head][0] + jnp.log2(carry[head][1])


def backward_kernel(
    table,
    query_ref,
    key_ref,
    value_ref,
    grad_ref,
    exact_ref,
    log_ref,
    query_out,
    key_out,
    value_out,
    key_t,
    key_sum,
    value_sum,
    weights,
    grad_weights,
    query_sum,
):
    length = table[2]
    scale = HEAD_DIM ** -0.5
    key_sum[...] = jnp.zeros_like(key_sum)
    value_sum[...] = jnp.zeros_like(value_sum)
    for part in range(key_ref.shape[0] // BLK):
        rows = slice(part * BLK, (part + 1) * BLK)
        key_t[:, rows] = key_ref[rows, :].T
    for block in range(query_ref.shape[0] // BLK):
        place = table[block]
        rows = slice(block * BLK, (block + 1) * BLK)
        query_plain = query_ref[rows, :].astype(jnp.float32).T
        split_queries(query_plain * (LOG2E * scale), weights)
        query_t = query_plain.astype(jnp.bfloat16)
        grad_plain = grad_ref[rows, :].astype(jnp.float32).T
        grad_t = grad_plain.astype(jnp.bfloat16)
        weighted = grad_plain * exact_ref[:, rows]
        zero = jnp.zeros((HEAD_DIM, BLK), jnp.bfloat16)
        grad_weights[0] = jnp.concatenate([grad_t[:HEAD_DIM], zero], axis=0)
        grad_weights[1] = jnp.concatenate([zero, grad_t[HEAD_DIM:]], axis=0)
        dots = [
            jnp.sum(weighted[head * HEAD_DIM : (head + 1) * HEAD_DIM], axis=0, keepdims=True)
            for head in range(2)
        ]
        logs = [log_ref[0, head : head + 1, rows] for head in range(2)]
        query_sum[...] = jnp.zeros_like(query_sum)
        live = place * BLK < length
        count = jnp.where(live, jnp.minimum(place + 1, (length + BLK - 1) // BLK), 0)

        def step(number, masked):
            start = pl.multiple_of(table[4 + number] * BLK, BLK)
            span = pl.ds(start, BLK)
            keys = key_ref[span, :]
            keys = jnp.concatenate([keys, keys], axis=1)
            values = value_ref[span, :]
            scores_list = [nn(keys, weights[head]) for head in range(2)]
            grads_list = [nn(values, grad_weights[head]) for head in range(2)]
            for head in range(2):
                half = slice(head * HEAD_DIM, (head + 1) * HEAD_DIM)
                scores = scores_list[head]
                size = jnp.abs(scores) - logs[head]
                if masked:
                    size = jnp.where(block_mask(number, place, length), size, LOW)
                positive = jnp.exp2(size).astype(jnp.bfloat16)
                sign = sign_of(scores)
                signed = positive * sign
                inner = grads_list[head] - dots[head] * sign.astype(jnp.float32)
                score_grads = (positive.astype(jnp.float32) * inner).astype(jnp.bfloat16)
                value_sum[half, span] += nt(grad_t[half], signed)
                key_sum[half, span] += nt(query_t[half], score_grads)
                query_sum[half, :] += nn(key_t[half, span], score_grads)

        @pl.when(count > 0)
        def _():
            @pl.loop(0, count - 1)
            def _(number):
                step(number, False)

            step(count - 1, True)

        query_out[rows, :] = (query_sum[...] * scale).T.astype(jnp.bfloat16)
    for part in range(key_ref.shape[0] // BLK):
        rows = slice(part * BLK, (part + 1) * BLK)
        key_out[rows, :] = (key_sum[:, rows] * scale).T.astype(jnp.bfloat16)
        value_out[rows, :] = value_sum[:, rows].T.astype(jnp.bfloat16)


def make_table(block_order, length, ctx_index, blocks_here):
    places = lax.dynamic_slice_in_dim(block_order, ctx_index * blocks_here, blocks_here)
    stored = jnp.argsort(block_order).astype(jnp.int32)
    return jnp.concatenate([places, length[None], jnp.zeros((1,), jnp.int32), stored])


def attend_forward(table, packed, pairs_all):
    rows, slots = packed.shape[0], pairs_all.shape[0]
    width = pairs_all.shape[1] // 2
    pairs = width // 128
    return pl.pallas_call(
        forward_kernel,
        grid_spec=pltpu.PrefetchScalarGridSpec(
            num_scalar_prefetch=1,
            grid=(pairs,),
            in_specs=[
                pl.BlockSpec((rows, 128), lambda i, t: (0, i)),
                pl.BlockSpec((slots, 128), lambda i, t: (0, i)),
                pl.BlockSpec((slots, 128), lambda i, t: (0, i + pairs)),
            ],
            out_specs=[
                pl.BlockSpec((rows, 128), lambda i, t: (0, i)),
                pl.BlockSpec((128, rows), lambda i, t: (i, 0)),
                pl.BlockSpec((1, 2, rows), lambda i, t: (i, 0, 0)),
            ],
            scratch_shapes=[
                pltpu.VMEM((128, slots), jnp.bfloat16),
                pltpu.VMEM((2, 256, BLK), jnp.bfloat16),
            ],
        ),
        out_shape=[
            jax.ShapeDtypeStruct((rows, width), jnp.bfloat16),
            jax.ShapeDtypeStruct((width, rows), jnp.float32),
            jax.ShapeDtypeStruct((pairs, 2, rows), jnp.float32),
        ],
        compiler_params=pltpu.CompilerParams(vmem_limit_bytes=48 << 20),
        name="attend_forward",
    )(table, packed, pairs_all, pairs_all)


def attend_backward(table, packed, pairs_all, grad_mixed, exact, logs):
    rows, slots = packed.shape[0], pairs_all.shape[0]
    width = pairs_all.shape[1] // 2
    pairs = width // 128
    return pl.pallas_call(
        backward_kernel,
        grid_spec=pltpu.PrefetchScalarGridSpec(
            num_scalar_prefetch=1,
            grid=(pairs,),
            in_specs=[
                pl.BlockSpec((rows, 128), lambda i, t: (0, i)),
                pl.BlockSpec((slots, 128), lambda i, t: (0, i)),
                pl.BlockSpec((slots, 128), lambda i, t: (0, i + pairs)),
                pl.BlockSpec((rows, 128), lambda i, t: (0, i)),
                pl.BlockSpec((128, rows), lambda i, t: (i, 0)),
                pl.BlockSpec((1, 2, rows), lambda i, t: (i, 0, 0)),
            ],
            out_specs=[
                pl.BlockSpec((rows, 128), lambda i, t: (0, i)),
                pl.BlockSpec((slots, 128), lambda i, t: (0, i)),
                pl.BlockSpec((slots, 128), lambda i, t: (0, i)),
            ],
            scratch_shapes=[
                pltpu.VMEM((128, slots), jnp.bfloat16),
                pltpu.VMEM((128, slots), jnp.float32),
                pltpu.VMEM((128, slots), jnp.float32),
                pltpu.VMEM((2, 256, BLK), jnp.bfloat16),
                pltpu.VMEM((2, 128, BLK), jnp.bfloat16),
                pltpu.VMEM((128, BLK), jnp.float32),
            ],
        ),
        out_shape=[
            jax.ShapeDtypeStruct((rows, width), jnp.bfloat16),
            jax.ShapeDtypeStruct((slots, width), jnp.bfloat16),
            jax.ShapeDtypeStruct((slots, width), jnp.bfloat16),
        ],
        compiler_params=pltpu.CompilerParams(vmem_limit_bytes=48 << 20),
        name="attend_backward",
    )(table, packed, pairs_all, pairs_all, grad_mixed, exact, logs)


def layer_norm(values, gain):
    centre = jnp.mean(values, axis=-1, keepdims=True)
    centred = values - centre
    spread = jnp.mean(centred * centred, axis=-1, keepdims=True)
    return centred * lax.rsqrt(spread + 1e-05) * gain


def gelu_tanh(values):
    return jax.nn.gelu(values, approximate=True)


def project(left_operand, right_operand):
    return jnp.einsum(
        "buj,jn->bun", left_operand, right_operand, preferred_element_type=jnp.float32
    )


def project_back(gradient_list, right_operand):
    return jnp.einsum(
        "mzg,og->mzo", gradient_list, right_operand, preferred_element_type=jnp.float32
    )


def weight_grad(left_operand, gradient_list):
    return jnp.einsum(
        "hcb,hct->bt", left_operand, gradient_list, preferred_element_type=jnp.float32
    )


def per_device(
    tokens_in, out_grad, gain_attn, gain_mlp, w_qkv, w_out, w_up, w_down, lengths, block_order
):
    seq_count, local_rows, width = tokens_in.shape
    ctx_index = lax.axis_index("ctx")
    gain_one, w_qkv_all, w_out_all = (
        lax.all_gather(gain_attn, "fsdp", axis=0, tiled=True),
        lax.all_gather(w_qkv, "fsdp", axis=0, tiled=True),
        lax.all_gather(w_out, "fsdp", axis=0, tiled=True),
    )
    offsets = jnp.arange(BLK, dtype=jnp.int32)
    key_places = (block_order[:, :, None] * BLK + offsets[None, None, :]).reshape(seq_count, -1)
    query_places = lax.dynamic_slice_in_dim(key_places, ctx_index * local_rows, local_rows, 1)
    tokens_f = tokens_in.astype(jnp.float32)
    normed_one, norm_one_back = jax.vjp(layer_norm, tokens_f, gain_one.astype(jnp.float32))
    normed_one = normed_one.astype(jnp.bfloat16)
    packed = project(normed_one, w_qkv_all).astype(jnp.bfloat16)
    pairs_all = lax.all_gather(packed[0, :, width:], "ctx", axis=0, tiled=True)
    table = make_table(block_order[0], lengths[0], ctx_index, local_rows // BLK)
    mixture, exact, logs = attend_forward(table, packed[0], pairs_all)
    mixed = mixture[None]
    middle = tokens_f + project(mixed, w_out_all)
    gain_two, w_up_all, w_down_all = (
        lax.all_gather(gain_mlp, "fsdp", axis=0, tiled=True),
        lax.all_gather(w_up, "fsdp", axis=0, tiled=True),
        lax.all_gather(w_down, "fsdp", axis=0, tiled=True),
    )
    normed_two, norm_two_back = jax.vjp(layer_norm, middle, gain_two.astype(jnp.float32))
    normed_two = normed_two.astype(jnp.bfloat16)
    pre_act = project(normed_two, w_up_all)
    activation, gelu_back = jax.vjp(gelu_tanh, pre_act)
    activation = activation.astype(jnp.bfloat16)
    result = (middle + project(activation, w_down_all)).astype(jnp.bfloat16)
    w_up_back, w_down_back = (
        lax.all_gather(w_up, "fsdp", axis=0, tiled=True),
        lax.all_gather(w_down, "fsdp", axis=0, tiled=True),
    )
    live_mask = (query_places < lengths[:, None]).astype(jnp.float32)
    output_gradient = out_grad.astype(jnp.float32) * live_mask[:, :, None]
    grad_z = output_gradient.astype(jnp.bfloat16)
    grad_w_down = weight_grad(activation, grad_z)
    grad_act = project_back(grad_z, w_down_back)
    grad_pre = gelu_back(grad_act)[0].astype(jnp.bfloat16)
    grad_w_up = weight_grad(normed_two, grad_pre)
    grad_normed_two = project_back(grad_pre, w_up_back)
    grad_middle_norm, grad_gain_two = norm_two_back(grad_normed_two)
    mlp_shards = (
        lax.psum_scatter(grad_w_up, "fsdp", scatter_dimension=0, tiled=True),
        lax.psum_scatter(grad_w_down, "fsdp", scatter_dimension=0, tiled=True),
        lax.psum_scatter(grad_gain_two, "fsdp", scatter_dimension=0, tiled=True),
    )
    grad_middle = output_gradient + grad_middle_norm
    w_qkv_back, w_out_back = (
        lax.all_gather(w_qkv, "fsdp", axis=0, tiled=True),
        lax.all_gather(w_out, "fsdp", axis=0, tiled=True),
    )
    grad_branch = grad_middle.astype(jnp.bfloat16)
    grad_w_out = weight_grad(mixed, grad_branch)
    grad_mixed = project_back(grad_branch, w_out_back).astype(jnp.bfloat16)
    query_grads, key_gradients, value_grads = attend_backward(
        table, packed[0], pairs_all, grad_mixed[0], exact, logs
    )
    key_mine = lax.psum_scatter(key_gradients, "ctx", scatter_dimension=0, tiled=True)
    value_mine = lax.psum_scatter(value_grads, "ctx", scatter_dimension=0, tiled=True)
    packed_items = [jnp.concatenate([query_grads, key_mine, value_mine], axis=-1)]
    grad_packed = jnp.stack(packed_items).astype(jnp.bfloat16)
    grad_w_qkv = weight_grad(normed_one, grad_packed)
    grad_normed_one = project_back(grad_packed, w_qkv_back)
    grad_tokens_norm, grad_gain_one = norm_one_back(grad_normed_one)
    grad_tokens = (grad_middle + grad_tokens_norm).astype(jnp.bfloat16)
    attn_shards = (
        lax.psum_scatter(grad_w_qkv, "fsdp", scatter_dimension=0, tiled=True),
        lax.psum_scatter(grad_w_out, "fsdp", scatter_dimension=0, tiled=True),
        lax.psum_scatter(grad_gain_one, "fsdp", scatter_dimension=0, tiled=True),
    )
    summed = (
        lax.psum(attn_shards[0].astype(jnp.bfloat16), "ctx").astype(jnp.float32),
        lax.psum(attn_shards[1].astype(jnp.bfloat16), "ctx").astype(jnp.float32),
        lax.psum(attn_shards[2].astype(jnp.bfloat16), "ctx").astype(jnp.float32),
        lax.psum(mlp_shards[0].astype(jnp.bfloat16), "ctx").astype(jnp.float32),
        lax.psum(mlp_shards[1].astype(jnp.bfloat16), "ctx").astype(jnp.float32),
        lax.psum(mlp_shards[2].astype(jnp.bfloat16), "ctx").astype(jnp.float32),
    )
    return (result, grad_tokens, summed[2], summed[5], summed[0], summed[1], summed[3], summed[4])


def solution(mesh):
    return jax.shard_map(
        per_device,
        mesh=mesh,
        in_specs=(
            P("fsdp", "ctx", None),
            P("fsdp", "ctx", None),
            P("fsdp"),
            P("fsdp"),
            P("fsdp", None),
            P("fsdp", None),
            P("fsdp", None),
            P("fsdp", None),
            P("fsdp"),
            P("fsdp", None),
        ),
        out_specs=(
            P("fsdp", "ctx", None),
            P("fsdp", "ctx", None),
            P("fsdp"),
            P("fsdp"),
            P("fsdp", None),
            P("fsdp", None),
            P("fsdp", None),
            P("fsdp", None),
        ),
        check_vma=False,
    )
```

```python
import functools

import jax
import jax.numpy as jnp
from jax import lax
from jax.experimental import pallas as pl
from jax.experimental.pallas import tpu as pltpu
from jax.sharding import PartitionSpec as P

HEAD_DIM = 64
BLK = 512
HALF = 256
LOG2E = 1.4426950408889634
BIG = 3e38
LOW = -1e30


def nn(left, right):
    return lax.dot_general(left, right, (((1,), (0,)), ((), ())), preferred_element_type=jnp.float32)


def nt(left, right):
    return lax.dot_general(left, right, (((1,), (1,)), ((), ())), preferred_element_type=jnp.float32)


def sign_of(scores):
    return jnp.tanh(scores.astype(jnp.bfloat16) * jnp.bfloat16(BIG))


def block_mask(key_start, query_start, length, shape):
    keys = key_start + lax.broadcasted_iota(jnp.int32, shape, 0)
    queries = query_start + lax.broadcasted_iota(jnp.int32, shape, 1)
    return keys <= jnp.minimum(queries, length - 1)


def gather_columns(refs, out):
    span = refs[0].shape[1]
    for part, ref in enumerate(refs):
        out[:, part * span : (part + 1) * span] = ref[...]


def turn_rows(source, out, twice):
    for part in range(source.shape[1] // BLK):
        span = slice(part * BLK, (part + 1) * BLK)
        piece = source[:, span]
        out[span, :] = jnp.concatenate([piece, piece if twice else jnp.zeros_like(piece)], axis=0).T


def query_weights(query_t):
    scaled = query_t.astype(jnp.float32) * (LOG2E * HEAD_DIM ** -0.5)
    high = scaled.astype(jnp.bfloat16)
    return jnp.concatenate([high, (scaled - high.astype(jnp.float32)).astype(jnp.bfloat16)], axis=0)


def forward_kernel(parts, table, *refs):
    query_refs, key_refs, value_refs = refs[:parts], refs[parts : 2 * parts], refs[2 * parts : 3 * parts]
    sends = refs[3 * parts : 4 * parts]
    exact_ref, log_ref, queries, keys_t, values, keys, weights = refs[4 * parts :]
    blocks = queries.shape[1] // BLK
    length = table[blocks]
    gather_columns(query_refs, queries)
    gather_columns(key_refs, keys_t)
    gather_columns(value_refs, values)
    turn_rows(keys_t, keys, True)
    full = (length + BLK - 1) // BLK

    @pl.loop(0, blocks)
    def _(place):
        span = pl.ds(pl.multiple_of(table[place] * BLK, BLK), BLK)
        weights[...] = query_weights(queries[:, span])
        count = jnp.minimum(place + 1, full)

        def step(number, carry, masked):
            key_span = pl.ds(pl.multiple_of(table[number] * BLK, BLK), BLK)
            key_rows = keys[key_span, :]
            value_rows = values[:, key_span]
            result = []
            scores_list = [nn(key_rows, weights[:, h * HALF : (h + 1) * HALF]) for h in range(2)]
            for half in range(2):
                top, total, mixed = carry[half]
                scores = scores_list[half]
                size = jnp.abs(scores)
                if masked:
                    mask = block_mask(number * BLK, place * BLK + half * HALF, length, size.shape)
                    size = jnp.where(mask, size, LOW)
                new_top = jnp.maximum(top, jnp.max(size, axis=0, keepdims=True))
                fade = jnp.exp2(top - new_top)
                powers = jnp.exp2(size - new_top)
                new_total = total * fade + jnp.sum(powers, axis=0, keepdims=True)
                signed = powers.astype(jnp.bfloat16) * sign_of(scores)
                result.append((new_top, new_total, mixed * fade + nn(value_rows, signed)))
            return tuple(result)

        begin = (
            jnp.full((1, HALF), LOW, jnp.float32),
            jnp.zeros((1, HALF), jnp.float32),
            jnp.zeros((HEAD_DIM, HALF), jnp.float32),
        )
        carry = lax.fori_loop(0, count - 1, functools.partial(step, masked=False), (begin, begin))
        carry = step(count - 1, carry, True)
        exact_ref[:, span] = jnp.concatenate([c[2] / c[1] for c in carry], axis=1)
        log_ref[:, span] = jnp.concatenate([c[0] + jnp.log2(c[1]) for c in carry], axis=1)

    width = sends[0].shape[1]
    for part in range(parts):
        sends[part][...] = exact_ref[:, part * width : (part + 1) * width].astype(jnp.bfloat16)


def backward_kernel(parts, table, *refs):
    query_refs, key_refs, value_refs = refs[:parts], refs[parts : 2 * parts], refs[2 * parts : 3 * parts]
    grad_refs, refs = refs[3 * parts : 4 * parts], refs[4 * parts :]
    exact_ref, log_ref, sends, refs = refs[0], refs[1], refs[2 : 2 + parts], refs[2 + parts :]
    whole_ref, queries, keys_t, values_t, grads, keys, values, sums, weights, grad_weights, dots = refs
    blocks = queries.shape[1] // BLK
    length = table[blocks]
    scale = HEAD_DIM ** -0.5
    gather_columns(query_refs, queries)
    gather_columns(key_refs, keys_t)
    gather_columns(value_refs, values_t)
    gather_columns(grad_refs, grads)
    turn_rows(keys_t, keys, True)
    turn_rows(values_t, values, False)
    sums[...] = jnp.zeros_like(sums)
    grad_weights[...] = jnp.zeros_like(grad_weights)
    full = (length + BLK - 1) // BLK

    @pl.loop(0, full)
    def _(place):
        span = pl.ds(pl.multiple_of(table[place] * BLK, BLK), BLK)
        weights[...] = query_weights(queries[:, span])
        grad_t = grads[:, span]
        grad_weights[:HEAD_DIM, :] = grad_t
        dots[...] = jnp.sum(grad_t.astype(jnp.float32) * exact_ref[:, span], axis=0, keepdims=True)

        def step(number, masked):
            key_span = pl.ds(pl.multiple_of(table[number] * BLK, BLK), BLK)
            key_rows, value_rows = keys[key_span, :], values[key_span, :]
            halves = [slice(h * HALF, (h + 1) * HALF) for h in range(2)]
            scores_list = [nn(key_rows, weights[:, h]) for h in halves]
            inner_list = [nn(value_rows, grad_weights[:, h]) for h in halves]
            signed_list, score_grads_list = [], []
            for half in range(2):
                scores = scores_list[half]
                log_row = log_ref[:, pl.ds(pl.multiple_of(table[place] * BLK + half * HALF, HALF), HALF)]
                size = jnp.abs(scores) - log_row
                if masked:
                    mask = block_mask(number * BLK, place * BLK + half * HALF, length, size.shape)
                    size = jnp.where(mask, size, LOW)
                positive = jnp.exp2(size).astype(jnp.bfloat16)
                sign = sign_of(scores)
                signed_list.append(positive * sign)
                inner = inner_list[half] - dots[:, halves[half]] * sign.astype(jnp.float32)
                score_grads_list.append((positive.astype(jnp.float32) * inner).astype(jnp.bfloat16))
            signed = jnp.concatenate(signed_list, axis=1)
            score_grads = jnp.concatenate(score_grads_list, axis=1)
            sums[0:64, span] += nn(keys_t[:, key_span], score_grads)
            sums[64:128, key_span] += nt(queries[:, span], score_grads)
            sums[128:192, key_span] += nt(grads[:, span], signed)

        @pl.loop(0, place)
        def _(number):
            step(number, False)

        step(place, True)

    width = sends[0].shape[1]
    for part in range(parts):
        span = slice(part * width, (part + 1) * width)
        for rows, factor in ((slice(0, 128), scale), (slice(128, 192), 1.0)):
            done = (sums[rows, span] * factor).astype(jnp.bfloat16)
            whole_ref[rows, span] = done
            sends[part][rows, :] = done


def make_table(block_order, length, ctx_index, ctx):
    here = block_order.shape[0] // ctx
    order = (ctx_index - jnp.arange(ctx)) % ctx
    places = block_order.reshape(ctx, here)[order].reshape(-1)
    return jnp.concatenate([jnp.argsort(places).astype(jnp.int32), length[None]])


def head_specs(parts, span, row):
    return [pl.BlockSpec((HEAD_DIM, span), lambda i, t, row=row: (row, 0)) for _ in range(parts)]


def attend_forward(table, head, heads, packed_list):
    parts, span = len(packed_list), packed_list[0].shape[1]
    slots = parts * span
    whole = lambda shape: pl.BlockSpec(shape, lambda i, t: (0, 0))
    return pl.pallas_call(
        functools.partial(forward_kernel, parts),
        grid_spec=pltpu.PrefetchScalarGridSpec(
            num_scalar_prefetch=1,
            grid=(1,),
            in_specs=head_specs(parts, span, head)
            + head_specs(parts, span, heads + head)
            + head_specs(parts, span, 2 * heads + head),
            out_specs=[whole((HEAD_DIM, span))] * parts + [whole((HEAD_DIM, slots)), whole((1, slots))],
            scratch_shapes=[pltpu.VMEM((HEAD_DIM, slots), jnp.bfloat16)] * 3
            + [pltpu.VMEM((slots, 128), jnp.bfloat16), pltpu.VMEM((128, BLK), jnp.bfloat16)],
        ),
        out_shape=[jax.ShapeDtypeStruct((HEAD_DIM, span), jnp.bfloat16)] * parts
        + [
            jax.ShapeDtypeStruct((HEAD_DIM, slots), jnp.float32),
            jax.ShapeDtypeStruct((1, slots), jnp.float32),
        ],
        compiler_params=pltpu.CompilerParams(vmem_limit_bytes=40 << 20),
        cost_estimate=pl.CostEstimate(flops=20_000_000_000, bytes_accessed=4_000_000, transcendentals=0),
        name="attend_forward",
    )(table, *packed_list, *packed_list, *packed_list)


def attend_backward(table, head, heads, packed_list, grad_list, exact, logs):
    parts, span = len(packed_list), packed_list[0].shape[1]
    slots = parts * span
    whole = lambda shape: pl.BlockSpec(shape, lambda i, t: (0, 0))
    three = 3 * HEAD_DIM
    return pl.pallas_call(
        functools.partial(backward_kernel, parts),
        grid_spec=pltpu.PrefetchScalarGridSpec(
            num_scalar_prefetch=1,
            grid=(1,),
            in_specs=head_specs(parts, span, head)
            + head_specs(parts, span, heads + head)
            + head_specs(parts, span, 2 * heads + head)
            + [whole((HEAD_DIM, span))] * parts
            + [whole((HEAD_DIM, slots)), whole((1, slots))],
            out_specs=[whole((three, span))] * parts + [whole((three, slots))],
            scratch_shapes=[pltpu.VMEM((HEAD_DIM, slots), jnp.bfloat16)] * 4
            + [pltpu.VMEM((slots, 128), jnp.bfloat16)] * 2
            + [
                pltpu.VMEM((three, slots), jnp.float32),
                pltpu.VMEM((128, BLK), jnp.bfloat16),
                pltpu.VMEM((128, BLK), jnp.bfloat16),
                pltpu.VMEM((1, BLK), jnp.float32),
            ],
        ),
        out_shape=[jax.ShapeDtypeStruct((three, span), jnp.bfloat16)] * parts
        + [jax.ShapeDtypeStruct((three, slots), jnp.bfloat16)],
        compiler_params=pltpu.CompilerParams(vmem_limit_bytes=40 << 20),
        cost_estimate=pl.CostEstimate(flops=40_000_000_000, bytes_accessed=6_000_000, transcendentals=0),
        name="attend_backward",
    )(table, *packed_list, *packed_list, *packed_list, *grad_list, exact, logs)


def layer_norm(values, gain):
    centre = jnp.mean(values, axis=-1, keepdims=True)
    centred = values - centre
    spread = jnp.mean(centred * centred, axis=-1, keepdims=True)
    return centred * lax.rsqrt(spread + 1e-05) * gain


def gelu_tanh(values):
    return jax.nn.gelu(values, approximate=True)


def product(equation, left, right):
    return jnp.einsum(equation, left, right, preferred_element_type=jnp.float32)


def shift(array, ctx, by):
    if by % ctx == 0:
        return array
    return lax.ppermute(array, "ctx", [(i, (i + by) % ctx) for i in range(ctx)])


def turned(array, axis, by):
    return lax.dynamic_slice_in_dim(
        jnp.concatenate([array, array], axis=axis), by, array.shape[axis], axis
    )


def gather_rows(array):
    return lax.all_gather(array, "fsdp", axis=0, tiled=True)


def scatter_rows(array):
    return lax.psum_scatter(
        array.astype(jnp.bfloat16), "fsdp", scatter_dimension=0, tiled=True
    )


def per_device(
    ctx, tokens_in, out_grad, gain_attn, gain_mlp, w_qkv, w_out, w_up, w_down, lengths, block_order
):
    local_rows, width = tokens_in.shape[1:]
    tokens_in, out_grad, length, block_order = tokens_in[0], out_grad[0], lengths[0], block_order[0]
    ctx_index = lax.axis_index("ctx")
    heads_here = width // HEAD_DIM // ctx
    own = heads_here * HEAD_DIM
    table = make_table(block_order, length, ctx_index, ctx)

    tokens_list = [tokens_in]
    for _ in range(1, ctx):
        tokens_list.append(shift(tokens_list[-1], ctx, 1))

    gains = jnp.stack([gain_attn, gain_mlp], axis=1)
    gains = jnp.pad(gains, ((0, 0), (0, 126)))
    first = gather_rows(jnp.concatenate([w_qkv, gains], axis=1))
    w_qkv_all = first[:, : 3 * width]
    gain_one = first[:, 3 * width].astype(jnp.float32)
    gain_two = first[:, 3 * width + 1].astype(jnp.float32)
    w_out_all = gather_rows(w_out)
    w_up_all = gather_rows(w_up)
    w_down_all = gather_rows(w_down)

    w_heads = w_qkv_all.reshape(width, 3, ctx, own)
    w_own = lax.dynamic_index_in_dim(w_heads, ctx_index, 2, keepdims=False).reshape(width, 3 * own)
    normed_list, packed_list = [], []
    for part in range(ctx):
        normed = layer_norm(tokens_list[part].astype(jnp.float32), gain_one).astype(jnp.bfloat16)
        normed_list.append(normed)
        packed_list.append(product("jn,uj->nu", w_own, normed).astype(jnp.bfloat16))
    kept, mixed_parts = [], []
    for head in range(heads_here):
        results = attend_forward(table, head, heads_here, packed_list)
        kept.append((results[ctx], results[ctx + 1]))
        mixed_parts += [shift(results[part], ctx, -part) for part in range(ctx)]
    mixed_t = jnp.concatenate(mixed_parts, axis=0)

    w_out_turned = turned(w_out_all.reshape(ctx, heads_here, HEAD_DIM, width), 0, ctx_index)
    w_out_turned = w_out_turned.transpose(1, 0, 2, 3).reshape(width, width)
    tokens_f = tokens_in.astype(jnp.float32)
    middle = tokens_f + product("nu,nj->uj", mixed_t, w_out_turned)
    normed_two, norm_two_back = jax.vjp(lambda v: layer_norm(v, gain_two), middle)
    normed_two = normed_two.astype(jnp.bfloat16)
    pre_act, = (product("uj,jn->un", normed_two, w_up_all),)
    activation, gelu_back = jax.vjp(gelu_tanh, pre_act)
    activation = activation.astype(jnp.bfloat16)
    result = (middle + product("un,nj->uj", activation, w_down_all)).astype(jnp.bfloat16)

    here = local_rows // BLK
    places = lax.dynamic_slice_in_dim(block_order, ctx_index * here, here)
    places = (places[:, None] * BLK + jnp.arange(BLK, dtype=jnp.int32)[None]).reshape(-1)
    grad_y = out_grad.astype(jnp.float32) * (places < length).astype(jnp.float32)[:, None]
    grad_z = grad_y.astype(jnp.bfloat16)
    grad_act = product("uj,nj->un", grad_z, w_down_all)
    grad_pre = gelu_back(grad_act)[0].astype(jnp.bfloat16)
    grad_normed_two = product("un,jn->uj", grad_pre, w_up_all)
    grad_middle = grad_y + norm_two_back(grad_normed_two)[0]
    grad_branch = grad_middle.astype(jnp.bfloat16)
    grad_mixed_t = product("nj,uj->nu", w_out_turned, grad_branch).astype(jnp.bfloat16)
    grads_by_head = []
    for head in range(heads_here):
        pieces = []
        for part in range(ctx):
            row = (head * ctx + part) * HEAD_DIM
            pieces.append(shift(grad_mixed_t[row : row + HEAD_DIM], ctx, part))
        grads_by_head.append(pieces)

    grad_w_down = scatter_rows(product("un,uj->nj", activation, grad_z))
    grad_w_up = scatter_rows(product("uj,un->jn", normed_two, grad_pre))
    grad_w_out = product("nu,uj->nj", mixed_t, grad_branch).astype(jnp.bfloat16)
    grad_w_out = turned(
        grad_w_out.reshape(heads_here, ctx, HEAD_DIM, width).transpose(1, 0, 2, 3), 0, (ctx - ctx_index) % ctx
    )
    grad_w_out = scatter_rows(grad_w_out.reshape(width, width))

    grad_parts, grad_whole = [], []
    for head in range(heads_here):
        results = attend_backward(
            table, head, heads_here, packed_list, grads_by_head[head], *kept[head]
        )
        grad_parts += [shift(results[part], ctx, -part) for part in range(ctx)]
        grad_whole.append(results[ctx])
    normed_all = jnp.concatenate(normed_list, axis=0)
    grad_qkv_own = product("uj,nu->jn", normed_all, jnp.concatenate(grad_whole, axis=0))
    grad_qkv_own = scatter_rows(grad_qkv_own)
    grad_qkv = lax.all_gather(grad_qkv_own, "ctx", axis=0)
    rows_here = grad_qkv.shape[1]
    grad_qkv = grad_qkv.reshape(ctx, rows_here, heads_here, 3, HEAD_DIM)
    grad_w_qkv = grad_qkv.transpose(1, 3, 0, 2, 4).reshape(rows_here, 3 * width).astype(jnp.float32)

    w_turned = turned(w_qkv_all.reshape(width, 3, ctx, heads_here, HEAD_DIM), 2, ctx_index)
    w_turned = w_turned.transpose(0, 3, 2, 1, 4).reshape(width, 3 * width)
    grad_packed_t = jnp.concatenate(grad_parts, axis=0)
    grad_normed_one = product("nu,jn->uj", grad_packed_t, w_turned)
    norm_one_back = jax.vjp(lambda v: layer_norm(v, gain_one), tokens_f)[1]
    grad_tokens = (grad_middle + norm_one_back(grad_normed_one)[0]).astype(jnp.bfloat16)

    grad_w_out, grad_w_up, grad_w_down = [
        lax.psum(g, "ctx").astype(jnp.float32) for g in (grad_w_out, grad_w_up, grad_w_down)
    ]

    def gain_grad(grad_weight, weight, gain):
        total = jnp.sum(grad_weight * weight.astype(jnp.float32), axis=1)
        return total / gain.astype(jnp.float32)

    return (
        result[None],
        grad_tokens[None],
        gain_grad(grad_w_qkv, w_qkv, gain_attn),
        gain_grad(grad_w_up, w_up, gain_mlp),
        grad_w_qkv,
        grad_w_out,
        grad_w_up,
        grad_w_down,
    )


def solution(mesh):
    rows = P("fsdp", None)
    whole = P("fsdp", "ctx", None)
    return jax.shard_map(
        functools.partial(per_device, mesh.shape["ctx"]),
        mesh=mesh,
        in_specs=(whole, whole, P("fsdp"), P("fsdp"), rows, rows, rows, rows, P("fsdp"), rows),
        out_specs=(whole, whole, P("fsdp"), P("fsdp"), rows, rows, rows, rows),
        check_vma=False,
    )
```

```python
import functools

import jax
import jax.numpy as jnp
from jax import lax
from jax.experimental import pallas as pl
from jax.experimental.pallas import tpu as pltpu
from jax.sharding import PartitionSpec as P


HEAD_DIM = 64
BLK = 512
HALF = 256
LOG2E = 1.4426950408889634
BIG = 3e38
LOW = -1e30


def nn(left, right):
    return lax.dot_general(left, right, (((1,), (0,)), ((), ())), preferred_element_type=jnp.float32)


def nt(left, right):
    return lax.dot_general(left, right, (((1,), (1,)), ((), ())), preferred_element_type=jnp.float32)


def sign_of(scores):
    return jnp.tanh(scores.astype(jnp.bfloat16) * jnp.bfloat16(BIG))


def block_mask(key_start, query_start, length, shape):
    keys = key_start + lax.broadcasted_iota(jnp.int32, shape, 0)
    queries = query_start + lax.broadcasted_iota(jnp.int32, shape, 1)
    return keys <= jnp.minimum(queries, length - 1)


def gather_columns(refs, out):
    span = refs[0].shape[1]
    for part, ref in enumerate(refs):
        out[:, part * span : (part + 1) * span] = ref[...]


def turn_rows(source, out, twice):
    for part in range(source.shape[1] // BLK):
        span = slice(part * BLK, (part + 1) * BLK)
        piece = source[:, span]
        out[span, :] = jnp.concatenate([piece, piece if twice else jnp.zeros_like(piece)], axis=0).T


def query_weights(query_t):
    scaled = query_t.astype(jnp.float32) * (LOG2E * HEAD_DIM ** -0.5)
    high = scaled.astype(jnp.bfloat16)
    return jnp.concatenate([high, (scaled - high.astype(jnp.float32)).astype(jnp.bfloat16)], axis=0)


def forward_kernel(parts, table, *refs):
    query_refs, key_refs, value_refs = refs[:parts], refs[parts : 2 * parts], refs[2 * parts : 3 * parts]
    sends = refs[3 * parts : 4 * parts]
    exact_ref, log_ref, queries, keys_t, values, keys, weights = refs[4 * parts :]
    blocks = queries.shape[1] // BLK
    length = table[blocks]
    gather_columns(query_refs, queries)
    gather_columns(key_refs, keys_t)
    gather_columns(value_refs, values)
    turn_rows(keys_t, keys, True)
    full = (length + BLK - 1) // BLK

    @pl.loop(0, blocks)
    def _(place):
        span = pl.ds(pl.multiple_of(table[place] * BLK, BLK), BLK)
        weights[...] = query_weights(queries[:, span])
        count = jnp.minimum(place + 1, full)

        def step(number, carry, masked):
            key_span = pl.ds(pl.multiple_of(table[number] * BLK, BLK), BLK)
            key_rows = keys[key_span, :]
            value_rows = values[:, key_span]
            result = []
            scores_list = [nn(key_rows, weights[:, h * HALF : (h + 1) * HALF]) for h in range(2)]
            for half in range(2):
                top, total, mixed = carry[half]
                scores = scores_list[half]
                size = jnp.abs(scores)
                if masked:
                    mask = block_mask(number * BLK, place * BLK + half * HALF, length, size.shape)
                    size = jnp.where(mask, size, LOW)
                new_top = jnp.maximum(top, jnp.max(size, axis=0, keepdims=True))
                fade = jnp.exp2(top - new_top)
                powers = jnp.exp2(size - new_top)
                new_total = total * fade + jnp.sum(powers, axis=0, keepdims=True)
                signed = powers.astype(jnp.bfloat16) * sign_of(scores)
                result.append((new_top, new_total, mixed * fade + nn(value_rows, signed)))
            return tuple(result)

        begin = (
            jnp.full((1, HALF), LOW, jnp.float32),
            jnp.zeros((1, HALF), jnp.float32),
            jnp.zeros((HEAD_DIM, HALF), jnp.float32),
        )
        carry = lax.fori_loop(0, count - 1, functools.partial(step, masked=False), (begin, begin))
        carry = step(count - 1, carry, True)
        exact_ref[:, span] = jnp.concatenate([c[2] / c[1] for c in carry], axis=1)
        log_ref[:, span] = jnp.concatenate([c[0] + jnp.log2(c[1]) for c in carry], axis=1)

    width = sends[0].shape[1]
    for part in range(parts):
        sends[part][...] = exact_ref[:, part * width : (part + 1) * width].astype(jnp.bfloat16)


def backward_kernel(parts, table, *refs):
    query_refs, key_refs, value_refs = refs[:parts], refs[parts : 2 * parts], refs[2 * parts : 3 * parts]
    grad_refs, refs = refs[3 * parts : 4 * parts], refs[4 * parts :]
    exact_ref, log_ref, sends, refs = refs[0], refs[1], refs[2 : 2 + parts], refs[2 + parts :]
    whole_ref, queries, keys_t, values_t, grads, keys, values, sums, weights, grad_weights, dots = refs
    blocks = queries.shape[1] // BLK
    length = table[blocks]
    scale = HEAD_DIM ** -0.5
    gather_columns(query_refs, queries)
    gather_columns(key_refs, keys_t)
    gather_columns(value_refs, values_t)
    gather_columns(grad_refs, grads)
    turn_rows(keys_t, keys, True)
    turn_rows(values_t, values, False)
    sums[...] = jnp.zeros_like(sums)
    grad_weights[...] = jnp.zeros_like(grad_weights)
    full = (length + BLK - 1) // BLK

    @pl.loop(0, full)
    def _(place):
        span = pl.ds(pl.multiple_of(table[place] * BLK, BLK), BLK)
        weights[...] = query_weights(queries[:, span])
        grad_t = grads[:, span]
        grad_weights[:HEAD_DIM, :] = grad_t
        dots[...] = jnp.sum(grad_t.astype(jnp.float32) * exact_ref[:, span], axis=0, keepdims=True)

        def step(number, masked):
            key_span = pl.ds(pl.multiple_of(table[number] * BLK, BLK), BLK)
            key_rows, value_rows = keys[key_span, :], values[key_span, :]
            halves = [slice(h * HALF, (h + 1) * HALF) for h in range(2)]
            scores_list = [nn(key_rows, weights[:, h]) for h in halves]
            inner_list = [nn(value_rows, grad_weights[:, h]) for h in halves]
            signed_list, score_grads_list = [], []
            for half in range(2):
                scores = scores_list[half]
                log_row = log_ref[:, pl.ds(pl.multiple_of(table[place] * BLK + half * HALF, HALF), HALF)]
                size = jnp.abs(scores) - log_row
                if masked:
                    mask = block_mask(number * BLK, place * BLK + half * HALF, length, size.shape)
                    size = jnp.where(mask, size, LOW)
                positive = jnp.exp2(size).astype(jnp.bfloat16)
                sign = sign_of(scores)
                signed_list.append(positive * sign)
                inner = inner_list[half] - dots[:, halves[half]] * sign.astype(jnp.float32)
                score_grads_list.append((positive.astype(jnp.float32) * inner).astype(jnp.bfloat16))
            signed = jnp.concatenate(signed_list, axis=1)
            score_grads = jnp.concatenate(score_grads_list, axis=1)
            sums[0:64, span] += nn(keys_t[:, key_span], score_grads)
            sums[64:128, key_span] += nt(queries[:, span], score_grads)
            sums[128:192, key_span] += nt(grads[:, span], signed)

        @pl.loop(0, place)
        def _(number):
            step(number, False)

        step(place, True)

    width = sends[0].shape[1]
    for part in range(parts):
        span = slice(part * width, (part + 1) * width)
        for rows, factor in ((slice(0, 128), scale), (slice(128, 192), 1.0)):
            done = (sums[rows, span] * factor).astype(jnp.bfloat16)
            whole_ref[rows, span] = done
            sends[part][rows, :] = done


def make_table(block_order, length, ctx_index, ctx):
    here = block_order.shape[0] // ctx
    order = (ctx_index - jnp.arange(ctx)) % ctx
    places = block_order.reshape(ctx, here)[order].reshape(-1)
    return jnp.concatenate([jnp.argsort(places).astype(jnp.int32), length[None]])


def head_specs(parts, span, row):
    return [pl.BlockSpec((HEAD_DIM, span), lambda i, t, row=row: (row, 0)) for _ in range(parts)]


def attend_forward(table, head, heads, packed_list):
    parts, span = len(packed_list), packed_list[0].shape[1]
    slots = parts * span
    whole = lambda shape: pl.BlockSpec(shape, lambda i, t: (0, 0))
    return pl.pallas_call(
        functools.partial(forward_kernel, parts),
        grid_spec=pltpu.PrefetchScalarGridSpec(
            num_scalar_prefetch=1,
            grid=(1,),
            in_specs=head_specs(parts, span, head)
            + head_specs(parts, span, heads + head)
            + head_specs(parts, span, 2 * heads + head),
            out_specs=[whole((HEAD_DIM, span))] * parts + [whole((HEAD_DIM, slots)), whole((1, slots))],
            scratch_shapes=[pltpu.VMEM((HEAD_DIM, slots), jnp.bfloat16)] * 3
            + [pltpu.VMEM((slots, 128), jnp.bfloat16), pltpu.VMEM((128, BLK), jnp.bfloat16)],
        ),
        out_shape=[jax.ShapeDtypeStruct((HEAD_DIM, span), jnp.bfloat16)] * parts
        + [
            jax.ShapeDtypeStruct((HEAD_DIM, slots), jnp.float32),
            jax.ShapeDtypeStruct((1, slots), jnp.float32),
        ],
        compiler_params=pltpu.CompilerParams(vmem_limit_bytes=40 << 20),
        cost_estimate=pl.CostEstimate(flops=20_000_000_000, bytes_accessed=4_000_000, transcendentals=0),
        name="attend_forward",
    )(table, *packed_list, *packed_list, *packed_list)


def attend_backward(table, head, heads, packed_list, grad_list, exact, logs):
    parts, span = len(packed_list), packed_list[0].shape[1]
    slots = parts * span
    whole = lambda shape: pl.BlockSpec(shape, lambda i, t: (0, 0))
    three = 3 * HEAD_DIM
    return pl.pallas_call(
        functools.partial(backward_kernel, parts),
        grid_spec=pltpu.PrefetchScalarGridSpec(
            num_scalar_prefetch=1,
            grid=(1,),
            in_specs=head_specs(parts, span, head)
            + head_specs(parts, span, heads + head)
            + head_specs(parts, span, 2 * heads + head)
            + [whole((HEAD_DIM, span))] * parts
            + [whole((HEAD_DIM, slots)), whole((1, slots))],
            out_specs=[whole((three, span))] * parts + [whole((three, slots))],
            scratch_shapes=[pltpu.VMEM((HEAD_DIM, slots), jnp.bfloat16)] * 4
            + [pltpu.VMEM((slots, 128), jnp.bfloat16)] * 2
            + [
                pltpu.VMEM((three, slots), jnp.float32),
                pltpu.VMEM((128, BLK), jnp.bfloat16),
                pltpu.VMEM((128, BLK), jnp.bfloat16),
                pltpu.VMEM((1, BLK), jnp.float32),
            ],
        ),
        out_shape=[jax.ShapeDtypeStruct((three, span), jnp.bfloat16)] * parts
        + [jax.ShapeDtypeStruct((three, slots), jnp.bfloat16)],
        compiler_params=pltpu.CompilerParams(vmem_limit_bytes=40 << 20),
        cost_estimate=pl.CostEstimate(flops=40_000_000_000, bytes_accessed=6_000_000, transcendentals=0),
        name="attend_backward",
    )(table, *packed_list, *packed_list, *packed_list, *grad_list, exact, logs)


def layer_norm(values, gain):
    centre = jnp.mean(values, axis=-1, keepdims=True)
    centred = values - centre
    spread = jnp.mean(centred * centred, axis=-1, keepdims=True)
    return centred * lax.rsqrt(spread + 1e-05) * gain


def gelu_tanh(values):
    return jax.nn.gelu(values, approximate=True)


def product(equation, left, right):
    return jnp.einsum(equation, left, right, preferred_element_type=jnp.float32)


def shift(array, ctx, by):
    if by % ctx == 0:
        return array
    return lax.ppermute(array, "ctx", [(i, (i + by) % ctx) for i in range(ctx)])


def turned(array, axis, by):
    return lax.dynamic_slice_in_dim(
        jnp.concatenate([array, array], axis=axis), by, array.shape[axis], axis
    )


def gather_rows(array):
    return lax.all_gather(array, "fsdp", axis=0, tiled=True)


def scatter_rows(array):
    return lax.psum_scatter(
        array.astype(jnp.bfloat16), "fsdp", scatter_dimension=0, tiled=True
    )


def scatter_pairs(array, fsdp):
    me = lax.axis_index("fsdp")
    core, chip = me % 2, me // 2
    parts = array.reshape(fsdp // 2, 2, array.shape[0] // fsdp, array.shape[1])
    kept = lax.dynamic_index_in_dim(parts, core, 1, keepdims=False)
    sent = lax.dynamic_index_in_dim(parts, 1 - core, 1, keepdims=False).astype(jnp.bfloat16)
    got = lax.ppermute(sent, "fsdp", [(i, i ^ 1) for i in range(fsdp)])
    kept = kept.astype(jnp.float32) + got.astype(jnp.float32)
    total = lax.dynamic_index_in_dim(kept, chip, 0, keepdims=False)
    narrow = kept.astype(jnp.bfloat16)
    for other in range(1, fsdp // 2):
        sent = lax.dynamic_index_in_dim(narrow, chip ^ other, 0, keepdims=False)
        got = lax.ppermute(sent, "fsdp", [(i, i ^ (2 * other)) for i in range(fsdp)])
        total += got.astype(jnp.float32)
    return total


def per_device(
    ctx, fsdp, tokens_in, out_grad, gain_attn, gain_mlp, w_qkv, w_out, w_up, w_down, lengths, block_order
):
    local_rows, width = tokens_in.shape[1:]
    tokens_in, out_grad, length, block_order = tokens_in[0], out_grad[0], lengths[0], block_order[0]
    ctx_index = lax.axis_index("ctx")
    heads_here = width // HEAD_DIM // ctx
    own = heads_here * HEAD_DIM
    table = make_table(block_order, length, ctx_index, ctx)

    gains = jnp.stack([gain_attn, gain_mlp], axis=1)
    gains = jnp.pad(gains, ((0, 0), (0, 126)))
    first = gather_rows(jnp.concatenate([w_qkv, gains], axis=1))
    gain_one = first[:, 3 * width].astype(jnp.float32)
    gain_two = first[:, 3 * width + 1].astype(jnp.float32)
    w_out_all = gather_rows(w_out)
    w_up_all = gather_rows(w_up)
    w_down_all = gather_rows(w_down)
    w_own = jnp.concatenate(
        [
            lax.dynamic_slice_in_dim(first, kind * width + ctx_index * own, own, 1)
            for kind in range(3)
        ],
        axis=1,
    )
    w_out_turned = turned(w_out_all.reshape(ctx, heads_here, HEAD_DIM, width), 0, ctx_index)
    w_out_turned = w_out_turned.transpose(1, 0, 2, 3).reshape(width, width)
    w_turned = turned(first[:, : 3 * width].reshape(width, 3, ctx, heads_here, HEAD_DIM), 2, ctx_index)
    w_turned = w_turned.transpose(0, 3, 2, 1, 4).reshape(width, 3 * width)

    here = local_rows // BLK
    places = lax.dynamic_slice_in_dim(block_order, ctx_index * here, here)
    places = (places[:, None] * BLK + jnp.arange(BLK, dtype=jnp.int32)[None]).reshape(-1)
    grad_z = out_grad * (places < length).astype(jnp.bfloat16)[:, None]

    normed_list, packed_list = [], []
    tokens = tokens_in
    for part in range(ctx):
        normed = layer_norm(tokens.astype(jnp.float32), gain_one).astype(jnp.bfloat16)
        normed_list.append(normed)
        packed_list.append(product("jn,uj->nu", w_own, normed).astype(jnp.bfloat16))
        if part == ctx - 2:
            tokens, w_out_turned, w_turned, grad_z = lax.optimization_barrier(
                (tokens, w_out_turned, w_turned, grad_z)
            )
        if part < ctx - 1:
            tokens = shift(tokens, ctx, 1)
    kept, mixed_parts = [], []
    for head in range(heads_here):
        results = attend_forward(table, head, heads_here, packed_list)
        kept.append((results[ctx], results[ctx + 1]))
        mixed_parts += [shift(results[part], ctx, -part) for part in range(ctx)]
    mixed_t = jnp.concatenate(mixed_parts, axis=0)

    tokens_f = tokens_in.astype(jnp.float32)
    middle = tokens_f + product("nu,nj->uj", mixed_t, w_out_turned)
    normed_two, norm_two_back = jax.vjp(lambda v: layer_norm(v, gain_two), middle)
    normed_two = normed_two.astype(jnp.bfloat16)
    pre_act = product("uj,jn->un", normed_two, w_up_all)
    activation, gelu_back = jax.vjp(gelu_tanh, pre_act)
    activation = activation.astype(jnp.bfloat16)
    result = (middle + product("un,nj->uj", activation, w_down_all)).astype(jnp.bfloat16)

    grad_act = product("uj,nj->un", grad_z, w_down_all)
    grad_pre = gelu_back(grad_act)[0].astype(jnp.bfloat16)
    grad_normed_two = product("un,jn->uj", grad_pre, w_up_all)
    grad_middle = grad_z.astype(jnp.float32) + norm_two_back(grad_normed_two)[0]
    grad_branch = grad_middle.astype(jnp.bfloat16)
    grad_mixed_t = product("nj,uj->nu", w_out_turned, grad_branch).astype(jnp.bfloat16)
    grads_by_head = []
    for head in range(heads_here):
        pieces = []
        for part in range(ctx):
            row = (head * ctx + part) * HEAD_DIM
            piece = grad_mixed_t[row : row + HEAD_DIM]
            pieces.append(shift(piece, ctx, part))
        grads_by_head.append(pieces)

    grad_w_down = product("un,uj->nj", activation, grad_z).astype(jnp.bfloat16)
    grad_w_up = product("uj,un->jn", normed_two, grad_pre).astype(jnp.bfloat16)
    grad_w_out = product("nu,uj->nj", mixed_t, grad_branch).astype(jnp.bfloat16)
    grad_w_out = turned(
        grad_w_out.reshape(heads_here, ctx, HEAD_DIM, width).transpose(1, 0, 2, 3), 0, (ctx - ctx_index) % ctx
    )
    grad_w_down = scatter_rows(grad_w_down)
    grad_up_out = scatter_rows(
        jnp.concatenate([grad_w_up, grad_w_out.reshape(width, width)], axis=1)
    )

    grad_parts, grad_whole = [], []
    for head in range(heads_here):
        if head == heads_here - 1:
            grad_up_out, grad_w_down, table = lax.optimization_barrier(
                (grad_up_out, grad_w_down, table)
            )
            grad_up_out, grad_w_down = lax.psum((grad_up_out, grad_w_down), "ctx")
        results = attend_backward(
            table, head, heads_here, packed_list, grads_by_head[head], *kept[head]
        )
        grad_parts += [shift(results[part], ctx, -part) for part in range(ctx)]
        grad_whole.append(results[ctx])
    normed_all = jnp.concatenate(normed_list, axis=0)
    grad_qkv_own = product("uj,nu->jn", normed_all, jnp.concatenate(grad_whole, axis=0))
    grad_qkv_own = scatter_pairs(grad_qkv_own, fsdp).astype(jnp.bfloat16)
    grad_qkv = lax.all_gather(grad_qkv_own, "ctx", axis=0)
    rows_here = grad_qkv.shape[1]
    grad_qkv = grad_qkv.reshape(ctx, rows_here, heads_here, 3, HEAD_DIM)
    grad_w_qkv = grad_qkv.transpose(1, 3, 0, 2, 4).reshape(rows_here, 3 * width).astype(jnp.float32)

    grad_packed_t = jnp.concatenate(grad_parts, axis=0)
    grad_normed_one = product("nu,jn->uj", grad_packed_t, w_turned)
    norm_one_back = jax.vjp(lambda v: layer_norm(v, gain_one), tokens_f)[1]
    grad_tokens = (grad_middle + norm_one_back(grad_normed_one)[0]).astype(jnp.bfloat16)

    grad_w_down = grad_w_down.astype(jnp.float32)
    grad_w_up = grad_up_out[:, : w_up.shape[1]].astype(jnp.float32)
    grad_w_out = grad_up_out[:, w_up.shape[1] :].astype(jnp.float32)

    def gain_grad(grad_weight, weight, gain):
        total = jnp.sum(grad_weight * weight.astype(jnp.float32), axis=1)
        return total / gain.astype(jnp.float32)

    return (
        result[None],
        grad_tokens[None],
        gain_grad(grad_w_qkv, w_qkv, gain_attn),
        gain_grad(grad_w_up, w_up, gain_mlp),
        grad_w_qkv,
        grad_w_out,
        grad_w_up,
        grad_w_down,
    )


def solution(mesh):
    rows = P("fsdp", None)
    whole = P("fsdp", "ctx", None)
    ctx, fsdp = mesh.shape["ctx"], mesh.shape["fsdp"]

    def layer(*arrays):
        return per_device(ctx, fsdp, *arrays)

    return jax.shard_map(
        layer,
        mesh=mesh,
        in_specs=(whole, whole, P("fsdp"), P("fsdp"), rows, rows, rows, rows, P("fsdp"), rows),
        out_specs=(whole, whole, P("fsdp"), P("fsdp"), rows, rows, rows, rows),
        check_vma=False,
    )
```

```python
import functools

import jax
import jax.numpy as jnp
from jax import lax
from jax.experimental import pallas as pl
from jax.experimental.pallas import tpu as pltpu
from jax.sharding import PartitionSpec as P


HEAD_DIM = 64
BLK = 512
HALF = 256
LOG2E = 1.4426950408889634
BIG = 3e38
LOW = -1e30


def nn(left, right):
    return lax.dot_general(left, right, (((1,), (0,)), ((), ())), preferred_element_type=jnp.float32)


def nt(left, right):
    return lax.dot_general(left, right, (((1,), (1,)), ((), ())), preferred_element_type=jnp.float32)


def sign_of(scores):
    return jnp.tanh(scores.astype(jnp.bfloat16) * jnp.bfloat16(BIG))


def block_mask(key_start, query_start, length, shape):
    keys = key_start + lax.broadcasted_iota(jnp.int32, shape, 0)
    queries = query_start + lax.broadcasted_iota(jnp.int32, shape, 1)
    return keys <= jnp.minimum(queries, length - 1)


def gather_columns(refs, out):
    span = refs[0].shape[1]
    for part, ref in enumerate(refs):
        out[:, part * span : (part + 1) * span] = ref[...]


def turn_rows(source, out, twice):
    for part in range(source.shape[1] // BLK):
        span = slice(part * BLK, (part + 1) * BLK)
        piece = source[:, span]
        out[span, :] = jnp.concatenate([piece, piece if twice else jnp.zeros_like(piece)], axis=0).T


def query_weights(query_t):
    scaled = query_t.astype(jnp.float32) * (LOG2E * HEAD_DIM ** -0.5)
    high = scaled.astype(jnp.bfloat16)
    return jnp.concatenate([high, (scaled - high.astype(jnp.float32)).astype(jnp.bfloat16)], axis=0)


def pair_step(table, index, masked, weights, keys, values, top_ref, total_ref, mixed_ref):
    blocks = keys.shape[0] // BLK
    code = table[3 + blocks + index]
    query_block, key_block = code // blocks, code % blocks
    key_span = pl.ds(pl.multiple_of(key_block * BLK, BLK), BLK)
    key_rows, value_rows = keys[key_span, :], values[:, key_span]
    spans = [
        pl.ds(pl.multiple_of(query_block * BLK + half * HALF, HALF), HALF) for half in range(2)
    ]
    scores_list = [nn(key_rows, weights[:, span]) for span in spans]
    for half in range(2):
        span, scores = spans[half], scores_list[half]
        top = top_ref[:, span]
        size = jnp.abs(scores)
        if masked:
            key_start = table[3 + key_block] * BLK
            query_start = table[3 + query_block] * BLK + half * HALF
            size = jnp.where(block_mask(key_start, query_start, table[2], size.shape), size, LOW)
        new_top = jnp.maximum(top, jnp.max(size, axis=0, keepdims=True))
        fade = jnp.exp2(top - new_top)
        powers = jnp.exp2(size - new_top)
        signed = powers.astype(jnp.bfloat16) * sign_of(scores)
        top_ref[:, span] = new_top
        total_ref[:, span] = total_ref[:, span] * fade + jnp.sum(powers, axis=0, keepdims=True)
        mixed_ref[:, span] = mixed_ref[:, span] * fade + nn(value_rows, signed)


def run_pairs(table, *refs):
    @pl.loop(0, table[0])
    def _(index):
        pair_step(table, index, False, *refs)

    @pl.loop(table[0], table[1])
    def _(index):
        pair_step(table, index, True, *refs)


def load_head_part(part, query_ref, key_ref, value_ref, weights, keys, values):
    width = query_ref.shape[1]
    span = slice(part * width, (part + 1) * width)
    weights[:, span] = query_weights(query_ref[...])
    key_rows = key_ref[...]
    for start in range(0, width, BLK):
        piece = key_rows[:, start : start + BLK]
        rows = slice(part * width + start, part * width + start + BLK)
        keys[rows, :] = jnp.concatenate([piece, piece], axis=0).T
    values[:, span] = value_ref[...]


def early_kernel(parts, heads, first, table, *refs):
    packed_refs, refs = refs[:parts], refs[parts:]
    if not first:
        before, refs = refs[:3], refs[3:]
    top_ref, total_ref, mixed_ref, weights, keys, values = refs

    @pl.loop(0, heads)
    def _(head):
        def rows_of(kind):
            return pl.ds(pl.multiple_of((kind * heads + head) * HEAD_DIM, HEAD_DIM), HEAD_DIM)

        for part, ref in enumerate(packed_refs):
            three = [ref.at[rows_of(kind), :] for kind in range(3)]
            load_head_part(part, *three, weights, keys, values)
        state = (top_ref.at[head], total_ref.at[head], mixed_ref.at[head])
        if first:
            for ref, value in zip(state, (LOW, 0.0, 0.0)):
                ref[...] = jnp.full(ref.shape, value, jnp.float32)
        else:
            for ref, old in zip(state, before):
                ref[...] = old[head]
        run_pairs(table, weights, keys, values, *state)


def last_kernel(parts, table, *refs):
    query_refs, key_refs, value_refs = refs[:parts], refs[parts : 2 * parts], refs[2 * parts : 3 * parts]
    before, refs = refs[3 * parts : 3 * parts + 3], refs[3 * parts + 3 :]
    sends, refs = refs[:parts], refs[parts:]
    exact_ref, log_ref, weights, keys, values, top_ref, total_ref = refs
    for part in range(parts):
        load_head_part(part, query_refs[part], key_refs[part], value_refs[part], weights, keys, values)
    top_ref[...] = before[0][0]
    total_ref[...] = before[1][0]
    exact_ref[...] = before[2][0]
    run_pairs(table, weights, keys, values, top_ref, total_ref, exact_ref)
    log_ref[...] = top_ref[...] + jnp.log2(total_ref[...])
    width = sends[0].shape[1]
    for part in range(parts):
        span = slice(part * width, (part + 1) * width)
        done = exact_ref[:, span] / total_ref[:, span]
        exact_ref[:, span] = done
        sends[part][...] = done.astype(jnp.bfloat16)


def backward_kernel(parts, table, *refs):
    query_refs, key_refs, value_refs = refs[:parts], refs[parts : 2 * parts], refs[2 * parts : 3 * parts]
    grad_refs, refs = refs[3 * parts : 4 * parts], refs[4 * parts :]
    exact_ref, log_ref, sends, refs = refs[0], refs[1], refs[2 : 2 + parts], refs[2 + parts :]
    whole_ref, queries, keys_t, values_t, grads, keys, values, sums, weights, grad_weights, dots = refs
    blocks = queries.shape[1] // BLK
    length = table[blocks]
    scale = HEAD_DIM ** -0.5
    gather_columns(query_refs, queries)
    gather_columns(key_refs, keys_t)
    gather_columns(value_refs, values_t)
    gather_columns(grad_refs, grads)
    turn_rows(keys_t, keys, True)
    turn_rows(values_t, values, False)
    sums[...] = jnp.zeros_like(sums)
    grad_weights[...] = jnp.zeros_like(grad_weights)
    full = (length + BLK - 1) // BLK

    @pl.loop(0, full)
    def _(place):
        span = pl.ds(pl.multiple_of(table[place] * BLK, BLK), BLK)
        weights[...] = query_weights(queries[:, span])
        grad_t = grads[:, span]
        grad_weights[:HEAD_DIM, :] = grad_t
        dots[...] = jnp.sum(grad_t.astype(jnp.float32) * exact_ref[:, span], axis=0, keepdims=True)

        def step(number, masked):
            key_span = pl.ds(pl.multiple_of(table[number] * BLK, BLK), BLK)
            key_rows, value_rows = keys[key_span, :], values[key_span, :]
            halves = [slice(h * HALF, (h + 1) * HALF) for h in range(2)]
            scores_list = [nn(key_rows, weights[:, h]) for h in halves]
            inner_list = [nn(value_rows, grad_weights[:, h]) for h in halves]
            signed_list, score_grads_list = [], []
            for half in range(2):
                scores = scores_list[half]
                log_row = log_ref[:, pl.ds(pl.multiple_of(table[place] * BLK + half * HALF, HALF), HALF)]
                size = jnp.abs(scores) - log_row
                if masked:
                    mask = block_mask(number * BLK, place * BLK + half * HALF, length, size.shape)
                    size = jnp.where(mask, size, LOW)
                positive = jnp.exp2(size).astype(jnp.bfloat16)
                sign = sign_of(scores)
                signed_list.append(positive * sign)
                inner = inner_list[half] - dots[:, halves[half]] * sign.astype(jnp.float32)
                score_grads_list.append((positive.astype(jnp.float32) * inner).astype(jnp.bfloat16))
            signed = jnp.concatenate(signed_list, axis=1)
            score_grads = jnp.concatenate(score_grads_list, axis=1)
            sums[0:64, span] += nn(keys_t[:, key_span], score_grads)
            sums[64:128, key_span] += nt(queries[:, span], score_grads)
            sums[128:192, key_span] += nt(grads[:, span], signed)

        @pl.loop(0, place)
        def _(number):
            step(number, False)

        step(place, True)

    width = sends[0].shape[1]
    for part in range(parts):
        span = slice(part * width, (part + 1) * width)
        for rows, factor in ((slice(0, 128), scale), (slice(128, 192), 1.0)):
            done = (sums[rows, span] * factor).astype(jnp.bfloat16)
            whole_ref[rows, span] = done
            sends[part][rows, :] = done


def make_table(block_order, length, ctx_index, ctx):
    here = block_order.shape[0] // ctx
    order = (ctx_index - jnp.arange(ctx)) % ctx
    places = block_order.reshape(ctx, here)[order].reshape(-1)
    return jnp.concatenate([jnp.argsort(places).astype(jnp.int32), length[None]])


def head_specs(parts, span, row):
    return [pl.BlockSpec((HEAD_DIM, span), lambda i, t, row=row: (row, 0)) for _ in range(parts)]


def pair_tables(block_order, length, ctx_index, ctx):
    here = block_order.shape[0] // ctx
    order = (ctx_index - jnp.arange(ctx)) % ctx
    places = block_order.reshape(ctx, here)[order].reshape(-1)
    blocks = places.shape[0]
    part = jnp.arange(blocks) // here
    query, key = places[:, None], places[None, :]
    seen = ((key <= query) & (key * BLK < length)).reshape(-1)
    masked = ((key == query) | ((key + 1) * BLK > length)).reshape(-1)
    newest = jnp.maximum(part[:, None], part[None, :]).reshape(-1)
    phase = jnp.maximum(newest, 1)
    pairs = jnp.arange(blocks * blocks, dtype=jnp.int32)
    tables = []
    for number in range(1, ctx):
        mine = seen & (phase == number)
        plain = mine & ~masked
        rank = jnp.where(plain, 0, jnp.where(mine, 1, 2)) * pairs.shape[0] + pairs
        slot = jnp.sum((rank[None, :] < rank[:, None]).astype(jnp.int32), axis=1)
        codes = jnp.sum(jnp.where(slot[:, None] == pairs[None, :], pairs[:, None], 0), axis=0)
        counts = jnp.stack([jnp.sum(plain.astype(jnp.int32)), jnp.sum(mine.astype(jnp.int32)), length])
        tables.append(jnp.concatenate([counts, places, codes]).astype(jnp.int32))
    return tables


def attend_early(table, heads, ctx, packed_list, state):
    parts, span = len(packed_list), packed_list[0].shape[1]
    slots = ctx * span
    shapes = [(heads, 1, slots), (heads, 1, slots), (heads, HEAD_DIM, slots)]
    whole = lambda shape: pl.BlockSpec(shape, lambda i, t: (0,) * len(shape))
    return pl.pallas_call(
        functools.partial(early_kernel, parts, heads, state is None),
        grid_spec=pltpu.PrefetchScalarGridSpec(
            num_scalar_prefetch=1,
            grid=(1,),
            in_specs=[whole(packed_list[0].shape)] * parts
            + ([] if state is None else [whole(shape) for shape in shapes]),
            out_specs=[whole(shape) for shape in shapes],
            scratch_shapes=[
                pltpu.VMEM((128, slots), jnp.bfloat16),
                pltpu.VMEM((slots, 128), jnp.bfloat16),
                pltpu.VMEM((HEAD_DIM, slots), jnp.bfloat16),
            ],
        ),
        out_shape=[jax.ShapeDtypeStruct(shape, jnp.float32) for shape in shapes],
        compiler_params=pltpu.CompilerParams(vmem_limit_bytes=48 << 20),
        cost_estimate=pl.CostEstimate(flops=20_000_000_000, bytes_accessed=4_000_000, transcendentals=0),
        name="attend_early",
    )(table, *packed_list, *([] if state is None else state))


def attend_last(table, head, heads, packed_list, state):
    parts, span = len(packed_list), packed_list[0].shape[1]
    slots = parts * span
    whole = lambda shape: pl.BlockSpec(shape, lambda i, t: (0,) * len(shape))
    piece = lambda rows: pl.BlockSpec((1, rows, slots), lambda i, t: (head, 0, 0))
    return pl.pallas_call(
        functools.partial(last_kernel, parts),
        grid_spec=pltpu.PrefetchScalarGridSpec(
            num_scalar_prefetch=1,
            grid=(1,),
            in_specs=head_specs(parts, span, head)
            + head_specs(parts, span, heads + head)
            + head_specs(parts, span, 2 * heads + head)
            + [piece(1), piece(1), piece(HEAD_DIM)],
            out_specs=[whole((HEAD_DIM, span))] * parts + [whole((HEAD_DIM, slots)), whole((1, slots))],
            scratch_shapes=[
                pltpu.VMEM((128, slots), jnp.bfloat16),
                pltpu.VMEM((slots, 128), jnp.bfloat16),
                pltpu.VMEM((HEAD_DIM, slots), jnp.bfloat16),
                pltpu.VMEM((1, slots), jnp.float32),
                pltpu.VMEM((1, slots), jnp.float32),
            ],
        ),
        out_shape=[jax.ShapeDtypeStruct((HEAD_DIM, span), jnp.bfloat16)] * parts
        + [
            jax.ShapeDtypeStruct((HEAD_DIM, slots), jnp.float32),
            jax.ShapeDtypeStruct((1, slots), jnp.float32),
        ],
        compiler_params=pltpu.CompilerParams(vmem_limit_bytes=40 << 20),
        cost_estimate=pl.CostEstimate(flops=10_000_000_000, bytes_accessed=4_000_000, transcendentals=0),
        name="attend_last",
    )(table, *packed_list, *packed_list, *packed_list, *state)


def attend_backward(table, head, heads, packed_list, grad_list, exact, logs):
    parts, span = len(packed_list), packed_list[0].shape[1]
    slots = parts * span
    whole = lambda shape: pl.BlockSpec(shape, lambda i, t: (0, 0))
    three = 3 * HEAD_DIM
    return pl.pallas_call(
        functools.partial(backward_kernel, parts),
        grid_spec=pltpu.PrefetchScalarGridSpec(
            num_scalar_prefetch=1,
            grid=(1,),
            in_specs=head_specs(parts, span, head)
            + head_specs(parts, span, heads + head)
            + head_specs(parts, span, 2 * heads + head)
            + [whole((HEAD_DIM, span))] * parts
            + [whole((HEAD_DIM, slots)), whole((1, slots))],
            out_specs=[whole((three, span))] * parts + [whole((three, slots))],
            scratch_shapes=[pltpu.VMEM((HEAD_DIM, slots), jnp.bfloat16)] * 4
            + [pltpu.VMEM((slots, 128), jnp.bfloat16)] * 2
            + [
                pltpu.VMEM((three, slots), jnp.float32),
                pltpu.VMEM((128, BLK), jnp.bfloat16),
                pltpu.VMEM((128, BLK), jnp.bfloat16),
                pltpu.VMEM((1, BLK), jnp.float32),
            ],
        ),
        out_shape=[jax.ShapeDtypeStruct((three, span), jnp.bfloat16)] * parts
        + [jax.ShapeDtypeStruct((three, slots), jnp.bfloat16)],
        compiler_params=pltpu.CompilerParams(vmem_limit_bytes=40 << 20),
        cost_estimate=pl.CostEstimate(flops=40_000_000_000, bytes_accessed=6_000_000, transcendentals=0),
        name="attend_backward",
    )(table, *packed_list, *packed_list, *packed_list, *grad_list, exact, logs)


def layer_norm(values, gain):
    centre = jnp.mean(values, axis=-1, keepdims=True)
    centred = values - centre
    spread = jnp.mean(centred * centred, axis=-1, keepdims=True)
    return centred * lax.rsqrt(spread + 1e-05) * gain


def gelu_tanh(values):
    return jax.nn.gelu(values, approximate=True)


def product(equation, left, right):
    return jnp.einsum(equation, left, right, preferred_element_type=jnp.float32)


def shift(array, ctx, by):
    if by % ctx == 0:
        return array
    return lax.ppermute(array, "ctx", [(i, (i + by) % ctx) for i in range(ctx)])


def turned(array, axis, by):
    return lax.dynamic_slice_in_dim(
        jnp.concatenate([array, array], axis=axis), by, array.shape[axis], axis
    )


def gather_rows(array):
    return lax.all_gather(array, "fsdp", axis=0, tiled=True)


def scatter_rows(array):
    return lax.psum_scatter(
        array.astype(jnp.bfloat16), "fsdp", scatter_dimension=0, tiled=True
    )


def scatter_pairs(array, fsdp):
    me = lax.axis_index("fsdp")
    core, chip = me % 2, me // 2
    parts = array.reshape(fsdp // 2, 2, array.shape[0] // fsdp, array.shape[1])
    kept = lax.dynamic_index_in_dim(parts, core, 1, keepdims=False)
    sent = lax.dynamic_index_in_dim(parts, 1 - core, 1, keepdims=False).astype(jnp.bfloat16)
    got = lax.ppermute(sent, "fsdp", [(i, i ^ 1) for i in range(fsdp)])
    kept = kept.astype(jnp.float32) + got.astype(jnp.float32)
    total = lax.dynamic_index_in_dim(kept, chip, 0, keepdims=False)
    narrow = kept.astype(jnp.bfloat16)
    for other in range(1, fsdp // 2):
        sent = lax.dynamic_index_in_dim(narrow, chip ^ other, 0, keepdims=False)
        got = lax.ppermute(sent, "fsdp", [(i, i ^ (2 * other)) for i in range(fsdp)])
        total += got.astype(jnp.float32)
    return total


def per_device(
    ctx, fsdp, tokens_in, out_grad, gain_attn, gain_mlp, w_qkv, w_out, w_up, w_down, lengths, block_order
):
    local_rows, width = tokens_in.shape[1:]
    tokens_in, out_grad, length, block_order = tokens_in[0], out_grad[0], lengths[0], block_order[0]
    ctx_index = lax.axis_index("ctx")
    heads_here = width // HEAD_DIM // ctx
    own = heads_here * HEAD_DIM
    table = make_table(block_order, length, ctx_index, ctx)

    gains = jnp.stack([gain_attn, gain_mlp], axis=1)
    gains = jnp.pad(gains, ((0, 0), (0, 126)))
    first = gather_rows(jnp.concatenate([w_qkv, gains], axis=1))
    gain_one = first[:, 3 * width].astype(jnp.float32)
    gain_two = first[:, 3 * width + 1].astype(jnp.float32)
    w_out_all = gather_rows(w_out)
    w_up_all = gather_rows(w_up)
    w_down_all = gather_rows(w_down)

    def columns(by):
        device = (ctx_index + by) % ctx
        return [
            lax.dynamic_slice_in_dim(first, kind * width + device * own, own, 1)
            for kind in range(3)
        ]

    w_own = jnp.concatenate(columns(0), axis=1)
    w_out_turned = turned(w_out_all.reshape(ctx, heads_here, HEAD_DIM, width), 0, ctx_index)
    w_out_turned = w_out_turned.transpose(1, 0, 2, 3).reshape(width, width)
    w_turned = jnp.concatenate(sum([columns(by) for by in range(ctx)], []), axis=1)

    here = local_rows // BLK
    places = lax.dynamic_slice_in_dim(block_order, ctx_index * here, here)
    places = (places[:, None] * BLK + jnp.arange(BLK, dtype=jnp.int32)[None]).reshape(-1)
    grad_z = out_grad * (places < length).astype(jnp.bfloat16)[:, None]

    tables = pair_tables(block_order, length, ctx_index, ctx)
    normed_list, packed_list = [], []
    tokens, state = tokens_in, None
    for part in range(ctx):
        here_tokens, gain_here, state = lax.optimization_barrier((tokens, gain_one, state))
        normed = layer_norm(here_tokens.astype(jnp.float32), gain_here).astype(jnp.bfloat16)
        normed_list.append(normed)
        packed_list.append(product("jn,uj->nu", w_own, normed).astype(jnp.bfloat16))
        if 0 < part < ctx - 1:
            state = attend_early(tables[part - 1], heads_here, ctx, packed_list, state)
        if part == 1:
            tokens, grad_z, tables = lax.optimization_barrier((tokens, grad_z, tables))
        if part < ctx - 1:
            tokens = shift(tokens, ctx, 1)
    kept, mixed_parts = [], []
    for head in range(heads_here):
        results = attend_last(tables[-1], head, heads_here, packed_list, state)
        kept.append((results[ctx], results[ctx + 1]))
        mixed_parts += [shift(results[part], ctx, -part) for part in range(ctx)]
    mixed_t = jnp.concatenate(mixed_parts, axis=0)

    tokens_f = tokens_in.astype(jnp.float32)
    middle = tokens_f + product("nu,nj->uj", mixed_t, w_out_turned)
    normed_two, norm_two_back = jax.vjp(lambda v: layer_norm(v, gain_two), middle)
    normed_two = normed_two.astype(jnp.bfloat16)
    pre_act = product("uj,jn->un", normed_two, w_up_all)
    activation, gelu_back = jax.vjp(gelu_tanh, pre_act)
    activation = activation.astype(jnp.bfloat16)
    result = (middle + product("un,nj->uj", activation, w_down_all)).astype(jnp.bfloat16)

    grad_act = product("uj,nj->un", grad_z, w_down_all)
    grad_pre = gelu_back(grad_act)[0].astype(jnp.bfloat16)
    grad_normed_two = product("un,jn->uj", grad_pre, w_up_all)
    grad_middle = grad_z.astype(jnp.float32) + norm_two_back(grad_normed_two)[0]
    grad_branch = grad_middle.astype(jnp.bfloat16)
    grad_mixed_t = product("nj,uj->nu", w_out_turned, grad_branch).astype(jnp.bfloat16)
    grads_by_head = []
    for head in range(heads_here):
        pieces = []
        for part in range(ctx):
            row = (head * ctx + part) * HEAD_DIM
            piece = grad_mixed_t[row : row + HEAD_DIM]
            pieces.append(shift(piece, ctx, part))
        grads_by_head.append(pieces)

    grad_w_down = product("un,uj->nj", activation, grad_z).astype(jnp.bfloat16)
    grad_w_up = product("uj,un->jn", normed_two, grad_pre).astype(jnp.bfloat16)
    grad_w_out = product("nu,uj->nj", mixed_t, grad_branch).astype(jnp.bfloat16)
    grad_w_out = turned(
        grad_w_out.reshape(heads_here, ctx, HEAD_DIM, width).transpose(1, 0, 2, 3), 0, (ctx - ctx_index) % ctx
    )
    grad_w_down = scatter_rows(grad_w_down)
    grad_up_out = scatter_rows(
        jnp.concatenate([grad_w_up, grad_w_out.reshape(width, width)], axis=1)
    )

    grad_parts, grad_whole = [], []
    for head in range(heads_here):
        if head == heads_here - 1:
            grad_up_out, grad_w_down, table = lax.optimization_barrier(
                (grad_up_out, grad_w_down, table)
            )
            grad_up_out, grad_w_down = lax.psum((grad_up_out, grad_w_down), "ctx")
        results = attend_backward(
            table, head, heads_here, packed_list, grads_by_head[head], *kept[head]
        )
        grad_parts.append([shift(results[part], ctx, -part) for part in range(ctx)])
        grad_whole.append(results[ctx])
    normed_all = jnp.concatenate(normed_list, axis=0)
    grad_qkv_own = product("uj,nu->jn", normed_all, jnp.concatenate(grad_whole, axis=0))
    grad_qkv_own = scatter_pairs(grad_qkv_own, fsdp).astype(jnp.bfloat16)
    grad_qkv = lax.all_gather(grad_qkv_own, "ctx", axis=0)
    rows_here = grad_qkv.shape[1]
    grad_qkv = grad_qkv.reshape(ctx, rows_here, heads_here, 3, HEAD_DIM)
    grad_w_qkv = grad_qkv.transpose(1, 3, 0, 2, 4).reshape(rows_here, 3 * width).astype(jnp.float32)

    grad_packed_t = jnp.concatenate(
        [
            grad_parts[head][part][kind * HEAD_DIM : (kind + 1) * HEAD_DIM]
            for part in range(ctx)
            for kind in range(3)
            for head in range(heads_here)
        ],
        axis=0,
    )
    grad_normed_one = product("nu,jn->uj", grad_packed_t, w_turned)
    norm_one_back = jax.vjp(lambda v: layer_norm(v, gain_one), tokens_f)[1]
    grad_tokens = (grad_middle + norm_one_back(grad_normed_one)[0]).astype(jnp.bfloat16)

    grad_w_down = grad_w_down.astype(jnp.float32)
    grad_w_up = grad_up_out[:, : w_up.shape[1]].astype(jnp.float32)
    grad_w_out = grad_up_out[:, w_up.shape[1] :].astype(jnp.float32)

    def gain_grad(grad_weight, weight, gain):
        total = jnp.sum(grad_weight * weight.astype(jnp.float32), axis=1)
        return total / gain.astype(jnp.float32)

    return (
        result[None],
        grad_tokens[None],
        gain_grad(grad_w_qkv, w_qkv, gain_attn),
        gain_grad(grad_w_up, w_up, gain_mlp),
        grad_w_qkv,
        grad_w_out,
        grad_w_up,
        grad_w_down,
    )


def solution(mesh):
    rows = P("fsdp", None)
    whole = P("fsdp", "ctx", None)
    ctx, fsdp = mesh.shape["ctx"], mesh.shape["fsdp"]

    def layer(*arrays):
        return per_device(ctx, fsdp, *arrays)

    return jax.shard_map(
        layer,
        mesh=mesh,
        in_specs=(whole, whole, P("fsdp"), P("fsdp"), rows, rows, rows, rows, P("fsdp"), rows),
        out_specs=(whole, whole, P("fsdp"), P("fsdp"), rows, rows, rows, rows),
        check_vma=False,
    )
```

```python
import functools

import jax
import jax.numpy as jnp
from jax import lax
from jax.experimental import pallas as pl
from jax.experimental.pallas import tpu as pltpu
from jax.sharding import PartitionSpec as P


HEAD_DIM = 64
BLK = 512
HALF = 256
LOG2E = 1.4426950408889634
BIG = 3e38
LOW = -1e30


def nn(left, right):
    return lax.dot_general(left, right, (((1,), (0,)), ((), ())), preferred_element_type=jnp.float32)


def nt(left, right):
    return lax.dot_general(left, right, (((1,), (1,)), ((), ())), preferred_element_type=jnp.float32)


def sign_of(scores):
    return jnp.tanh(scores.astype(jnp.bfloat16) * jnp.bfloat16(BIG))


def block_mask(key_start, query_start, length, shape):
    keys = key_start + lax.broadcasted_iota(jnp.int32, shape, 0)
    queries = query_start + lax.broadcasted_iota(jnp.int32, shape, 1)
    return keys <= jnp.minimum(queries, length - 1)


def gather_columns(refs, out):
    span = refs[0].shape[1]
    for part, ref in enumerate(refs):
        out[:, part * span : (part + 1) * span] = ref[...]


def turn_rows(source, out, twice):
    for part in range(source.shape[1] // BLK):
        span = slice(part * BLK, (part + 1) * BLK)
        piece = source[:, span]
        out[span, :] = jnp.concatenate([piece, piece if twice else jnp.zeros_like(piece)], axis=0).T


def query_weights(query_t):
    scaled = query_t.astype(jnp.float32) * (LOG2E * HEAD_DIM ** -0.5)
    high = scaled.astype(jnp.bfloat16)
    return jnp.concatenate([high, (scaled - high.astype(jnp.float32)).astype(jnp.bfloat16)], axis=0)


def pair_step(table, index, masked, weights, keys, values, top_ref, total_ref, mixed_ref):
    blocks = keys.shape[0] // BLK
    code = table[3 + blocks + index]
    query_block, key_block = code // blocks, code % blocks
    key_span = pl.ds(pl.multiple_of(key_block * BLK, BLK), BLK)
    key_rows, value_rows = keys[key_span, :], values[:, key_span]
    spans = [
        pl.ds(pl.multiple_of(query_block * BLK + half * HALF, HALF), HALF) for half in range(2)
    ]
    scores_list = [nn(key_rows, weights[:, span]) for span in spans]
    for half in range(2):
        span, scores = spans[half], scores_list[half]
        top = top_ref[:, span]
        size = jnp.abs(scores)
        if masked:
            key_start = table[3 + key_block] * BLK
            query_start = table[3 + query_block] * BLK + half * HALF
            size = jnp.where(block_mask(key_start, query_start, table[2], size.shape), size, LOW)
        new_top = jnp.maximum(top, jnp.max(size, axis=0, keepdims=True))
        fade = jnp.exp2(top - new_top)
        powers = jnp.exp2(size - new_top)
        signed = powers.astype(jnp.bfloat16) * sign_of(scores)
        top_ref[:, span] = new_top
        total_ref[:, span] = total_ref[:, span] * fade + jnp.sum(powers, axis=0, keepdims=True)
        mixed_ref[:, span] = mixed_ref[:, span] * fade + nn(value_rows, signed)


def run_pairs(table, *refs):
    @pl.loop(0, table[0])
    def _(index):
        pair_step(table, index, False, *refs)

    @pl.loop(table[0], table[1])
    def _(index):
        pair_step(table, index, True, *refs)


def load_head_part(part, query_ref, key_ref, value_ref, weights, keys, values):
    width = query_ref.shape[1]
    span = slice(part * width, (part + 1) * width)
    weights[:, span] = query_weights(query_ref[...])
    key_rows = key_ref[...]
    for start in range(0, width, BLK):
        piece = key_rows[:, start : start + BLK]
        rows = slice(part * width + start, part * width + start + BLK)
        keys[rows, :] = jnp.concatenate([piece, piece], axis=0).T
    values[:, span] = value_ref[...]


def early_kernel(parts, heads, first, table, *refs):
    packed_refs, refs = refs[:parts], refs[parts:]
    if not first:
        before, refs = refs[:3], refs[3:]
    top_ref, total_ref, mixed_ref, weights, keys, values = refs

    @pl.loop(0, heads)
    def _(head):
        def rows_of(kind):
            return pl.ds(pl.multiple_of((3 * head + kind) * HEAD_DIM, HEAD_DIM), HEAD_DIM)

        for part, ref in enumerate(packed_refs):
            three = [ref.at[rows_of(kind), :] for kind in range(3)]
            load_head_part(part, *three, weights, keys, values)
        state = (top_ref.at[head], total_ref.at[head], mixed_ref.at[head])
        if first:
            for ref, value in zip(state, (LOW, 0.0, 0.0)):
                ref[...] = jnp.full(ref.shape, value, jnp.float32)
        else:
            for ref, old in zip(state, before):
                ref[...] = old[head]
        run_pairs(table, weights, keys, values, *state)


def last_kernel(parts, table, *refs):
    query_refs, key_refs, value_refs = refs[:parts], refs[parts : 2 * parts], refs[2 * parts : 3 * parts]
    before, refs = refs[3 * parts : 3 * parts + 3], refs[3 * parts + 3 :]
    sends, refs = refs[:parts], refs[parts:]
    exact_ref, log_ref, weights, keys, values, top_ref, total_ref = refs
    for part in range(parts):
        load_head_part(part, query_refs[part], key_refs[part], value_refs[part], weights, keys, values)
    top_ref[...] = before[0][0]
    total_ref[...] = before[1][0]
    exact_ref[...] = before[2][0]
    run_pairs(table, weights, keys, values, top_ref, total_ref, exact_ref)
    log_ref[...] = top_ref[...] + jnp.log2(total_ref[...])
    width = sends[0].shape[1]
    for part in range(parts):
        span = slice(part * width, (part + 1) * width)
        done = exact_ref[:, span] / total_ref[:, span]
        exact_ref[:, span] = done
        sends[part][...] = done.astype(jnp.bfloat16)


def backward_kernel(parts, table, *refs):
    query_refs, key_refs, value_refs = refs[:parts], refs[parts : 2 * parts], refs[2 * parts : 3 * parts]
    grad_refs, refs = refs[3 * parts : 4 * parts], refs[4 * parts :]
    exact_ref, log_ref, sends, refs = refs[0], refs[1], refs[2 : 2 + parts], refs[2 + parts :]
    whole_ref, queries, keys_t, values_t, grads, keys, values, sums, weights, grad_weights, dots = refs
    blocks = queries.shape[1] // BLK
    length = table[blocks]
    scale = HEAD_DIM ** -0.5
    gather_columns(query_refs, queries)
    gather_columns(key_refs, keys_t)
    gather_columns(value_refs, values_t)
    gather_columns(grad_refs, grads)
    turn_rows(keys_t, keys, True)
    turn_rows(values_t, values, False)
    sums[...] = jnp.zeros_like(sums)
    grad_weights[...] = jnp.zeros_like(grad_weights)
    full = (length + BLK - 1) // BLK

    @pl.loop(0, full)
    def _(place):
        span = pl.ds(pl.multiple_of(table[place] * BLK, BLK), BLK)
        weights[...] = query_weights(queries[:, span])
        grad_t = grads[:, span]
        grad_weights[:HEAD_DIM, :] = grad_t
        dots[...] = jnp.sum(grad_t.astype(jnp.float32) * exact_ref[:, span], axis=0, keepdims=True)

        def step(number, masked):
            key_span = pl.ds(pl.multiple_of(table[number] * BLK, BLK), BLK)
            key_rows, value_rows = keys[key_span, :], values[key_span, :]
            halves = [slice(h * HALF, (h + 1) * HALF) for h in range(2)]
            scores_list = [nn(key_rows, weights[:, h]) for h in halves]
            inner_list = [nn(value_rows, grad_weights[:, h]) for h in halves]
            signed_list, score_grads_list = [], []
            for half in range(2):
                scores = scores_list[half]
                log_row = log_ref[:, pl.ds(pl.multiple_of(table[place] * BLK + half * HALF, HALF), HALF)]
                size = jnp.abs(scores) - log_row
                if masked:
                    mask = block_mask(number * BLK, place * BLK + half * HALF, length, size.shape)
                    size = jnp.where(mask, size, LOW)
                positive = jnp.exp2(size).astype(jnp.bfloat16)
                sign = sign_of(scores)
                signed_list.append(positive * sign)
                inner = inner_list[half] - dots[:, halves[half]] * sign.astype(jnp.float32)
                score_grads_list.append((positive.astype(jnp.float32) * inner).astype(jnp.bfloat16))
            signed = jnp.concatenate(signed_list, axis=1)
            score_grads = jnp.concatenate(score_grads_list, axis=1)
            sums[0:64, span] += nn(keys_t[:, key_span], score_grads)
            sums[64:128, key_span] += nt(queries[:, span], score_grads)
            sums[128:192, key_span] += nt(grads[:, span], signed)

        @pl.loop(0, place)
        def _(number):
            step(number, False)

        step(place, True)

    width = sends[0].shape[1]
    for part in range(parts):
        span = slice(part * width, (part + 1) * width)
        for rows, factor in ((slice(0, 128), scale), (slice(128, 192), 1.0)):
            done = (sums[rows, span] * factor).astype(jnp.bfloat16)
            whole_ref[rows, span] = done
            sends[part][rows, :] = done


def make_table(block_order, length, ctx_index, ctx):
    here = block_order.shape[0] // ctx
    order = (ctx_index - jnp.arange(ctx)) % ctx
    places = block_order.reshape(ctx, here)[order].reshape(-1)
    return jnp.concatenate([jnp.argsort(places).astype(jnp.int32), length[None]])


def head_specs(parts, span, row):
    return [pl.BlockSpec((HEAD_DIM, span), lambda i, t, row=row: (row, 0)) for _ in range(parts)]


def pair_tables(block_order, length, ctx_index, ctx):
    here = block_order.shape[0] // ctx
    order = (ctx_index - jnp.arange(ctx)) % ctx
    places = block_order.reshape(ctx, here)[order].reshape(-1)
    blocks = places.shape[0]
    part = jnp.arange(blocks) // here
    query, key = places[:, None], places[None, :]
    seen = ((key <= query) & (key * BLK < length)).reshape(-1)
    masked = ((key == query) | ((key + 1) * BLK > length)).reshape(-1)
    newest = jnp.maximum(part[:, None], part[None, :]).reshape(-1)
    phase = jnp.maximum(newest, 1)
    pairs = jnp.arange(blocks * blocks, dtype=jnp.int32)
    tables = []
    for number in range(1, ctx):
        mine = seen & (phase == number)
        plain = mine & ~masked
        rank = jnp.where(plain, 0, jnp.where(mine, 1, 2)) * pairs.shape[0] + pairs
        slot = jnp.sum((rank[None, :] < rank[:, None]).astype(jnp.int32), axis=1)
        codes = jnp.sum(jnp.where(slot[:, None] == pairs[None, :], pairs[:, None], 0), axis=0)
        counts = jnp.stack([jnp.sum(plain.astype(jnp.int32)), jnp.sum(mine.astype(jnp.int32)), length])
        tables.append(jnp.concatenate([counts, places, codes]).astype(jnp.int32))
    return tables


def attend_early(table, heads, ctx, packed_list, state):
    parts, span = len(packed_list), packed_list[0].shape[1]
    slots = ctx * span
    shapes = [(heads, 1, slots), (heads, 1, slots), (heads, HEAD_DIM, slots)]
    whole = lambda shape: pl.BlockSpec(shape, lambda i, t: (0,) * len(shape))
    return pl.pallas_call(
        functools.partial(early_kernel, parts, heads, state is None),
        grid_spec=pltpu.PrefetchScalarGridSpec(
            num_scalar_prefetch=1,
            grid=(1,),
            in_specs=[whole(packed_list[0].shape)] * parts
            + ([] if state is None else [whole(shape) for shape in shapes]),
            out_specs=[whole(shape) for shape in shapes],
            scratch_shapes=[
                pltpu.VMEM((128, slots), jnp.bfloat16),
                pltpu.VMEM((slots, 128), jnp.bfloat16),
                pltpu.VMEM((HEAD_DIM, slots), jnp.bfloat16),
            ],
        ),
        out_shape=[jax.ShapeDtypeStruct(shape, jnp.float32) for shape in shapes],
        compiler_params=pltpu.CompilerParams(vmem_limit_bytes=48 << 20),
        cost_estimate=pl.CostEstimate(flops=20_000_000_000, bytes_accessed=4_000_000, transcendentals=0),
        name="attend_early",
    )(table, *packed_list, *([] if state is None else state))


def attend_last(table, head, packed_list, state):
    parts, span = len(packed_list), packed_list[0].shape[1]
    slots = parts * span
    whole = lambda shape: pl.BlockSpec(shape, lambda i, t: (0,) * len(shape))
    piece = lambda rows: pl.BlockSpec((1, rows, slots), lambda i, t: (head, 0, 0))
    return pl.pallas_call(
        functools.partial(last_kernel, parts),
        grid_spec=pltpu.PrefetchScalarGridSpec(
            num_scalar_prefetch=1,
            grid=(1,),
            in_specs=head_specs(parts, span, 3 * head)
            + head_specs(parts, span, 3 * head + 1)
            + head_specs(parts, span, 3 * head + 2)
            + [piece(1), piece(1), piece(HEAD_DIM)],
            out_specs=[whole((HEAD_DIM, span))] * parts + [whole((HEAD_DIM, slots)), whole((1, slots))],
            scratch_shapes=[
                pltpu.VMEM((128, slots), jnp.bfloat16),
                pltpu.VMEM((slots, 128), jnp.bfloat16),
                pltpu.VMEM((HEAD_DIM, slots), jnp.bfloat16),
                pltpu.VMEM((1, slots), jnp.float32),
                pltpu.VMEM((1, slots), jnp.float32),
            ],
        ),
        out_shape=[jax.ShapeDtypeStruct((HEAD_DIM, span), jnp.bfloat16)] * parts
        + [
            jax.ShapeDtypeStruct((HEAD_DIM, slots), jnp.float32),
            jax.ShapeDtypeStruct((1, slots), jnp.float32),
        ],
        compiler_params=pltpu.CompilerParams(vmem_limit_bytes=40 << 20),
        cost_estimate=pl.CostEstimate(flops=10_000_000_000, bytes_accessed=4_000_000, transcendentals=0),
        name="attend_last",
    )(table, *packed_list, *packed_list, *packed_list, *state)


def attend_backward(table, head, packed_list, grad_list, exact, logs):
    parts, span = len(packed_list), packed_list[0].shape[1]
    slots = parts * span
    whole = lambda shape: pl.BlockSpec(shape, lambda i, t: (0, 0))
    three = 3 * HEAD_DIM
    return pl.pallas_call(
        functools.partial(backward_kernel, parts),
        grid_spec=pltpu.PrefetchScalarGridSpec(
            num_scalar_prefetch=1,
            grid=(1,),
            in_specs=head_specs(parts, span, 3 * head)
            + head_specs(parts, span, 3 * head + 1)
            + head_specs(parts, span, 3 * head + 2)
            + [whole((HEAD_DIM, span))] * parts
            + [whole((HEAD_DIM, slots)), whole((1, slots))],
            out_specs=[whole((three, span))] * parts + [whole((three, slots))],
            scratch_shapes=[pltpu.VMEM((HEAD_DIM, slots), jnp.bfloat16)] * 4
            + [pltpu.VMEM((slots, 128), jnp.bfloat16)] * 2
            + [
                pltpu.VMEM((three, slots), jnp.float32),
                pltpu.VMEM((128, BLK), jnp.bfloat16),
                pltpu.VMEM((128, BLK), jnp.bfloat16),
                pltpu.VMEM((1, BLK), jnp.float32),
            ],
        ),
        out_shape=[jax.ShapeDtypeStruct((three, span), jnp.bfloat16)] * parts
        + [jax.ShapeDtypeStruct((three, slots), jnp.bfloat16)],
        compiler_params=pltpu.CompilerParams(vmem_limit_bytes=40 << 20),
        cost_estimate=pl.CostEstimate(flops=40_000_000_000, bytes_accessed=6_000_000, transcendentals=0),
        name="attend_backward",
    )(table, *packed_list, *packed_list, *packed_list, *grad_list, exact, logs)


def layer_norm(values, gain):
    centre = jnp.mean(values, axis=-1, keepdims=True)
    centred = values - centre
    spread = jnp.mean(centred * centred, axis=-1, keepdims=True)
    return centred * lax.rsqrt(spread + 1e-05) * gain


def gelu_tanh(values):
    return jax.nn.gelu(values, approximate=True)


def product(equation, left, right):
    return jnp.einsum(equation, left, right, preferred_element_type=jnp.float32)


def shift(array, ctx, by):
    if by % ctx == 0:
        return array
    return lax.ppermute(array, "ctx", [(i, (i + by) % ctx) for i in range(ctx)])


def turned(array, axis, by):
    return lax.dynamic_slice_in_dim(
        jnp.concatenate([array, array], axis=axis), by, array.shape[axis], axis
    )


def gather_rows(array):
    return lax.all_gather(array, "fsdp", axis=0, tiled=True)


def scatter_rows(array):
    return lax.psum_scatter(
        array.astype(jnp.bfloat16), "fsdp", scatter_dimension=0, tiled=True
    )


def scatter_pairs(array, fsdp):
    me = lax.axis_index("fsdp")
    core, chip = me % 2, me // 2
    parts = array.reshape(fsdp // 2, 2, array.shape[0] // fsdp, array.shape[1])
    kept = lax.dynamic_index_in_dim(parts, core, 1, keepdims=False)
    sent = lax.dynamic_index_in_dim(parts, 1 - core, 1, keepdims=False).astype(jnp.bfloat16)
    got = lax.ppermute(sent, "fsdp", [(i, i ^ 1) for i in range(fsdp)])
    kept = kept.astype(jnp.float32) + got.astype(jnp.float32)
    total = lax.dynamic_index_in_dim(kept, chip, 0, keepdims=False)
    narrow = kept.astype(jnp.bfloat16)
    for other in range(1, fsdp // 2):
        sent = lax.dynamic_index_in_dim(narrow, chip ^ other, 0, keepdims=False)
        got = lax.ppermute(sent, "fsdp", [(i, i ^ (2 * other)) for i in range(fsdp)])
        total += got.astype(jnp.float32)
    return total


def per_device(
    ctx, fsdp, tokens_in, out_grad, gain_attn, gain_mlp, w_qkv, w_out, w_up, w_down, lengths, block_order
):
    local_rows, width = tokens_in.shape[1:]
    tokens_in, out_grad, length, block_order = tokens_in[0], out_grad[0], lengths[0], block_order[0]
    ctx_index = lax.axis_index("ctx")
    heads_here = width // HEAD_DIM // ctx
    own = heads_here * HEAD_DIM
    table = make_table(block_order, length, ctx_index, ctx)

    gains = jnp.stack([gain_attn, gain_mlp], axis=1)
    gains = jnp.pad(gains, ((0, 0), (0, 126)))
    ordered = w_qkv.reshape(-1, 3, ctx, heads_here, HEAD_DIM).transpose(0, 2, 3, 1, 4)
    ordered = turned(ordered.reshape(-1, ctx, 3 * own), 1, ctx_index).reshape(w_qkv.shape)
    first = gather_rows(jnp.concatenate([ordered, gains], axis=1))
    gain_one = first[:, 3 * width].astype(jnp.float32)
    gain_two = first[:, 3 * width + 1].astype(jnp.float32)
    w_out_all = gather_rows(w_out)
    w_up_all = gather_rows(w_up)
    w_down_all = gather_rows(w_down)
    w_own = first[:, : 3 * own]
    w_out_turned = turned(w_out_all.reshape(ctx, heads_here, HEAD_DIM, width), 0, ctx_index)
    w_out_turned = w_out_turned.transpose(1, 0, 2, 3).reshape(width, width)

    here = local_rows // BLK
    places = lax.dynamic_slice_in_dim(block_order, ctx_index * here, here)
    places = (places[:, None] * BLK + jnp.arange(BLK, dtype=jnp.int32)[None]).reshape(-1)
    grad_z = out_grad * (places < length).astype(jnp.bfloat16)[:, None]

    tables = pair_tables(block_order, length, ctx_index, ctx)
    normed_list, packed_list = [], []
    tokens, state = tokens_in, None
    for part in range(ctx):
        here_tokens, gain_here, state = lax.optimization_barrier((tokens, gain_one, state))
        normed = layer_norm(here_tokens.astype(jnp.float32), gain_here).astype(jnp.bfloat16)
        normed_list.append(normed)
        packed_list.append(product("jn,uj->nu", w_own, normed).astype(jnp.bfloat16))
        if 0 < part < ctx - 1:
            state = attend_early(tables[part - 1], heads_here, ctx, packed_list, state)
        if part == 1:
            tokens, grad_z, tables = lax.optimization_barrier((tokens, grad_z, tables))
        if part < ctx - 1:
            tokens = shift(tokens, ctx, 1)
    kept, mixed_parts = [], []
    for head in range(heads_here):
        results = attend_last(tables[-1], head, packed_list, state)
        kept.append((results[ctx], results[ctx + 1]))
        mixed_parts += [shift(results[part], ctx, -part) for part in range(ctx)]
    mixed_t = jnp.concatenate(mixed_parts, axis=0)

    tokens_f = tokens_in.astype(jnp.float32)
    middle = tokens_f + product("nu,nj->uj", mixed_t, w_out_turned)
    normed_two, norm_two_back = jax.vjp(lambda v: layer_norm(v, gain_two), middle)
    normed_two = normed_two.astype(jnp.bfloat16)
    pre_act = product("uj,jn->un", normed_two, w_up_all)
    activation, gelu_back = jax.vjp(gelu_tanh, pre_act)
    activation = activation.astype(jnp.bfloat16)
    result = (middle + product("un,nj->uj", activation, w_down_all)).astype(jnp.bfloat16)

    grad_act = product("uj,nj->un", grad_z, w_down_all)
    grad_pre = gelu_back(grad_act)[0].astype(jnp.bfloat16)
    grad_normed_two = product("un,jn->uj", grad_pre, w_up_all)
    grad_middle = grad_z.astype(jnp.float32) + norm_two_back(grad_normed_two)[0]
    grad_branch = grad_middle.astype(jnp.bfloat16)
    grad_mixed_t = product("nj,uj->nu", w_out_turned, grad_branch).astype(jnp.bfloat16)
    grads_by_head = []
    for head in range(heads_here):
        pieces = []
        for part in range(ctx):
            row = (head * ctx + part) * HEAD_DIM
            piece = grad_mixed_t[row : row + HEAD_DIM]
            pieces.append(shift(piece, ctx, part))
        grads_by_head.append(pieces)

    grad_w_down = product("un,uj->nj", activation, grad_z).astype(jnp.bfloat16)
    grad_w_up = product("uj,un->jn", normed_two, grad_pre).astype(jnp.bfloat16)
    grad_w_out = product("nu,uj->nj", mixed_t, grad_branch).astype(jnp.bfloat16)
    grad_w_out = turned(
        grad_w_out.reshape(heads_here, ctx, HEAD_DIM, width).transpose(1, 0, 2, 3), 0, (ctx - ctx_index) % ctx
    )
    grad_w_down = scatter_rows(grad_w_down)
    grad_up_out = scatter_rows(
        jnp.concatenate([grad_w_up, grad_w_out.reshape(width, width)], axis=1)
    )

    grad_parts, grad_whole = [], []
    for head in range(heads_here):
        if head == max(heads_here - 2, 0):
            grad_up_out, grad_w_down, table = lax.optimization_barrier(
                (grad_up_out, grad_w_down, table)
            )
            grad_up_out, grad_w_down = lax.psum((grad_up_out, grad_w_down), "ctx")
        results = attend_backward(table, head, packed_list, grads_by_head[head], *kept[head])
        grad_parts.append([shift(results[part], ctx, -part) for part in range(ctx)])
        grad_whole.append(results[ctx])
    normed_all = jnp.concatenate(normed_list, axis=0)
    grad_qkv_own = product("uj,nu->jn", normed_all, jnp.concatenate(grad_whole, axis=0))
    grad_qkv_own = scatter_pairs(grad_qkv_own, fsdp).astype(jnp.bfloat16)
    grad_qkv = lax.all_gather(grad_qkv_own, "ctx", axis=0)
    rows_here = grad_qkv.shape[1]
    grad_qkv = grad_qkv.reshape(ctx, rows_here, heads_here, 3, HEAD_DIM)
    grad_w_qkv = grad_qkv.transpose(1, 3, 0, 2, 4).reshape(rows_here, 3 * width).astype(jnp.float32)

    grad_packed_t = jnp.concatenate(
        [grad_parts[head][part] for part in range(ctx) for head in range(heads_here)], axis=0
    )
    grad_normed_one = product("nu,jn->uj", grad_packed_t, first[:, : 3 * width])
    norm_one_back = jax.vjp(lambda v: layer_norm(v, gain_one), tokens_f)[1]
    grad_tokens = (grad_middle + norm_one_back(grad_normed_one)[0]).astype(jnp.bfloat16)

    grad_w_down = grad_w_down.astype(jnp.float32)
    grad_w_up = grad_up_out[:, : w_up.shape[1]].astype(jnp.float32)
    grad_w_out = grad_up_out[:, w_up.shape[1] :].astype(jnp.float32)

    def gain_grad(grad_weight, weight, gain):
        total = jnp.sum(grad_weight * weight.astype(jnp.float32), axis=1)
        return total / gain.astype(jnp.float32)

    return (
        result[None],
        grad_tokens[None],
        gain_grad(grad_w_qkv, w_qkv, gain_attn),
        gain_grad(grad_w_up, w_up, gain_mlp),
        grad_w_qkv,
        grad_w_out,
        grad_w_up,
        grad_w_down,
    )


def solution(mesh):
    rows = P("fsdp", None)
    whole = P("fsdp", "ctx", None)
    ctx, fsdp = mesh.shape["ctx"], mesh.shape["fsdp"]

    def layer(*arrays):
        return per_device(ctx, fsdp, *arrays)

    return jax.shard_map(
        layer,
        mesh=mesh,
        in_specs=(whole, whole, P("fsdp"), P("fsdp"), rows, rows, rows, rows, P("fsdp"), rows),
        out_specs=(whole, whole, P("fsdp"), P("fsdp"), rows, rows, rows, rows),
        check_vma=False,
    )
```

```python
import functools

import jax
import jax.numpy as jnp
from jax import lax
from jax.experimental import pallas as pl
from jax.experimental.pallas import tpu as pltpu
from jax.sharding import PartitionSpec as P


HEAD_DIM = 64
BLK = 512
HALF = 256
LOG2E = 1.4426950408889634
BIG = 3e38
LOW = -1e30


def nn(left, right):
    return lax.dot_general(left, right, (((1,), (0,)), ((), ())), preferred_element_type=jnp.float32)


def nt(left, right):
    return lax.dot_general(left, right, (((1,), (1,)), ((), ())), preferred_element_type=jnp.float32)


def sign_of(scores):
    return jnp.clip(scores.astype(jnp.bfloat16) * jnp.bfloat16(BIG), -1.0, 1.0).astype(jnp.bfloat16)


def block_mask(key_start, query_start, length, shape):
    keys = key_start + lax.broadcasted_iota(jnp.int32, shape, 0)
    queries = query_start + lax.broadcasted_iota(jnp.int32, shape, 1)
    return keys <= jnp.minimum(queries, length - 1)


def gather_columns(refs, out):
    span = refs[0].shape[1]
    for part, ref in enumerate(refs):
        out[:, part * span : (part + 1) * span] = ref[...]


def turn_rows(source, out, twice):
    for part in range(source.shape[1] // BLK):
        span = slice(part * BLK, (part + 1) * BLK)
        piece = source[:, span]
        out[span, :] = jnp.concatenate([piece, piece if twice else jnp.zeros_like(piece)], axis=0).T


def query_weights(query_t):
    scaled = query_t.astype(jnp.float32) * (LOG2E * HEAD_DIM ** -0.5)
    high = scaled.astype(jnp.bfloat16)
    return jnp.concatenate([high, (scaled - high.astype(jnp.float32)).astype(jnp.bfloat16)], axis=0)


def pair_step(table, index, masked, weights, keys, values, top_ref, total_ref, mixed_ref):
    blocks = keys.shape[0] // BLK
    code = table[3 + blocks + index]
    query_block, key_block = code // blocks, code % blocks
    key_span = pl.ds(pl.multiple_of(key_block * BLK, BLK), BLK)
    key_rows, value_rows = keys[key_span, :], values[:, key_span]
    spans = [
        pl.ds(pl.multiple_of(query_block * BLK + half * HALF, HALF), HALF) for half in range(2)
    ]
    scores_list = [nn(key_rows, weights[:, span]) for span in spans]
    for half in range(2):
        span, scores = spans[half], scores_list[half]
        top = top_ref[:, span]
        size = jnp.abs(scores)
        if masked:
            key_start = table[3 + key_block] * BLK
            query_start = table[3 + query_block] * BLK + half * HALF
            size = jnp.where(block_mask(key_start, query_start, table[2], size.shape), size, LOW)
        new_top = jnp.maximum(top, jnp.max(size, axis=0, keepdims=True))
        fade = jnp.exp2(top - new_top)
        powers = jnp.exp2(size - new_top)
        signed = powers.astype(jnp.bfloat16) * sign_of(scores)
        top_ref[:, span] = new_top
        total_ref[:, span] = total_ref[:, span] * fade + jnp.sum(powers, axis=0, keepdims=True)
        mixed_ref[:, span] = mixed_ref[:, span] * fade + nn(value_rows, signed)


def run_pairs(table, *refs):
    @pl.loop(0, table[0])
    def _(index):
        pair_step(table, index, False, *refs)

    @pl.loop(table[0], table[1])
    def _(index):
        pair_step(table, index, True, *refs)


def load_head_part(part, query_ref, key_ref, value_ref, weights, keys, values):
    width = query_ref.shape[1]
    span = slice(part * width, (part + 1) * width)
    weights[:, span] = query_weights(query_ref[...])
    key_rows = key_ref[...]
    for start in range(0, width, BLK):
        piece = key_rows[:, start : start + BLK]
        rows = slice(part * width + start, part * width + start + BLK)
        keys[rows, :] = jnp.concatenate([piece, piece], axis=0).T
    values[:, span] = value_ref[...]


def early_kernel(parts, heads, first, table, *refs):
    packed_refs, refs = refs[:parts], refs[parts:]
    if not first:
        before, refs = refs[:3], refs[3:]
    top_ref, total_ref, mixed_ref, weights, keys, values = refs

    @pl.loop(0, heads)
    def _(head):
        def rows_of(kind):
            return pl.ds(pl.multiple_of((3 * head + kind) * HEAD_DIM, HEAD_DIM), HEAD_DIM)

        for part, ref in enumerate(packed_refs):
            three = [ref.at[rows_of(kind), :] for kind in range(3)]
            load_head_part(part, *three, weights, keys, values)
        state = (top_ref.at[head], total_ref.at[head], mixed_ref.at[head])
        if first:
            for ref, value in zip(state, (LOW, 0.0, 0.0)):
                ref[...] = jnp.full(ref.shape, value, jnp.float32)
        else:
            for ref, old in zip(state, before):
                ref[...] = old[head]
        run_pairs(table, weights, keys, values, *state)


def last_kernel(parts, table, *refs):
    query_refs, key_refs, value_refs = refs[:parts], refs[parts : 2 * parts], refs[2 * parts : 3 * parts]
    before, refs = refs[3 * parts : 3 * parts + 3], refs[3 * parts + 3 :]
    sends, refs = refs[:parts], refs[parts:]
    exact_ref, log_ref, weights, keys, values, top_ref, total_ref = refs
    for part in range(parts):
        load_head_part(part, query_refs[part], key_refs[part], value_refs[part], weights, keys, values)
    top_ref[...] = before[0][0]
    total_ref[...] = before[1][0]
    exact_ref[...] = before[2][0]
    run_pairs(table, weights, keys, values, top_ref, total_ref, exact_ref)
    log_ref[...] = top_ref[...] + jnp.log2(total_ref[...])
    width = sends[0].shape[1]
    for part in range(parts):
        span = slice(part * width, (part + 1) * width)
        done = exact_ref[:, span] / total_ref[:, span]
        exact_ref[:, span] = done
        sends[part][...] = done.astype(jnp.bfloat16)


def backward_kernel(parts, table, *refs):
    query_refs, key_refs, value_refs = refs[:parts], refs[parts : 2 * parts], refs[2 * parts : 3 * parts]
    grad_refs, refs = refs[3 * parts : 4 * parts], refs[4 * parts :]
    exact_ref, log_ref, sends, refs = refs[0], refs[1], refs[2 : 2 + parts], refs[2 + parts :]
    whole_ref, queries, keys_t, values_t, grads, keys, values, sums, weights, grad_weights, dots = refs
    blocks = queries.shape[1] // BLK
    length = table[blocks]
    scale = HEAD_DIM ** -0.5
    gather_columns(query_refs, queries)
    gather_columns(key_refs, keys_t)
    gather_columns(value_refs, values_t)
    gather_columns(grad_refs, grads)
    turn_rows(keys_t, keys, True)
    turn_rows(values_t, values, False)
    sums[...] = jnp.zeros_like(sums)
    grad_weights[...] = jnp.zeros_like(grad_weights)
    full = (length + BLK - 1) // BLK

    @pl.loop(0, full)
    def _(place):
        span = pl.ds(pl.multiple_of(table[place] * BLK, BLK), BLK)
        weights[...] = query_weights(queries[:, span])
        grad_t = grads[:, span]
        grad_weights[:HEAD_DIM, :] = grad_t
        dots[...] = jnp.sum(grad_t.astype(jnp.float32) * exact_ref[:, span], axis=0, keepdims=True)

        def step(number, masked):
            key_span = pl.ds(pl.multiple_of(table[number] * BLK, BLK), BLK)
            key_rows, value_rows = keys[key_span, :], values[key_span, :]
            halves = [slice(h * HALF, (h + 1) * HALF) for h in range(2)]
            scores_list = [nn(key_rows, weights[:, h]) for h in halves]
            inner_list = [nn(value_rows, grad_weights[:, h]) for h in halves]
            signed_list, score_grads_list = [], []
            for half in range(2):
                scores = scores_list[half]
                log_row = log_ref[:, pl.ds(pl.multiple_of(table[place] * BLK + half * HALF, HALF), HALF)]
                size = jnp.abs(scores) - log_row
                if masked:
                    mask = block_mask(number * BLK, place * BLK + half * HALF, length, size.shape)
                    size = jnp.where(mask, size, LOW)
                positive = jnp.exp2(size).astype(jnp.bfloat16)
                sign = sign_of(scores)
                signed_list.append(positive * sign)
                dot_row = dots[:, halves[half]].astype(jnp.bfloat16)
                inner = inner_list[half].astype(jnp.bfloat16) - dot_row * sign
                score_grads_list.append(positive * inner)
            signed = jnp.concatenate(signed_list, axis=1)
            score_grads = jnp.concatenate(score_grads_list, axis=1)
            sums[0:64, span] += nn(keys_t[:, key_span], score_grads)
            sums[64:128, key_span] += nt(queries[:, span], score_grads)
            sums[128:192, key_span] += nt(grads[:, span], signed)

        @pl.loop(0, place)
        def _(number):
            step(number, False)

        step(place, True)

    width = sends[0].shape[1]
    for part in range(parts):
        span = slice(part * width, (part + 1) * width)
        for rows, factor in ((slice(0, 128), scale), (slice(128, 192), 1.0)):
            done = (sums[rows, span] * factor).astype(jnp.bfloat16)
            whole_ref[rows, span] = done
            sends[part][rows, :] = done


def make_table(block_order, length, ctx_index, ctx):
    here = block_order.shape[0] // ctx
    order = (ctx_index - jnp.arange(ctx)) % ctx
    places = block_order.reshape(ctx, here)[order].reshape(-1)
    return jnp.concatenate([jnp.argsort(places).astype(jnp.int32), length[None]])


def head_specs(parts, span, row):
    return [pl.BlockSpec((HEAD_DIM, span), lambda i, t, row=row: (row, 0)) for _ in range(parts)]


def pair_tables(block_order, length, ctx_index, ctx):
    here = block_order.shape[0] // ctx
    order = (ctx_index - jnp.arange(ctx)) % ctx
    places = block_order.reshape(ctx, here)[order].reshape(-1)
    blocks = places.shape[0]
    part = jnp.arange(blocks) // here
    query, key = places[:, None], places[None, :]
    seen = ((key <= query) & (key * BLK < length)).reshape(-1)
    masked = ((key == query) | ((key + 1) * BLK > length)).reshape(-1)
    newest = jnp.maximum(part[:, None], part[None, :]).reshape(-1)
    phase = jnp.maximum(newest, 1)
    pairs = jnp.arange(blocks * blocks, dtype=jnp.int32)
    tables = []
    for number in range(1, ctx):
        mine = seen & (phase == number)
        plain = mine & ~masked
        rank = jnp.where(plain, 0, jnp.where(mine, 1, 2)) * pairs.shape[0] + pairs
        slot = jnp.sum((rank[None, :] < rank[:, None]).astype(jnp.int32), axis=1)
        codes = jnp.sum(jnp.where(slot[:, None] == pairs[None, :], pairs[:, None], 0), axis=0)
        counts = jnp.stack([jnp.sum(plain.astype(jnp.int32)), jnp.sum(mine.astype(jnp.int32)), length])
        tables.append(jnp.concatenate([counts, places, codes]).astype(jnp.int32))
    return tables


def attend_early(table, heads, ctx, packed_list, state):
    parts, span = len(packed_list), packed_list[0].shape[1]
    slots = ctx * span
    shapes = [(heads, 1, slots), (heads, 1, slots), (heads, HEAD_DIM, slots)]
    whole = lambda shape: pl.BlockSpec(shape, lambda i, t: (0,) * len(shape))
    return pl.pallas_call(
        functools.partial(early_kernel, parts, heads, state is None),
        grid_spec=pltpu.PrefetchScalarGridSpec(
            num_scalar_prefetch=1,
            grid=(1,),
            in_specs=[whole(packed_list[0].shape)] * parts
            + ([] if state is None else [whole(shape) for shape in shapes]),
            out_specs=[whole(shape) for shape in shapes],
            scratch_shapes=[
                pltpu.VMEM((128, slots), jnp.bfloat16),
                pltpu.VMEM((slots, 128), jnp.bfloat16),
                pltpu.VMEM((HEAD_DIM, slots), jnp.bfloat16),
            ],
        ),
        out_shape=[jax.ShapeDtypeStruct(shape, jnp.float32) for shape in shapes],
        compiler_params=pltpu.CompilerParams(vmem_limit_bytes=48 << 20),
        cost_estimate=pl.CostEstimate(flops=20_000_000_000, bytes_accessed=4_000_000, transcendentals=0),
        name="attend_early",
    )(table, *packed_list, *([] if state is None else state))


def attend_last(table, head, packed_list, state):
    parts, span = len(packed_list), packed_list[0].shape[1]
    slots = parts * span
    whole = lambda shape: pl.BlockSpec(shape, lambda i, t: (0,) * len(shape))
    piece = lambda rows: pl.BlockSpec((1, rows, slots), lambda i, t: (head, 0, 0))
    return pl.pallas_call(
        functools.partial(last_kernel, parts),
        grid_spec=pltpu.PrefetchScalarGridSpec(
            num_scalar_prefetch=1,
            grid=(1,),
            in_specs=head_specs(parts, span, 3 * head)
            + head_specs(parts, span, 3 * head + 1)
            + head_specs(parts, span, 3 * head + 2)
            + [piece(1), piece(1), piece(HEAD_DIM)],
            out_specs=[whole((HEAD_DIM, span))] * parts + [whole((HEAD_DIM, slots)), whole((1, slots))],
            scratch_shapes=[
                pltpu.VMEM((128, slots), jnp.bfloat16),
                pltpu.VMEM((slots, 128), jnp.bfloat16),
                pltpu.VMEM((HEAD_DIM, slots), jnp.bfloat16),
                pltpu.VMEM((1, slots), jnp.float32),
                pltpu.VMEM((1, slots), jnp.float32),
            ],
        ),
        out_shape=[jax.ShapeDtypeStruct((HEAD_DIM, span), jnp.bfloat16)] * parts
        + [
            jax.ShapeDtypeStruct((HEAD_DIM, slots), jnp.float32),
            jax.ShapeDtypeStruct((1, slots), jnp.float32),
        ],
        compiler_params=pltpu.CompilerParams(vmem_limit_bytes=40 << 20),
        cost_estimate=pl.CostEstimate(flops=10_000_000_000, bytes_accessed=4_000_000, transcendentals=0),
        name="attend_last",
    )(table, *packed_list, *packed_list, *packed_list, *state)


def attend_backward(table, head, packed_list, grad_list, exact, logs):
    parts, span = len(packed_list), packed_list[0].shape[1]
    slots = parts * span
    whole = lambda shape: pl.BlockSpec(shape, lambda i, t: (0, 0))
    three = 3 * HEAD_DIM
    return pl.pallas_call(
        functools.partial(backward_kernel, parts),
        grid_spec=pltpu.PrefetchScalarGridSpec(
            num_scalar_prefetch=1,
            grid=(1,),
            in_specs=head_specs(parts, span, 3 * head)
            + head_specs(parts, span, 3 * head + 1)
            + head_specs(parts, span, 3 * head + 2)
            + [whole((HEAD_DIM, span))] * parts
            + [whole((HEAD_DIM, slots)), whole((1, slots))],
            out_specs=[whole((three, span))] * parts + [whole((three, slots))],
            scratch_shapes=[pltpu.VMEM((HEAD_DIM, slots), jnp.bfloat16)] * 4
            + [pltpu.VMEM((slots, 128), jnp.bfloat16)] * 2
            + [
                pltpu.VMEM((three, slots), jnp.float32),
                pltpu.VMEM((128, BLK), jnp.bfloat16),
                pltpu.VMEM((128, BLK), jnp.bfloat16),
                pltpu.VMEM((1, BLK), jnp.float32),
            ],
        ),
        out_shape=[jax.ShapeDtypeStruct((three, span), jnp.bfloat16)] * parts
        + [jax.ShapeDtypeStruct((three, slots), jnp.bfloat16)],
        compiler_params=pltpu.CompilerParams(vmem_limit_bytes=40 << 20),
        cost_estimate=pl.CostEstimate(flops=40_000_000_000, bytes_accessed=6_000_000, transcendentals=0),
        name="attend_backward",
    )(table, *packed_list, *packed_list, *packed_list, *grad_list, exact, logs)


def layer_norm(values, gain):
    centre = jnp.mean(values, axis=-1, keepdims=True)
    centred = values - centre
    spread = jnp.mean(centred * centred, axis=-1, keepdims=True)
    return centred * lax.rsqrt(spread + 1e-05) * gain


def gelu_tanh(values):
    return jax.nn.gelu(values, approximate=True)


def product(equation, left, right):
    return jnp.einsum(equation, left, right, preferred_element_type=jnp.float32)


def shift(array, ctx, by):
    if by % ctx == 0:
        return array
    return lax.ppermute(array, "ctx", [(i, (i + by) % ctx) for i in range(ctx)])


def turned(array, axis, by):
    return lax.dynamic_slice_in_dim(
        jnp.concatenate([array, array], axis=axis), by, array.shape[axis], axis
    )


def gather_rows(array):
    return lax.all_gather(array, "fsdp", axis=0, tiled=True)


def scatter_rows(array):
    return lax.psum_scatter(
        array.astype(jnp.bfloat16), "fsdp", scatter_dimension=0, tiled=True
    )


def scatter_pairs(array, fsdp):
    me = lax.axis_index("fsdp")
    core, chip = me % 2, me // 2
    parts = array.reshape(fsdp // 2, 2, array.shape[0] // fsdp, array.shape[1])
    kept = lax.dynamic_index_in_dim(parts, core, 1, keepdims=False)
    sent = lax.dynamic_index_in_dim(parts, 1 - core, 1, keepdims=False).astype(jnp.bfloat16)
    got = lax.ppermute(sent, "fsdp", [(i, i ^ 1) for i in range(fsdp)])
    kept = kept.astype(jnp.float32) + got.astype(jnp.float32)
    total = lax.dynamic_index_in_dim(kept, chip, 0, keepdims=False)
    narrow = kept.astype(jnp.bfloat16)
    for other in range(1, fsdp // 2):
        sent = lax.dynamic_index_in_dim(narrow, chip ^ other, 0, keepdims=False)
        got = lax.ppermute(sent, "fsdp", [(i, i ^ (2 * other)) for i in range(fsdp)])
        total += got.astype(jnp.float32)
    return total


def per_device(
    ctx, fsdp, tokens_in, out_grad, gain_attn, gain_mlp, w_qkv, w_out, w_up, w_down, lengths, block_order
):
    local_rows, width = tokens_in.shape[1:]
    tokens_in, out_grad, length, block_order = tokens_in[0], out_grad[0], lengths[0], block_order[0]
    ctx_index = lax.axis_index("ctx")
    heads_here = width // HEAD_DIM // ctx
    own = heads_here * HEAD_DIM
    table = make_table(block_order, length, ctx_index, ctx)

    gains = jnp.stack([gain_attn, gain_mlp], axis=1)
    gains = jnp.pad(gains, ((0, 0), (0, 126)))
    ordered = w_qkv.reshape(-1, 3, ctx, heads_here, HEAD_DIM).transpose(0, 2, 3, 1, 4)
    ordered = turned(ordered.reshape(-1, ctx, 3 * own), 1, ctx_index).reshape(w_qkv.shape)
    first = gather_rows(jnp.concatenate([ordered, gains], axis=1))
    gain_one = first[:, 3 * width].astype(jnp.float32)
    gain_two = first[:, 3 * width + 1].astype(jnp.float32)
    w_out_all = gather_rows(w_out)
    w_up_all = gather_rows(w_up)
    w_down_all = gather_rows(w_down)
    w_own = first[:, : 3 * own]
    w_out_turned = turned(w_out_all.reshape(ctx, heads_here, HEAD_DIM, width), 0, ctx_index)
    w_out_turned = w_out_turned.transpose(1, 0, 2, 3).reshape(width, width)

    here = local_rows // BLK
    places = lax.dynamic_slice_in_dim(block_order, ctx_index * here, here)
    places = (places[:, None] * BLK + jnp.arange(BLK, dtype=jnp.int32)[None]).reshape(-1)
    grad_z = out_grad * (places < length).astype(jnp.bfloat16)[:, None]

    tables = pair_tables(block_order, length, ctx_index, ctx)
    normed_list, packed_list = [], []
    tokens, state = tokens_in, None
    for part in range(ctx):
        here_tokens, gain_here, state = lax.optimization_barrier((tokens, gain_one, state))
        normed = layer_norm(here_tokens.astype(jnp.float32), gain_here).astype(jnp.bfloat16)
        normed_list.append(normed)
        packed_list.append(product("jn,uj->nu", w_own, normed).astype(jnp.bfloat16))
        if 0 < part < ctx - 1:
            state = attend_early(tables[part - 1], heads_here, ctx, packed_list, state)
        if part == 1:
            tokens, grad_z, tables = lax.optimization_barrier((tokens, grad_z, tables))
        if part < ctx - 1:
            tokens = shift(tokens, ctx, 1)
    kept, mixed_parts = [], []
    for head in range(heads_here):
        results = attend_last(tables[-1], head, packed_list, state)
        kept.append((results[ctx], results[ctx + 1]))
        mixed_parts += [shift(results[part], ctx, -part) for part in range(ctx)]
    mixed_t = jnp.concatenate(mixed_parts, axis=0)

    tokens_f = tokens_in.astype(jnp.float32)
    middle = tokens_f + product("nu,nj->uj", mixed_t, w_out_turned)
    normed_two, norm_two_back = jax.vjp(lambda v: layer_norm(v, gain_two), middle)
    normed_two = normed_two.astype(jnp.bfloat16)
    pre_act = product("uj,jn->un", normed_two, w_up_all)
    activation, gelu_back = jax.vjp(gelu_tanh, pre_act)
    activation = activation.astype(jnp.bfloat16)
    result = (middle + product("un,nj->uj", activation, w_down_all)).astype(jnp.bfloat16)

    grad_act = product("uj,nj->un", grad_z, w_down_all)
    grad_pre = gelu_back(grad_act)[0].astype(jnp.bfloat16)
    grad_normed_two = product("un,jn->uj", grad_pre, w_up_all)
    grad_middle = grad_z.astype(jnp.float32) + norm_two_back(grad_normed_two)[0]
    grad_branch = grad_middle.astype(jnp.bfloat16)
    grad_mixed_t = product("nj,uj->nu", w_out_turned, grad_branch).astype(jnp.bfloat16)
    grads_by_head = []
    for head in range(heads_here):
        pieces = []
        for part in range(ctx):
            row = (head * ctx + part) * HEAD_DIM
            piece = grad_mixed_t[row : row + HEAD_DIM]
            pieces.append(shift(piece, ctx, part))
        grads_by_head.append(pieces)

    grad_w_down = product("un,uj->nj", activation, grad_z).astype(jnp.bfloat16)
    grad_w_up = product("uj,un->jn", normed_two, grad_pre).astype(jnp.bfloat16)
    grad_w_out = product("nu,uj->nj", mixed_t, grad_branch).astype(jnp.bfloat16)
    grad_w_out = turned(
        grad_w_out.reshape(heads_here, ctx, HEAD_DIM, width).transpose(1, 0, 2, 3), 0, (ctx - ctx_index) % ctx
    )
    grad_w_down = scatter_rows(grad_w_down)
    grad_up_out = scatter_rows(
        jnp.concatenate([grad_w_up, grad_w_out.reshape(width, width)], axis=1)
    )

    grad_parts, grad_whole = [], []
    for head in range(heads_here):
        if head == max(heads_here - 2, 0):
            grad_up_out, grad_w_down, table = lax.optimization_barrier(
                (grad_up_out, grad_w_down, table)
            )
            grad_up_out, grad_w_down = lax.psum((grad_up_out, grad_w_down), "ctx")
        results = attend_backward(table, head, packed_list, grads_by_head[head], *kept[head])
        grad_parts.append([shift(results[part], ctx, -part) for part in range(ctx)])
        grad_whole.append(results[ctx])
    normed_all = jnp.concatenate(normed_list, axis=0)
    grad_qkv_own = product("uj,nu->jn", normed_all, jnp.concatenate(grad_whole, axis=0))
    grad_qkv_own = scatter_pairs(grad_qkv_own, fsdp).astype(jnp.bfloat16)
    grad_qkv = lax.all_gather(grad_qkv_own, "ctx", axis=0)
    rows_here = grad_qkv.shape[1]
    grad_qkv = grad_qkv.reshape(ctx, rows_here, heads_here, 3, HEAD_DIM)
    grad_w_qkv = grad_qkv.transpose(1, 3, 0, 2, 4).reshape(rows_here, 3 * width).astype(jnp.float32)

    grad_packed_t = jnp.concatenate(
        [grad_parts[head][part] for part in range(ctx) for head in range(heads_here)], axis=0
    )
    grad_normed_one = product("nu,jn->uj", grad_packed_t, first[:, : 3 * width])
    norm_one_back = jax.vjp(lambda v: layer_norm(v, gain_one), tokens_f)[1]
    grad_tokens = (grad_middle + norm_one_back(grad_normed_one)[0]).astype(jnp.bfloat16)

    grad_w_down = grad_w_down.astype(jnp.float32)
    grad_w_up = grad_up_out[:, : w_up.shape[1]].astype(jnp.float32)
    grad_w_out = grad_up_out[:, w_up.shape[1] :].astype(jnp.float32)

    def gain_grad(grad_weight, weight, gain):
        total = jnp.sum(grad_weight * weight.astype(jnp.float32), axis=1)
        return total / gain.astype(jnp.float32)

    return (
        result[None],
        grad_tokens[None],
        gain_grad(grad_w_qkv, w_qkv, gain_attn),
        gain_grad(grad_w_up, w_up, gain_mlp),
        grad_w_qkv,
        grad_w_out,
        grad_w_up,
        grad_w_down,
    )


def solution(mesh):
    rows = P("fsdp", None)
    whole = P("fsdp", "ctx", None)
    ctx, fsdp = mesh.shape["ctx"], mesh.shape["fsdp"]

    def layer(*arrays):
        return per_device(ctx, fsdp, *arrays)

    return jax.shard_map(
        layer,
        mesh=mesh,
        in_specs=(whole, whole, P("fsdp"), P("fsdp"), rows, rows, rows, rows, P("fsdp"), rows),
        out_specs=(whole, whole, P("fsdp"), P("fsdp"), rows, rows, rows, rows),
        check_vma=False,
    )
```

```python
import functools

import jax
import jax.numpy as jnp
from jax import lax
from jax.experimental import pallas as pl
from jax.experimental.pallas import tpu as pltpu
from jax.sharding import PartitionSpec as P


HEAD_DIM = 64
BLK = 512
HALF = 256
LOG2E = 1.4426950408889634
BIG = 3e38
LOW = -1e30


def nn(left, right):
    return lax.dot_general(left, right, (((1,), (0,)), ((), ())), preferred_element_type=jnp.float32)


def nt(left, right):
    return lax.dot_general(left, right, (((1,), (1,)), ((), ())), preferred_element_type=jnp.float32)


def sign_of(scores):
    return jnp.clip(scores.astype(jnp.bfloat16) * jnp.bfloat16(BIG), -1.0, 1.0).astype(jnp.bfloat16)


def block_mask(key_start, query_start, length, shape):
    keys = key_start + lax.broadcasted_iota(jnp.int32, shape, 0)
    queries = query_start + lax.broadcasted_iota(jnp.int32, shape, 1)
    return keys <= jnp.minimum(queries, length - 1)


def gather_columns(refs, out):
    span = refs[0].shape[1]
    for part, ref in enumerate(refs):
        out[:, part * span : (part + 1) * span] = ref[...]


def turn_rows(source, out, twice):
    for part in range(source.shape[1] // BLK):
        span = slice(part * BLK, (part + 1) * BLK)
        piece = source[:, span]
        out[span, :] = jnp.concatenate([piece, piece if twice else jnp.zeros_like(piece)], axis=0).T


def query_weights(query_t):
    scaled = query_t.astype(jnp.float32) * (LOG2E * HEAD_DIM ** -0.5)
    high = scaled.astype(jnp.bfloat16)
    return jnp.concatenate([high, (scaled - high.astype(jnp.float32)).astype(jnp.bfloat16)], axis=0)


def pair_step(table, index, masked, weights, keys, values, top_ref, total_ref, mixed_ref):
    blocks = keys.shape[0] // BLK
    code = table[3 + blocks + index]
    query_block, key_block = code // blocks, code % blocks
    key_span = pl.ds(pl.multiple_of(key_block * BLK, BLK), BLK)
    key_rows, value_rows = keys[key_span, :], values[:, key_span]
    spans = [
        pl.ds(pl.multiple_of(query_block * BLK + half * HALF, HALF), HALF) for half in range(2)
    ]
    scores_list = [nn(key_rows, weights[:, span]) for span in spans]
    for half in range(2):
        span, scores = spans[half], scores_list[half]
        top = top_ref[:, span]
        size = jnp.abs(scores)
        if masked:
            key_start = table[3 + key_block] * BLK
            query_start = table[3 + query_block] * BLK + half * HALF
            size = jnp.where(block_mask(key_start, query_start, table[2], size.shape), size, LOW)
        new_top = jnp.maximum(top, jnp.max(size, axis=0, keepdims=True))
        fade = jnp.exp2(top - new_top)
        powers = jnp.exp2(size - new_top)
        signed = powers.astype(jnp.bfloat16) * sign_of(scores)
        top_ref[:, span] = new_top
        total_ref[:, span] = total_ref[:, span] * fade + jnp.sum(powers, axis=0, keepdims=True)
        mixed_ref[:, span] = mixed_ref[:, span] * fade + nn(value_rows, signed)


def run_pairs(table, *refs):
    @pl.loop(0, table[0])
    def _(index):
        pair_step(table, index, False, *refs)

    @pl.loop(table[0], table[1])
    def _(index):
        pair_step(table, index, True, *refs)


def load_head_part(part, query_ref, key_ref, value_ref, weights, keys, values):
    width = query_ref.shape[1]
    span = slice(part * width, (part + 1) * width)
    weights[:, span] = query_weights(query_ref[...])
    key_rows = key_ref[...]
    for start in range(0, width, BLK):
        piece = key_rows[:, start : start + BLK]
        rows = slice(part * width + start, part * width + start + BLK)
        keys[rows, :] = jnp.concatenate([piece, piece], axis=0).T
    values[:, span] = value_ref[...]


def early_kernel(parts, heads, first, table, *refs):
    packed_refs, refs = refs[:parts], refs[parts:]
    if not first:
        before, refs = refs[:3], refs[3:]
    top_ref, total_ref, mixed_ref, weights, keys, values = refs

    @pl.loop(0, heads)
    def _(head):
        def rows_of(kind):
            return pl.ds(pl.multiple_of((3 * head + kind) * HEAD_DIM, HEAD_DIM), HEAD_DIM)

        for part, ref in enumerate(packed_refs):
            three = [ref.at[rows_of(kind), :] for kind in range(3)]
            load_head_part(part, *three, weights, keys, values)
        state = (top_ref.at[head], total_ref.at[head], mixed_ref.at[head])
        if first:
            for ref, value in zip(state, (LOW, 0.0, 0.0)):
                ref[...] = jnp.full(ref.shape, value, jnp.float32)
        else:
            for ref, old in zip(state, before):
                ref[...] = old[head]
        run_pairs(table, weights, keys, values, *state)


def last_kernel(parts, table, *refs):
    query_refs, key_refs, value_refs = refs[:parts], refs[parts : 2 * parts], refs[2 * parts : 3 * parts]
    before, refs = refs[3 * parts : 3 * parts + 3], refs[3 * parts + 3 :]
    sends, refs = refs[:parts], refs[parts:]
    exact_ref, log_ref, weights, keys, values, top_ref, total_ref = refs
    for part in range(parts):
        load_head_part(part, query_refs[part], key_refs[part], value_refs[part], weights, keys, values)
    top_ref[...] = before[0][0]
    total_ref[...] = before[1][0]
    exact_ref[...] = before[2][0]
    run_pairs(table, weights, keys, values, top_ref, total_ref, exact_ref)
    log_ref[...] = top_ref[...] + jnp.log2(total_ref[...])
    width = sends[0].shape[1]
    for part in range(parts):
        span = slice(part * width, (part + 1) * width)
        done = exact_ref[:, span] / total_ref[:, span]
        exact_ref[:, span] = done
        sends[part][...] = done.astype(jnp.bfloat16)


def backward_kernel(parts, table, *refs):
    query_refs, key_refs, value_refs = refs[:parts], refs[parts : 2 * parts], refs[2 * parts : 3 * parts]
    grad_refs, refs = refs[3 * parts : 4 * parts], refs[4 * parts :]
    exact_ref, log_ref, sends, refs = refs[0], refs[1], refs[2 : 2 + parts], refs[2 + parts :]
    whole_ref, queries, keys_t, values_t, grads, keys, values, sums, weights, grad_weights, dots, scores_ref, inner_ref = refs
    blocks = queries.shape[1] // BLK
    length = table[blocks]
    scale = HEAD_DIM ** -0.5
    gather_columns(query_refs, queries)
    gather_columns(key_refs, keys_t)
    gather_columns(value_refs, values_t)
    gather_columns(grad_refs, grads)
    turn_rows(keys_t, keys, True)
    turn_rows(values_t, values, False)
    sums[...] = jnp.zeros_like(sums)
    grad_weights[...] = jnp.zeros_like(grad_weights)
    full = (length + BLK - 1) // BLK

    @pl.loop(0, full)
    def _(place):
        span = pl.ds(pl.multiple_of(table[place] * BLK, BLK), BLK)
        weights[...] = query_weights(queries[:, span])
        grad_t = grads[:, span]
        grad_weights[:HEAD_DIM, :] = grad_t
        dots[...] = jnp.sum(grad_t.astype(jnp.float32) * exact_ref[:, span], axis=0, keepdims=True)

        halves = [slice(h * HALF, (h + 1) * HALF) for h in range(2)]

        def start_half(number, half):
            key_span = pl.ds(pl.multiple_of(table[number] * BLK, BLK), BLK)
            scores_ref[half] = nn(keys[key_span, :], weights[:, halves[half]])
            inner_ref[half] = nn(values[key_span, :], grad_weights[:, halves[half]])

        def step(number, masked):
            key_span = pl.ds(pl.multiple_of(table[number] * BLK, BLK), BLK)
            signed_list, score_grads_list = [], []
            for half in range(2):
                scores = scores_ref[half]
                log_row = log_ref[:, pl.ds(pl.multiple_of(table[place] * BLK + half * HALF, HALF), HALF)]
                size = jnp.abs(scores) - log_row
                if masked:
                    mask = block_mask(number * BLK, place * BLK + half * HALF, length, size.shape)
                    size = jnp.where(mask, size, LOW)
                positive = jnp.exp2(size).astype(jnp.bfloat16)
                sign = sign_of(scores)
                signed_list.append(positive * sign)
                dot_row = dots[:, halves[half]].astype(jnp.bfloat16)
                inner = inner_ref[half].astype(jnp.bfloat16) - dot_row * sign
                score_grads_list.append(positive * inner)
                if not masked:
                    start_half(number + 1, half)
            signed = jnp.concatenate(signed_list, axis=1)
            score_grads = jnp.concatenate(score_grads_list, axis=1)
            sums[0:64, span] += nn(keys_t[:, key_span], score_grads)
            sums[64:128, key_span] += nt(queries[:, span], score_grads)
            sums[128:192, key_span] += nt(grads[:, span], signed)

        for half in range(2):
            start_half(0, half)

        @pl.loop(0, place)
        def _(number):
            step(number, False)

        step(place, True)

    width = sends[0].shape[1]
    for part in range(parts):
        span = slice(part * width, (part + 1) * width)
        for rows, factor in ((slice(0, 128), scale), (slice(128, 192), 1.0)):
            done = (sums[rows, span] * factor).astype(jnp.bfloat16)
            whole_ref[rows, span] = done
            sends[part][rows, :] = done


def join_kernel(*refs):
    pieces, weight_ref, out_ref, joined = refs[:-3], refs[-3], refs[-2], refs[-1]
    rows = pieces[0].shape[0]
    for number, piece in enumerate(pieces):
        joined[number * rows : (number + 1) * rows, :] = piece[...]

    @pl.loop(0, weight_ref.shape[0] // HALF)
    def _(tile):
        span = pl.ds(pl.multiple_of(tile * HALF, HALF), HALF)
        out_ref[:, span] = nn(weight_ref[span, : joined.shape[0]], joined[...]).T


def join_product(pieces, weight):
    rows, span = pieces[0].shape
    width = weight.shape[0]
    total = len(pieces) * rows
    return pl.pallas_call(
        join_kernel,
        out_shape=jax.ShapeDtypeStruct((span, width), jnp.float32),
        scratch_shapes=[pltpu.VMEM((total, span), jnp.bfloat16)],
        compiler_params=pltpu.CompilerParams(vmem_limit_bytes=48 << 20),
        cost_estimate=pl.CostEstimate(
            flops=2 * span * width * total, bytes_accessed=12_000_000, transcendentals=0
        ),
        name="join_product",
    )(*pieces, weight)


def make_table(block_order, length, ctx_index, ctx):
    here = block_order.shape[0] // ctx
    order = (ctx_index - jnp.arange(ctx)) % ctx
    places = block_order.reshape(ctx, here)[order].reshape(-1)
    return jnp.concatenate([jnp.argsort(places).astype(jnp.int32), length[None]])


def head_specs(parts, span, row):
    return [pl.BlockSpec((HEAD_DIM, span), lambda i, t, row=row: (row, 0)) for _ in range(parts)]


def pair_tables(block_order, length, ctx_index, ctx):
    here = block_order.shape[0] // ctx
    order = (ctx_index - jnp.arange(ctx)) % ctx
    places = block_order.reshape(ctx, here)[order].reshape(-1)
    blocks = places.shape[0]
    part = jnp.arange(blocks) // here
    query, key = places[:, None], places[None, :]
    seen = ((key <= query) & (key * BLK < length)).reshape(-1)
    masked = ((key == query) | ((key + 1) * BLK > length)).reshape(-1)
    newest = jnp.maximum(part[:, None], part[None, :]).reshape(-1)
    phase = jnp.maximum(newest, 1)
    pairs = jnp.arange(blocks * blocks, dtype=jnp.int32)
    tables = []
    for number in range(1, ctx):
        mine = seen & (phase == number)
        plain = mine & ~masked
        rank = jnp.where(plain, 0, jnp.where(mine, 1, 2)) * pairs.shape[0] + pairs
        slot = jnp.sum((rank[None, :] < rank[:, None]).astype(jnp.int32), axis=1)
        codes = jnp.sum(jnp.where(slot[:, None] == pairs[None, :], pairs[:, None], 0), axis=0)
        counts = jnp.stack([jnp.sum(plain.astype(jnp.int32)), jnp.sum(mine.astype(jnp.int32)), length])
        tables.append(jnp.concatenate([counts, places, codes]).astype(jnp.int32))
    return tables


def attend_early(table, heads, ctx, packed_list, state):
    parts, span = len(packed_list), packed_list[0].shape[1]
    slots = ctx * span
    shapes = [(heads, 1, slots), (heads, 1, slots), (heads, HEAD_DIM, slots)]
    whole = lambda shape: pl.BlockSpec(shape, lambda i, t: (0,) * len(shape))
    return pl.pallas_call(
        functools.partial(early_kernel, parts, heads, state is None),
        grid_spec=pltpu.PrefetchScalarGridSpec(
            num_scalar_prefetch=1,
            grid=(1,),
            in_specs=[whole(packed_list[0].shape)] * parts
            + ([] if state is None else [whole(shape) for shape in shapes]),
            out_specs=[whole(shape) for shape in shapes],
            scratch_shapes=[
                pltpu.VMEM((128, slots), jnp.bfloat16),
                pltpu.VMEM((slots, 128), jnp.bfloat16),
                pltpu.VMEM((HEAD_DIM, slots), jnp.bfloat16),
            ],
        ),
        out_shape=[jax.ShapeDtypeStruct(shape, jnp.float32) for shape in shapes],
        compiler_params=pltpu.CompilerParams(vmem_limit_bytes=48 << 20),
        cost_estimate=pl.CostEstimate(flops=20_000_000_000, bytes_accessed=4_000_000, transcendentals=0),
        name="attend_early",
    )(table, *packed_list, *([] if state is None else state))


def attend_last(table, head, packed_list, state):
    parts, span = len(packed_list), packed_list[0].shape[1]
    slots = parts * span
    whole = lambda shape: pl.BlockSpec(shape, lambda i, t: (0,) * len(shape))
    piece = lambda rows: pl.BlockSpec((1, rows, slots), lambda i, t: (head, 0, 0))
    return pl.pallas_call(
        functools.partial(last_kernel, parts),
        grid_spec=pltpu.PrefetchScalarGridSpec(
            num_scalar_prefetch=1,
            grid=(1,),
            in_specs=head_specs(parts, span, 3 * head)
            + head_specs(parts, span, 3 * head + 1)
            + head_specs(parts, span, 3 * head + 2)
            + [piece(1), piece(1), piece(HEAD_DIM)],
            out_specs=[whole((HEAD_DIM, span))] * parts + [whole((HEAD_DIM, slots)), whole((1, slots))],
            scratch_shapes=[
                pltpu.VMEM((128, slots), jnp.bfloat16),
                pltpu.VMEM((slots, 128), jnp.bfloat16),
                pltpu.VMEM((HEAD_DIM, slots), jnp.bfloat16),
                pltpu.VMEM((1, slots), jnp.float32),
                pltpu.VMEM((1, slots), jnp.float32),
            ],
        ),
        out_shape=[jax.ShapeDtypeStruct((HEAD_DIM, span), jnp.bfloat16)] * parts
        + [
            jax.ShapeDtypeStruct((HEAD_DIM, slots), jnp.float32),
            jax.ShapeDtypeStruct((1, slots), jnp.float32),
        ],
        compiler_params=pltpu.CompilerParams(vmem_limit_bytes=40 << 20),
        cost_estimate=pl.CostEstimate(flops=10_000_000_000, bytes_accessed=4_000_000, transcendentals=0),
        name="attend_last",
    )(table, *packed_list, *packed_list, *packed_list, *state)


def attend_backward(table, head, packed_list, grad_list, exact, logs):
    parts, span = len(packed_list), packed_list[0].shape[1]
    slots = parts * span
    whole = lambda shape: pl.BlockSpec(shape, lambda i, t: (0, 0))
    three = 3 * HEAD_DIM
    return pl.pallas_call(
        functools.partial(backward_kernel, parts),
        grid_spec=pltpu.PrefetchScalarGridSpec(
            num_scalar_prefetch=1,
            grid=(1,),
            in_specs=head_specs(parts, span, 3 * head)
            + head_specs(parts, span, 3 * head + 1)
            + head_specs(parts, span, 3 * head + 2)
            + [whole((HEAD_DIM, span))] * parts
            + [whole((HEAD_DIM, slots)), whole((1, slots))],
            out_specs=[whole((three, span))] * parts + [whole((three, slots))],
            scratch_shapes=[pltpu.VMEM((HEAD_DIM, slots), jnp.bfloat16)] * 4
            + [pltpu.VMEM((slots, 128), jnp.bfloat16)] * 2
            + [
                pltpu.VMEM((three, slots), jnp.float32),
                pltpu.VMEM((128, BLK), jnp.bfloat16),
                pltpu.VMEM((128, BLK), jnp.bfloat16),
                pltpu.VMEM((1, BLK), jnp.float32),
                pltpu.VMEM((2, BLK, HALF), jnp.float32),
                pltpu.VMEM((2, BLK, HALF), jnp.float32),
            ],
        ),
        out_shape=[jax.ShapeDtypeStruct((three, span), jnp.bfloat16)] * parts
        + [jax.ShapeDtypeStruct((three, slots), jnp.bfloat16)],
        compiler_params=pltpu.CompilerParams(vmem_limit_bytes=40 << 20),
        cost_estimate=pl.CostEstimate(flops=40_000_000_000, bytes_accessed=6_000_000, transcendentals=0),
        name="attend_backward",
    )(table, *packed_list, *packed_list, *packed_list, *grad_list, exact, logs)


def layer_norm(values, gain):
    centre = jnp.mean(values, axis=-1, keepdims=True)
    centred = values - centre
    spread = jnp.mean(centred * centred, axis=-1, keepdims=True)
    return centred * lax.rsqrt(spread + 1e-05) * gain


def gelu_tanh(values):
    return jax.nn.gelu(values, approximate=True)


def product(equation, left, right):
    return jnp.einsum(equation, left, right, preferred_element_type=jnp.float32)


def shift(array, ctx, by):
    if by % ctx == 0:
        return array
    return lax.ppermute(array, "ctx", [(i, (i + by) % ctx) for i in range(ctx)])


def turned(array, axis, by):
    return lax.dynamic_slice_in_dim(
        jnp.concatenate([array, array], axis=axis), by, array.shape[axis], axis
    )


def gather_rows(array):
    return lax.all_gather(array, "fsdp", axis=0, tiled=True)


def scatter_rows(array):
    return lax.psum_scatter(
        array.astype(jnp.bfloat16), "fsdp", scatter_dimension=0, tiled=True
    )


def scatter_pairs(array, fsdp):
    me = lax.axis_index("fsdp")
    core, chip = me % 2, me // 2
    parts = array.reshape(fsdp // 2, 2, array.shape[0] // fsdp, array.shape[1])
    kept = lax.dynamic_index_in_dim(parts, core, 1, keepdims=False)
    sent = lax.dynamic_index_in_dim(parts, 1 - core, 1, keepdims=False).astype(jnp.bfloat16)
    got = lax.ppermute(sent, "fsdp", [(i, i ^ 1) for i in range(fsdp)])
    kept = kept.astype(jnp.float32) + got.astype(jnp.float32)
    total = lax.dynamic_index_in_dim(kept, chip, 0, keepdims=False)
    narrow = kept.astype(jnp.bfloat16)
    for other in range(1, fsdp // 2):
        sent = lax.dynamic_index_in_dim(narrow, chip ^ other, 0, keepdims=False)
        got = lax.ppermute(sent, "fsdp", [(i, i ^ (2 * other)) for i in range(fsdp)])
        total += got.astype(jnp.float32)
    return total


def per_device(
    ctx, fsdp, tokens_in, out_grad, gain_attn, gain_mlp, w_qkv, w_out, w_up, w_down, lengths, block_order
):
    local_rows, width = tokens_in.shape[1:]
    tokens_in, out_grad, length, block_order = tokens_in[0], out_grad[0], lengths[0], block_order[0]
    ctx_index = lax.axis_index("ctx")
    heads_here = width // HEAD_DIM // ctx
    own = heads_here * HEAD_DIM
    table = make_table(block_order, length, ctx_index, ctx)

    gains = jnp.stack([gain_attn, gain_mlp], axis=1)
    gains = jnp.pad(gains, ((0, 0), (0, 126)))
    ordered = w_qkv.reshape(-1, 3, ctx, heads_here, HEAD_DIM).transpose(0, 2, 3, 1, 4)
    ordered = turned(ordered.reshape(-1, ctx, 3 * own), 1, ctx_index).reshape(w_qkv.shape)
    first = gather_rows(jnp.concatenate([ordered, gains], axis=1))
    gain_one = first[:, 3 * width].astype(jnp.float32)
    gain_two = first[:, 3 * width + 1].astype(jnp.float32)
    w_out_all = gather_rows(w_out)
    w_up_all = gather_rows(w_up)
    w_down_all = gather_rows(w_down)
    w_own = first[:, : 3 * own]
    w_out_turned = turned(w_out_all.reshape(ctx, heads_here, HEAD_DIM, width), 0, ctx_index)
    w_out_turned = w_out_turned.transpose(1, 0, 2, 3).reshape(width, width)

    here = local_rows // BLK
    places = lax.dynamic_slice_in_dim(block_order, ctx_index * here, here)
    places = (places[:, None] * BLK + jnp.arange(BLK, dtype=jnp.int32)[None]).reshape(-1)
    grad_z = out_grad * (places < length).astype(jnp.bfloat16)[:, None]

    tables = pair_tables(block_order, length, ctx_index, ctx)
    normed_list, packed_list = [], []
    tokens, state = tokens_in, None
    for part in range(ctx):
        here_tokens, gain_here, state = lax.optimization_barrier((tokens, gain_one, state))
        normed = layer_norm(here_tokens.astype(jnp.float32), gain_here).astype(jnp.bfloat16)
        normed_list.append(normed)
        packed_list.append(product("jn,uj->nu", w_own, normed).astype(jnp.bfloat16))
        if 0 < part < ctx - 1:
            state = attend_early(tables[part - 1], heads_here, ctx, packed_list, state)
        if part == 1:
            tokens, grad_z, tables = lax.optimization_barrier((tokens, grad_z, tables))
        if part < ctx - 1:
            tokens = shift(tokens, ctx, 1)
    kept, mixed_parts = [], []
    for head in range(heads_here):
        results = attend_last(tables[-1], head, packed_list, state)
        kept.append((results[ctx], results[ctx + 1]))
        mixed_parts += [shift(results[part], ctx, -part) for part in range(ctx)]
    mixed_t = jnp.concatenate(mixed_parts, axis=0)

    tokens_f = tokens_in.astype(jnp.float32)
    middle = tokens_f + product("nu,nj->uj", mixed_t, w_out_turned)
    normed_two, norm_two_back = jax.vjp(lambda v: layer_norm(v, gain_two), middle)
    normed_two = normed_two.astype(jnp.bfloat16)
    pre_act = product("uj,jn->un", normed_two, w_up_all)
    activation, gelu_back = jax.vjp(gelu_tanh, pre_act)
    activation = activation.astype(jnp.bfloat16)
    result = (middle + product("un,nj->uj", activation, w_down_all)).astype(jnp.bfloat16)

    grad_act = product("uj,nj->un", grad_z, w_down_all)
    grad_pre = gelu_back(grad_act)[0].astype(jnp.bfloat16)
    grad_normed_two = product("un,jn->uj", grad_pre, w_up_all)
    grad_middle = grad_z.astype(jnp.float32) + norm_two_back(grad_normed_two)[0]
    grad_branch = grad_middle.astype(jnp.bfloat16)
    grad_mixed_t = product("nj,uj->nu", w_out_turned, grad_branch).astype(jnp.bfloat16)
    grads_by_head = []
    for head in range(heads_here):
        pieces = []
        for part in range(ctx):
            row = (head * ctx + part) * HEAD_DIM
            piece = grad_mixed_t[row : row + HEAD_DIM]
            pieces.append(shift(piece, ctx, part))
        grads_by_head.append(pieces)

    grad_w_down = product("un,uj->nj", activation, grad_z).astype(jnp.bfloat16)
    grad_w_up = product("uj,un->jn", normed_two, grad_pre).astype(jnp.bfloat16)
    grad_w_out = product("nu,uj->nj", mixed_t, grad_branch).astype(jnp.bfloat16)
    grad_w_out = turned(
        grad_w_out.reshape(heads_here, ctx, HEAD_DIM, width).transpose(1, 0, 2, 3), 0, (ctx - ctx_index) % ctx
    )
    grad_w_down = scatter_rows(grad_w_down)
    grad_up_out = scatter_rows(
        jnp.concatenate([grad_w_up, grad_w_out.reshape(width, width)], axis=1)
    )

    grad_parts, grad_whole = [], []
    for head in range(heads_here):
        if head == max(heads_here - 2, 0):
            grad_up_out, grad_w_down, table = lax.optimization_barrier(
                (grad_up_out, grad_w_down, table)
            )
            grad_up_out, grad_w_down = lax.psum((grad_up_out, grad_w_down), "ctx")
        results = attend_backward(table, head, packed_list, grads_by_head[head], *kept[head])
        grad_parts.append([shift(results[part], ctx, -part) for part in range(ctx)])
        grad_whole.append(results[ctx])
    normed_all = jnp.concatenate(normed_list, axis=0)
    grad_qkv_own = product("uj,nu->jn", normed_all, jnp.concatenate(grad_whole, axis=0))
    grad_qkv_own = scatter_pairs(grad_qkv_own, fsdp).astype(jnp.bfloat16)
    grad_qkv = [shift(grad_qkv_own, ctx, -part) for part in range(ctx)]
    grad_qkv = turned(jnp.stack(grad_qkv), 0, (ctx - ctx_index) % ctx)
    rows_here = grad_qkv.shape[1]
    grad_qkv = grad_qkv.reshape(ctx, rows_here, heads_here, 3, HEAD_DIM)
    grad_w_qkv = grad_qkv.transpose(1, 3, 0, 2, 4).reshape(rows_here, 3 * width).astype(jnp.float32)

    grad_normed_one = join_product([grad_parts[head][part] for part in range(ctx) for head in range(heads_here)], first)
    norm_one_back = jax.vjp(lambda v: layer_norm(v, gain_one), tokens_f)[1]
    grad_tokens = (grad_middle + norm_one_back(grad_normed_one)[0]).astype(jnp.bfloat16)

    grad_w_down = grad_w_down.astype(jnp.float32)
    grad_w_up = grad_up_out[:, : w_up.shape[1]].astype(jnp.float32)
    grad_w_out = grad_up_out[:, w_up.shape[1] :].astype(jnp.float32)

    def gain_grad(grad_weight, weight, gain):
        total = jnp.sum(grad_weight * weight.astype(jnp.float32), axis=1)
        return total / gain.astype(jnp.float32)

    return (
        result[None],
        grad_tokens[None],
        gain_grad(grad_w_qkv, w_qkv, gain_attn),
        gain_grad(grad_w_up, w_up, gain_mlp),
        grad_w_qkv,
        grad_w_out,
        grad_w_up,
        grad_w_down,
    )


def solution(mesh):
    rows = P("fsdp", None)
    whole = P("fsdp", "ctx", None)
    ctx, fsdp = mesh.shape["ctx"], mesh.shape["fsdp"]

    def layer(*arrays):
        return per_device(ctx, fsdp, *arrays)

    return jax.shard_map(
        layer,
        mesh=mesh,
        in_specs=(whole, whole, P("fsdp"), P("fsdp"), rows, rows, rows, rows, P("fsdp"), rows),
        out_specs=(whole, whole, P("fsdp"), P("fsdp"), rows, rows, rows, rows),
        check_vma=False,
    )
```

```python
import functools

import jax
import jax.numpy as jnp
from jax import lax
from jax.experimental import pallas as pl
from jax.experimental.pallas import tpu as pltpu
from jax.sharding import PartitionSpec as P


HEAD_DIM = 64
BLK = 512
HALF = 256
LOG2E = 1.4426950408889634
BIG = 3e38
LOW = -1e30


def nn(left, right):
    return lax.dot_general(left, right, (((1,), (0,)), ((), ())), preferred_element_type=jnp.float32)


def nt(left, right):
    return lax.dot_general(left, right, (((1,), (1,)), ((), ())), preferred_element_type=jnp.float32)


def sign_of(scores):
    return jnp.clip(scores.astype(jnp.bfloat16) * jnp.bfloat16(BIG), -1.0, 1.0).astype(jnp.bfloat16)


def block_mask(key_start, query_start, length, shape):
    keys = key_start + lax.broadcasted_iota(jnp.int32, shape, 0)
    queries = query_start + lax.broadcasted_iota(jnp.int32, shape, 1)
    return keys <= jnp.minimum(queries, length - 1)


def gather_columns(refs, out):
    span = refs[0].shape[1]
    for part, ref in enumerate(refs):
        out[:, part * span : (part + 1) * span] = ref[...]


def turn_rows(source, out, twice):
    for part in range(source.shape[1] // BLK):
        span = slice(part * BLK, (part + 1) * BLK)
        piece = source[:, span]
        out[span, :] = jnp.concatenate([piece, piece if twice else jnp.zeros_like(piece)], axis=0).T


def query_weights(query_t):
    scaled = query_t.astype(jnp.float32) * (LOG2E * HEAD_DIM ** -0.5)
    high = scaled.astype(jnp.bfloat16)
    return jnp.concatenate([high, (scaled - high.astype(jnp.float32)).astype(jnp.bfloat16)], axis=0)


def pair_step(table, index, masked, weights, keys, values, top_ref, total_ref, mixed_ref):
    blocks = keys.shape[0] // BLK
    code = table[3 + blocks + index]
    query_block, key_block = code // blocks, code % blocks
    key_span = pl.ds(pl.multiple_of(key_block * BLK, BLK), BLK)
    key_rows, value_rows = keys[key_span, :], values[:, key_span]
    spans = [
        pl.ds(pl.multiple_of(query_block * BLK + half * HALF, HALF), HALF) for half in range(2)
    ]
    scores_list = [nn(key_rows, weights[:, span]) for span in spans]
    for half in range(2):
        span, scores = spans[half], scores_list[half]
        top = top_ref[:, span]
        size = jnp.abs(scores)
        if masked:
            key_start = table[3 + key_block] * BLK
            query_start = table[3 + query_block] * BLK + half * HALF
            size = jnp.where(block_mask(key_start, query_start, table[2], size.shape), size, LOW)
        new_top = jnp.maximum(top, jnp.max(size, axis=0, keepdims=True))
        fade = jnp.exp2(top - new_top)
        powers = jnp.exp2(size - new_top)
        signed = powers.astype(jnp.bfloat16) * sign_of(scores)
        top_ref[:, span] = new_top
        total_ref[:, span] = total_ref[:, span] * fade + jnp.sum(powers, axis=0, keepdims=True)
        mixed_ref[:, span] = mixed_ref[:, span] * fade + nn(value_rows, signed)


def run_pairs(table, *refs):
    @pl.loop(0, table[0])
    def _(index):
        pair_step(table, index, False, *refs)

    @pl.loop(table[0], table[1])
    def _(index):
        pair_step(table, index, True, *refs)


def load_head_part(part, query_ref, key_ref, value_ref, weights, keys, values):
    width = query_ref.shape[1]
    span = slice(part * width, (part + 1) * width)
    weights[:, span] = query_weights(query_ref[...])
    key_rows = key_ref[...]
    for start in range(0, width, BLK):
        piece = key_rows[:, start : start + BLK]
        rows = slice(part * width + start, part * width + start + BLK)
        keys[rows, :] = jnp.concatenate([piece, piece], axis=0).T
    values[:, span] = value_ref[...]


def early_kernel(parts, heads, first, table, *refs):
    packed_refs, refs = refs[:parts], refs[parts:]
    if not first:
        before, refs = refs[:3], refs[3:]
    top_ref, total_ref, mixed_ref, weights, keys, values = refs

    @pl.loop(0, heads)
    def _(head):
        def rows_of(kind):
            return pl.ds(pl.multiple_of((3 * head + kind) * HEAD_DIM, HEAD_DIM), HEAD_DIM)

        for part, ref in enumerate(packed_refs):
            three = [ref.at[rows_of(kind), :] for kind in range(3)]
            load_head_part(part, *three, weights, keys, values)
        state = (top_ref.at[head], total_ref.at[head], mixed_ref.at[head])
        if first:
            for ref, value in zip(state, (LOW, 0.0, 0.0)):
                ref[...] = jnp.full(ref.shape, value, jnp.float32)
        else:
            for ref, old in zip(state, before):
                ref[...] = old[head]
        run_pairs(table, weights, keys, values, *state)


def last_kernel(parts, table, *refs):
    query_refs, key_refs, value_refs = refs[:parts], refs[parts : 2 * parts], refs[2 * parts : 3 * parts]
    before, refs = refs[3 * parts : 3 * parts + 3], refs[3 * parts + 3 :]
    sends, refs = refs[:parts], refs[parts:]
    exact_ref, log_ref, weights, keys, values, top_ref, total_ref = refs
    for part in range(parts):
        load_head_part(part, query_refs[part], key_refs[part], value_refs[part], weights, keys, values)
    top_ref[...] = before[0][0]
    total_ref[...] = before[1][0]
    exact_ref[...] = before[2][0]
    run_pairs(table, weights, keys, values, top_ref, total_ref, exact_ref)
    log_ref[...] = top_ref[...] + jnp.log2(total_ref[...])
    width = sends[0].shape[1]
    for part in range(parts):
        span = slice(part * width, (part + 1) * width)
        done = exact_ref[:, span] / total_ref[:, span]
        exact_ref[:, span] = done
        sends[part][...] = done.astype(jnp.bfloat16)


def backward_kernel(parts, table, *refs):
    query_refs, key_refs, value_refs = refs[:parts], refs[parts : 2 * parts], refs[2 * parts : 3 * parts]
    grad_refs, refs = refs[3 * parts : 4 * parts], refs[4 * parts :]
    exact_ref, log_ref, sends, refs = refs[0], refs[1], refs[2 : 2 + parts], refs[2 + parts :]
    whole_ref, queries, keys_t, values_t, grads, keys, values, sums, weights, grad_weights, dots, scores_ref, inner_ref = refs
    blocks = queries.shape[1] // BLK
    length = table[blocks]
    scale = HEAD_DIM ** -0.5
    gather_columns(query_refs, queries)
    gather_columns(key_refs, keys_t)
    gather_columns(value_refs, values_t)
    gather_columns(grad_refs, grads)
    turn_rows(keys_t, keys, True)
    turn_rows(values_t, values, False)
    sums[...] = jnp.zeros_like(sums)
    grad_weights[...] = jnp.zeros_like(grad_weights)
    full = (length + BLK - 1) // BLK

    @pl.loop(0, full)
    def _(place):
        span = pl.ds(pl.multiple_of(table[place] * BLK, BLK), BLK)
        weights[...] = query_weights(queries[:, span])
        grad_t = grads[:, span]
        grad_weights[:HEAD_DIM, :] = grad_t
        dots[...] = jnp.sum(grad_t.astype(jnp.float32) * exact_ref[:, span], axis=0, keepdims=True)

        halves = [slice(h * HALF, (h + 1) * HALF) for h in range(2)]

        def start_half(number, half):
            key_span = pl.ds(pl.multiple_of(table[number] * BLK, BLK), BLK)
            scores_ref[half] = nn(keys[key_span, :], weights[:, halves[half]])
            inner_ref[half] = nn(values[key_span, :], grad_weights[:, halves[half]])

        def step(number, masked):
            key_span = pl.ds(pl.multiple_of(table[number] * BLK, BLK), BLK)
            signed_list, score_grads_list = [], []
            for half in range(2):
                scores = scores_ref[half]
                log_row = log_ref[:, pl.ds(pl.multiple_of(table[place] * BLK + half * HALF, HALF), HALF)]
                size = jnp.abs(scores) - log_row
                if masked:
                    mask = block_mask(number * BLK, place * BLK + half * HALF, length, size.shape)
                    size = jnp.where(mask, size, LOW)
                positive = jnp.exp2(size).astype(jnp.bfloat16)
                sign = sign_of(scores)
                signed_list.append(positive * sign)
                dot_row = dots[:, halves[half]].astype(jnp.bfloat16)
                inner = inner_ref[half].astype(jnp.bfloat16) - dot_row * sign
                score_grads_list.append(positive * inner)
                if not masked:
                    start_half(number + 1, half)
            signed = jnp.concatenate(signed_list, axis=1)
            score_grads = jnp.concatenate(score_grads_list, axis=1)
            sums[0:64, span] += nn(keys_t[:, key_span], score_grads)
            sums[64:128, key_span] += nt(queries[:, span], score_grads)
            sums[128:192, key_span] += nt(grads[:, span], signed)

        for half in range(2):
            start_half(0, half)

        @pl.loop(0, place)
        def _(number):
            step(number, False)

        step(place, True)

    width = sends[0].shape[1]
    for part in range(parts):
        span = slice(part * width, (part + 1) * width)
        for rows, factor in ((slice(0, 128), scale), (slice(128, 192), 1.0)):
            done = (sums[rows, span] * factor).astype(jnp.bfloat16)
            whole_ref[rows, span] = done
            sends[part][rows, :] = done


def join_kernel(*refs):
    pieces, weight_ref, out_ref, joined = refs[:-3], refs[-3], refs[-2], refs[-1]
    rows = pieces[0].shape[0]
    for number, piece in enumerate(pieces):
        joined[number * rows : (number + 1) * rows, :] = piece[...]

    @pl.loop(0, weight_ref.shape[0] // HALF)
    def _(tile):
        span = pl.ds(pl.multiple_of(tile * HALF, HALF), HALF)
        out_ref[:, span] = nn(weight_ref[span, : joined.shape[0]], joined[...]).T


def join_product(pieces, weight):
    rows, span = pieces[0].shape
    width = weight.shape[0]
    total = len(pieces) * rows
    return pl.pallas_call(
        join_kernel,
        out_shape=jax.ShapeDtypeStruct((span, width), jnp.float32),
        scratch_shapes=[pltpu.VMEM((total, span), jnp.bfloat16)],
        compiler_params=pltpu.CompilerParams(vmem_limit_bytes=62 << 20),
        cost_estimate=pl.CostEstimate(
            flops=2 * span * width * total, bytes_accessed=12_000_000, transcendentals=0
        ),
        name="join_product",
    )(*pieces, weight)


def make_table(block_order, length, ctx_index, ctx):
    here = block_order.shape[0] // ctx
    order = (ctx_index - jnp.arange(ctx)) % ctx
    places = block_order.reshape(ctx, here)[order].reshape(-1)
    return jnp.concatenate([jnp.argsort(places).astype(jnp.int32), length[None]])


def head_specs(parts, span, row):
    return [pl.BlockSpec((HEAD_DIM, span), lambda i, t, row=row: (row, 0)) for _ in range(parts)]


def pair_tables(block_order, length, ctx_index, ctx):
    here = block_order.shape[0] // ctx
    order = (ctx_index - jnp.arange(ctx)) % ctx
    places = block_order.reshape(ctx, here)[order].reshape(-1)
    blocks = places.shape[0]
    part = jnp.arange(blocks) // here
    query, key = places[:, None], places[None, :]
    seen = ((key <= query) & (key * BLK < length)).reshape(-1)
    masked = ((key == query) | ((key + 1) * BLK > length)).reshape(-1)
    newest = jnp.maximum(part[:, None], part[None, :]).reshape(-1)
    phase = jnp.maximum(newest, 1)
    pairs = jnp.arange(blocks * blocks, dtype=jnp.int32)
    tables = []
    for number in range(1, ctx):
        mine = seen & (phase == number)
        plain = mine & ~masked
        rank = jnp.where(plain, 0, jnp.where(mine, 1, 2)) * pairs.shape[0] + pairs
        slot = jnp.sum((rank[None, :] < rank[:, None]).astype(jnp.int32), axis=1)
        codes = jnp.sum(jnp.where(slot[:, None] == pairs[None, :], pairs[:, None], 0), axis=0)
        counts = jnp.stack([jnp.sum(plain.astype(jnp.int32)), jnp.sum(mine.astype(jnp.int32)), length])
        tables.append(jnp.concatenate([counts, places, codes]).astype(jnp.int32))
    return tables


def attend_early(table, heads, ctx, packed_list, state):
    parts, span = len(packed_list), packed_list[0].shape[1]
    slots = ctx * span
    shapes = [(heads, 1, slots), (heads, 1, slots), (heads, HEAD_DIM, slots)]
    whole = lambda shape: pl.BlockSpec(shape, lambda i, t: (0,) * len(shape))
    return pl.pallas_call(
        functools.partial(early_kernel, parts, heads, state is None),
        grid_spec=pltpu.PrefetchScalarGridSpec(
            num_scalar_prefetch=1,
            grid=(1,),
            in_specs=[whole(packed_list[0].shape)] * parts
            + ([] if state is None else [whole(shape) for shape in shapes]),
            out_specs=[whole(shape) for shape in shapes],
            scratch_shapes=[
                pltpu.VMEM((128, slots), jnp.bfloat16),
                pltpu.VMEM((slots, 128), jnp.bfloat16),
                pltpu.VMEM((HEAD_DIM, slots), jnp.bfloat16),
            ],
        ),
        out_shape=[jax.ShapeDtypeStruct(shape, jnp.float32) for shape in shapes],
        compiler_params=pltpu.CompilerParams(vmem_limit_bytes=62 << 20),
        cost_estimate=pl.CostEstimate(flops=20_000_000_000, bytes_accessed=4_000_000, transcendentals=0),
        name="attend_early",
    )(table, *packed_list, *([] if state is None else state))


def attend_last(table, head, packed_list, state):
    parts, span = len(packed_list), packed_list[0].shape[1]
    slots = parts * span
    whole = lambda shape: pl.BlockSpec(shape, lambda i, t: (0,) * len(shape))
    piece = lambda rows: pl.BlockSpec((1, rows, slots), lambda i, t: (head, 0, 0))
    return pl.pallas_call(
        functools.partial(last_kernel, parts),
        grid_spec=pltpu.PrefetchScalarGridSpec(
            num_scalar_prefetch=1,
            grid=(1,),
            in_specs=head_specs(parts, span, 3 * head)
            + head_specs(parts, span, 3 * head + 1)
            + head_specs(parts, span, 3 * head + 2)
            + [piece(1), piece(1), piece(HEAD_DIM)],
            out_specs=[whole((HEAD_DIM, span))] * parts + [whole((HEAD_DIM, slots)), whole((1, slots))],
            scratch_shapes=[
                pltpu.VMEM((128, slots), jnp.bfloat16),
                pltpu.VMEM((slots, 128), jnp.bfloat16),
                pltpu.VMEM((HEAD_DIM, slots), jnp.bfloat16),
                pltpu.VMEM((1, slots), jnp.float32),
                pltpu.VMEM((1, slots), jnp.float32),
            ],
        ),
        out_shape=[jax.ShapeDtypeStruct((HEAD_DIM, span), jnp.bfloat16)] * parts
        + [
            jax.ShapeDtypeStruct((HEAD_DIM, slots), jnp.float32),
            jax.ShapeDtypeStruct((1, slots), jnp.float32),
        ],
        compiler_params=pltpu.CompilerParams(vmem_limit_bytes=62 << 20),
        cost_estimate=pl.CostEstimate(flops=10_000_000_000, bytes_accessed=4_000_000, transcendentals=0),
        name="attend_last",
    )(table, *packed_list, *packed_list, *packed_list, *state)


def attend_backward(table, head, packed_list, grad_list, exact, logs):
    parts, span = len(packed_list), packed_list[0].shape[1]
    slots = parts * span
    whole = lambda shape: pl.BlockSpec(shape, lambda i, t: (0, 0))
    three = 3 * HEAD_DIM
    return pl.pallas_call(
        functools.partial(backward_kernel, parts),
        grid_spec=pltpu.PrefetchScalarGridSpec(
            num_scalar_prefetch=1,
            grid=(1,),
            in_specs=head_specs(parts, span, 3 * head)
            + head_specs(parts, span, 3 * head + 1)
            + head_specs(parts, span, 3 * head + 2)
            + head_specs(parts, span, max(head - 1, 0))
            + [whole((HEAD_DIM, slots)), whole((1, slots))],
            out_specs=[whole((three, span))] * parts + [whole((three, slots))],
            scratch_shapes=[pltpu.VMEM((HEAD_DIM, slots), jnp.bfloat16)] * 4
            + [pltpu.VMEM((slots, 128), jnp.bfloat16)] * 2
            + [
                pltpu.VMEM((three, slots), jnp.float32),
                pltpu.VMEM((128, BLK), jnp.bfloat16),
                pltpu.VMEM((128, BLK), jnp.bfloat16),
                pltpu.VMEM((1, BLK), jnp.float32),
                pltpu.VMEM((2, BLK, HALF), jnp.float32),
                pltpu.VMEM((2, BLK, HALF), jnp.float32),
            ],
        ),
        out_shape=[jax.ShapeDtypeStruct((three, span), jnp.bfloat16)] * parts
        + [jax.ShapeDtypeStruct((three, slots), jnp.bfloat16)],
        compiler_params=pltpu.CompilerParams(vmem_limit_bytes=62 << 20),
        cost_estimate=pl.CostEstimate(flops=40_000_000_000, bytes_accessed=6_000_000, transcendentals=0),
        name="attend_backward",
    )(table, *packed_list, *packed_list, *packed_list, *grad_list, exact, logs)


def layer_norm(values, gain):
    centre = jnp.mean(values, axis=-1, keepdims=True)
    centred = values - centre
    spread = jnp.mean(centred * centred, axis=-1, keepdims=True)
    return centred * lax.rsqrt(spread + 1e-05) * gain


def gelu_tanh(values):
    return jax.nn.gelu(values, approximate=True)


def product(equation, left, right):
    return jnp.einsum(equation, left, right, preferred_element_type=jnp.float32)


def shift(array, ctx, by):
    if by % ctx == 0:
        return array
    return lax.ppermute(array, "ctx", [(i, (i + by) % ctx) for i in range(ctx)])


def turned(array, axis, by):
    return lax.dynamic_slice_in_dim(
        jnp.concatenate([array, array], axis=axis), by, array.shape[axis], axis
    )


def gather_rows(array):
    return lax.all_gather(array, "fsdp", axis=0, tiled=True)


def scatter_rows(array):
    return lax.psum_scatter(
        array.astype(jnp.bfloat16), "fsdp", scatter_dimension=0, tiled=True
    )


def scatter_pairs(array, fsdp):
    me = lax.axis_index("fsdp")
    core, chip = me % 2, me // 2
    parts = array.reshape(fsdp // 2, 2, array.shape[0] // fsdp, array.shape[1])
    kept = lax.dynamic_index_in_dim(parts, core, 1, keepdims=False)
    sent = lax.dynamic_index_in_dim(parts, 1 - core, 1, keepdims=False).astype(jnp.bfloat16)
    got = lax.ppermute(sent, "fsdp", [(i, i ^ 1) for i in range(fsdp)])
    kept = kept.astype(jnp.float32) + got.astype(jnp.float32)
    total = lax.dynamic_index_in_dim(kept, chip, 0, keepdims=False)
    narrow = kept.astype(jnp.bfloat16)
    for other in range(1, fsdp // 2):
        sent = lax.dynamic_index_in_dim(narrow, chip ^ other, 0, keepdims=False)
        got = lax.ppermute(sent, "fsdp", [(i, i ^ (2 * other)) for i in range(fsdp)])
        total += got.astype(jnp.float32)
    return total


def per_device(
    ctx, fsdp, tokens_in, out_grad, gain_attn, gain_mlp, w_qkv, w_out, w_up, w_down, lengths, block_order
):
    local_rows, width = tokens_in.shape[1:]
    tokens_in, out_grad, length, block_order = tokens_in[0], out_grad[0], lengths[0], block_order[0]
    ctx_index = lax.axis_index("ctx")
    heads_here = width // HEAD_DIM // ctx
    own = heads_here * HEAD_DIM
    table = make_table(block_order, length, ctx_index, ctx)

    gains = jnp.stack([gain_attn, gain_mlp], axis=1)
    gains = jnp.pad(gains, ((0, 0), (0, 126)))
    ordered = w_qkv.reshape(-1, 3, ctx, heads_here, HEAD_DIM).transpose(0, 2, 3, 1, 4)
    ordered = turned(ordered.reshape(-1, ctx, 3 * own), 1, ctx_index).reshape(w_qkv.shape)
    first = gather_rows(jnp.concatenate([ordered, gains], axis=1))
    gain_one = first[:, 3 * width].astype(jnp.float32)
    gain_two = first[:, 3 * width + 1].astype(jnp.float32)
    w_out_all = gather_rows(w_out)
    w_up_all = gather_rows(w_up)
    w_down_all = gather_rows(w_down)
    w_own = first[:, : 3 * own]
    w_out_turned = turned(w_out_all.reshape(ctx, heads_here, HEAD_DIM, width), 0, ctx_index)
    w_out_turned = w_out_turned.transpose(1, 0, 2, 3).reshape(width, width)

    here = local_rows // BLK
    places = lax.dynamic_slice_in_dim(block_order, ctx_index * here, here)
    places = (places[:, None] * BLK + jnp.arange(BLK, dtype=jnp.int32)[None]).reshape(-1)
    grad_z = out_grad * (places < length).astype(jnp.bfloat16)[:, None]

    tables = pair_tables(block_order, length, ctx_index, ctx)
    normed_list, packed_list = [], []
    tokens, state = tokens_in, None
    for part in range(ctx):
        here_tokens, gain_here, state = lax.optimization_barrier((tokens, gain_one, state))
        normed = layer_norm(here_tokens.astype(jnp.float32), gain_here).astype(jnp.bfloat16)
        normed_list.append(normed)
        packed_list.append(product("jn,uj->nu", w_own, normed).astype(jnp.bfloat16))
        if 0 < part < ctx - 1:
            state = attend_early(tables[part - 1], heads_here, ctx, packed_list, state)
        if part == 1:
            tokens, grad_z, tables = lax.optimization_barrier((tokens, grad_z, tables))
        if part < ctx - 1:
            tokens = shift(tokens, ctx, 1)
    kept, mixed_parts = [], []
    for head in range(heads_here):
        results = attend_last(tables[-1], head, packed_list, state)
        kept.append((results[ctx], results[ctx + 1]))
        mixed_parts += [shift(results[part], ctx, -part) for part in range(ctx)]
    mixed_t = jnp.concatenate(mixed_parts, axis=0)

    tokens_f = tokens_in.astype(jnp.float32)
    middle = tokens_f + product("nu,nj->uj", mixed_t, w_out_turned)
    normed_two, norm_two_back = jax.vjp(lambda v: layer_norm(v, gain_two), middle)
    normed_two = normed_two.astype(jnp.bfloat16)
    pre_act = product("uj,jn->un", normed_two, w_up_all)
    activation, gelu_back = jax.vjp(gelu_tanh, pre_act)
    activation = activation.astype(jnp.bfloat16)
    result = (middle + product("un,nj->uj", activation, w_down_all)).astype(jnp.bfloat16)

    grad_act = product("uj,nj->un", grad_z, w_down_all)
    grad_pre = gelu_back(grad_act)[0].astype(jnp.bfloat16)
    grad_normed_two = product("un,jn->uj", grad_pre, w_up_all)
    grad_middle = grad_z.astype(jnp.float32) + norm_two_back(grad_normed_two)[0]
    grad_branch = grad_middle.astype(jnp.bfloat16)
    grad_mixed_t = product("nj,uj->nu", w_out_turned, grad_branch).astype(jnp.bfloat16)
    count = ctx * HEAD_DIM
    grads_by_head = [[] for _ in range(heads_here)]
    for part in range(ctx):
        rows = [head * count + part * HEAD_DIM for head in range(heads_here)]
        pieces = [grad_mixed_t[row : row + HEAD_DIM] for row in rows]
        grads_by_head[0].append(shift(pieces[0], ctx, part))
        others = shift(jnp.concatenate(pieces[1:], axis=0), ctx, part)
        for head in range(1, heads_here):
            grads_by_head[head].append(others)

    grad_w_down = product("un,uj->nj", activation, grad_z).astype(jnp.bfloat16)
    grad_w_up = product("uj,un->jn", normed_two, grad_pre).astype(jnp.bfloat16)
    grad_w_out = product("nu,uj->nj", mixed_t, grad_branch).astype(jnp.bfloat16)
    grad_w_out = turned(
        grad_w_out.reshape(heads_here, ctx, HEAD_DIM, width).transpose(1, 0, 2, 3), 0, (ctx - ctx_index) % ctx
    )
    grad_w_down = scatter_rows(grad_w_down)
    grad_up_out = scatter_rows(
        jnp.concatenate([grad_w_up, grad_w_out.reshape(width, width)], axis=1)
    )

    grad_parts, grad_whole = [], []
    for head in range(heads_here):
        if head == max(heads_here - 2, 0):
            grad_up_out, grad_w_down, table = lax.optimization_barrier(
                (grad_up_out, grad_w_down, table)
            )
            grad_up_out, grad_w_down = lax.psum((grad_up_out, grad_w_down), "ctx")
        results = attend_backward(table, head, packed_list, grads_by_head[head], *kept[head])
        grad_parts.append([shift(results[part], ctx, -part) for part in range(ctx)])
        grad_whole.append(results[ctx])
    normed_all = jnp.concatenate(normed_list, axis=0)
    grad_qkv_own = product("uj,nu->jn", normed_all, jnp.concatenate(grad_whole, axis=0))
    grad_qkv_own = scatter_pairs(grad_qkv_own, fsdp).astype(jnp.bfloat16)
    grad_qkv = [shift(grad_qkv_own, ctx, -part) for part in range(ctx)]
    grad_qkv = turned(jnp.stack(grad_qkv), 0, (ctx - ctx_index) % ctx)
    rows_here = grad_qkv.shape[1]
    grad_qkv = grad_qkv.reshape(ctx, rows_here, heads_here, 3, HEAD_DIM)
    grad_w_qkv = grad_qkv.transpose(1, 3, 0, 2, 4).reshape(rows_here, 3 * width).astype(jnp.float32)

    grad_normed_one = join_product([grad_parts[head][part] for part in range(ctx) for head in range(heads_here)], first)
    norm_one_back = jax.vjp(lambda v: layer_norm(v, gain_one), tokens_f)[1]
    grad_tokens = (grad_middle + norm_one_back(grad_normed_one)[0]).astype(jnp.bfloat16)

    grad_w_down = grad_w_down.astype(jnp.float32)
    grad_w_up = grad_up_out[:, : w_up.shape[1]].astype(jnp.float32)
    grad_w_out = grad_up_out[:, w_up.shape[1] :].astype(jnp.float32)

    def gain_grad(grad_weight, weight, gain):
        total = jnp.sum(grad_weight * weight.astype(jnp.float32), axis=1)
        return total / gain.astype(jnp.float32)

    return (
        result[None],
        grad_tokens[None],
        gain_grad(grad_w_qkv, w_qkv, gain_attn),
        gain_grad(grad_w_up, w_up, gain_mlp),
        grad_w_qkv,
        grad_w_out,
        grad_w_up,
        grad_w_down,
    )


def solution(mesh):
    rows = P("fsdp", None)
    whole = P("fsdp", "ctx", None)
    ctx, fsdp = mesh.shape["ctx"], mesh.shape["fsdp"]

    def layer(*arrays):
        return per_device(ctx, fsdp, *arrays)

    return jax.shard_map(
        layer,
        mesh=mesh,
        in_specs=(whole, whole, P("fsdp"), P("fsdp"), rows, rows, rows, rows, P("fsdp"), rows),
        out_specs=(whole, whole, P("fsdp"), P("fsdp"), rows, rows, rows, rows),
        check_vma=False,
    )
```

```python
import functools

import jax
import jax.numpy as jnp
from jax import lax
from jax.experimental import pallas as pl
from jax.experimental.pallas import tpu as pltpu
from jax.sharding import PartitionSpec as P


HEAD_DIM = 64
BLK = 512
HALF = 256
LOG2E = 1.4426950408889634
BIG = 3e38
LOW = -1e30


def nn(left, right):
    return lax.dot_general(left, right, (((1,), (0,)), ((), ())), preferred_element_type=jnp.float32)


def nt(left, right):
    return lax.dot_general(left, right, (((1,), (1,)), ((), ())), preferred_element_type=jnp.float32)


def sign_of(scores):
    return jnp.clip(scores.astype(jnp.bfloat16) * jnp.bfloat16(BIG), -1.0, 1.0).astype(jnp.bfloat16)


def block_mask(key_start, query_start, length, shape):
    keys = key_start + lax.broadcasted_iota(jnp.int32, shape, 0)
    queries = query_start + lax.broadcasted_iota(jnp.int32, shape, 1)
    return keys <= jnp.minimum(queries, length - 1)


def gather_columns(refs, out):
    span = refs[0].shape[1]
    for part, ref in enumerate(refs):
        out[:, part * span : (part + 1) * span] = ref[...]


def turn_rows(source, out, twice):
    for part in range(source.shape[1] // BLK):
        span = slice(part * BLK, (part + 1) * BLK)
        piece = source[:, span]
        out[span, :] = jnp.concatenate([piece, piece if twice else jnp.zeros_like(piece)], axis=0).T


def query_weights(query_t):
    scaled = query_t.astype(jnp.float32) * (LOG2E * HEAD_DIM ** -0.5)
    high = scaled.astype(jnp.bfloat16)
    return jnp.concatenate([high, (scaled - high.astype(jnp.float32)).astype(jnp.bfloat16)], axis=0)


def pair_step(table, index, masked, weights, keys, values, top_ref, total_ref, mixed_ref):
    blocks = keys.shape[0] // BLK
    code = table[3 + blocks + index]
    query_block, key_block = code // blocks, code % blocks
    key_span = pl.ds(pl.multiple_of(key_block * BLK, BLK), BLK)
    key_rows, value_rows = keys[key_span, :], values[:, key_span]
    spans = [
        pl.ds(pl.multiple_of(query_block * BLK + half * HALF, HALF), HALF) for half in range(2)
    ]
    scores_list = [nn(key_rows, weights[:, span]) for span in spans]
    for half in range(2):
        span, scores = spans[half], scores_list[half]
        top = top_ref[:, span]
        size = jnp.abs(scores)
        if masked:
            key_start = table[3 + key_block] * BLK
            query_start = table[3 + query_block] * BLK + half * HALF
            size = jnp.where(block_mask(key_start, query_start, table[2], size.shape), size, LOW)
        new_top = jnp.maximum(top, jnp.max(size, axis=0, keepdims=True))
        fade = jnp.exp2(top - new_top)
        powers = jnp.exp2(size - new_top)
        signed = powers.astype(jnp.bfloat16) * sign_of(scores)
        top_ref[:, span] = new_top
        total_ref[:, span] = total_ref[:, span] * fade + jnp.sum(powers, axis=0, keepdims=True)
        mixed_ref[:, span] = mixed_ref[:, span] * fade + nn(value_rows, signed)


def run_pairs(table, *refs):
    @pl.loop(0, table[0])
    def _(index):
        pair_step(table, index, False, *refs)

    @pl.loop(table[0], table[1])
    def _(index):
        pair_step(table, index, True, *refs)


def load_head_part(part, query_ref, key_ref, value_ref, weights, keys, values):
    width = query_ref.shape[1]
    span = slice(part * width, (part + 1) * width)
    weights[:, span] = query_weights(query_ref[...])
    key_rows = key_ref[...]
    for start in range(0, width, BLK):
        piece = key_rows[:, start : start + BLK]
        rows = slice(part * width + start, part * width + start + BLK)
        keys[rows, :] = jnp.concatenate([piece, piece], axis=0).T
    values[:, span] = value_ref[...]


def early_kernel(parts, heads, first, table, *refs):
    packed_refs, refs = refs[:parts], refs[parts:]
    if not first:
        before, refs = refs[:3], refs[3:]
    top_ref, total_ref, mixed_ref, weights, keys, values = refs

    @pl.loop(0, heads)
    def _(head):
        def rows_of(kind):
            return pl.ds(pl.multiple_of((3 * head + kind) * HEAD_DIM, HEAD_DIM), HEAD_DIM)

        for part, ref in enumerate(packed_refs):
            three = [ref.at[rows_of(kind), :] for kind in range(3)]
            load_head_part(part, *three, weights, keys, values)
        state = (top_ref.at[head], total_ref.at[head], mixed_ref.at[head])
        if first:
            for ref, value in zip(state, (LOW, 0.0, 0.0)):
                ref[...] = jnp.full(ref.shape, value, jnp.float32)
        else:
            for ref, old in zip(state, before):
                ref[...] = old[head]
        run_pairs(table, weights, keys, values, *state)


def last_kernel(parts, table, *refs):
    query_refs, key_refs, value_refs = refs[:parts], refs[parts : 2 * parts], refs[2 * parts : 3 * parts]
    before, refs = refs[3 * parts : 3 * parts + 3], refs[3 * parts + 3 :]
    sends, refs = refs[:parts], refs[parts:]
    exact_ref, log_ref, weights, keys, values, top_ref, total_ref = refs
    for part in range(parts):
        load_head_part(part, query_refs[part], key_refs[part], value_refs[part], weights, keys, values)
    top_ref[...] = before[0][0]
    total_ref[...] = before[1][0]
    exact_ref[...] = before[2][0]
    run_pairs(table, weights, keys, values, top_ref, total_ref, exact_ref)
    log_ref[...] = top_ref[...] + jnp.log2(total_ref[...])
    width = sends[0].shape[1]
    for part in range(parts):
        span = slice(part * width, (part + 1) * width)
        done = exact_ref[:, span] / total_ref[:, span]
        exact_ref[:, span] = done
        sends[part][...] = done.astype(jnp.bfloat16)


def backward_kernel(parts, table, *refs):
    query_refs, key_refs, value_refs = refs[:parts], refs[parts : 2 * parts], refs[2 * parts : 3 * parts]
    grad_refs, refs = refs[3 * parts : 4 * parts], refs[4 * parts :]
    exact_ref, log_ref, sends, refs = refs[0], refs[1], refs[2 : 2 + parts], refs[2 + parts :]
    whole_ref, queries, keys_t, values_t, grads, keys, values, sums, weights, grad_weights, dots, scores_ref, inner_ref = refs
    blocks = queries.shape[1] // BLK
    length = table[blocks]
    scale = HEAD_DIM ** -0.5
    gather_columns(query_refs, queries)
    gather_columns(key_refs, keys_t)
    gather_columns(value_refs, values_t)
    gather_columns(grad_refs, grads)
    turn_rows(keys_t, keys, True)
    turn_rows(values_t, values, False)
    sums[...] = jnp.zeros_like(sums)
    grad_weights[...] = jnp.zeros_like(grad_weights)
    full = (length + BLK - 1) // BLK

    @pl.loop(0, full)
    def _(place):
        span = pl.ds(pl.multiple_of(table[place] * BLK, BLK), BLK)
        weights[...] = query_weights(queries[:, span])
        grad_t = grads[:, span]
        grad_weights[:HEAD_DIM, :] = grad_t
        dots[...] = jnp.sum(grad_t.astype(jnp.float32) * exact_ref[:, span], axis=0, keepdims=True)

        halves = [slice(h * HALF, (h + 1) * HALF) for h in range(2)]

        def start_half(number, half):
            key_span = pl.ds(pl.multiple_of(table[number] * BLK, BLK), BLK)
            scores_ref[half] = nn(keys[key_span, :], weights[:, halves[half]])
            inner_ref[half] = nn(values[key_span, :], grad_weights[:, halves[half]])

        def step(number, masked):
            key_span = pl.ds(pl.multiple_of(table[number] * BLK, BLK), BLK)
            signed_list, score_grads_list = [], []
            for half in range(2):
                scores = scores_ref[half]
                log_row = log_ref[:, pl.ds(pl.multiple_of(table[place] * BLK + half * HALF, HALF), HALF)]
                size = jnp.abs(scores) - log_row
                if masked:
                    mask = block_mask(number * BLK, place * BLK + half * HALF, length, size.shape)
                    size = jnp.where(mask, size, LOW)
                positive = jnp.exp2(size).astype(jnp.bfloat16)
                sign = sign_of(scores)
                signed_list.append(positive * sign)
                dot_row = dots[:, halves[half]].astype(jnp.bfloat16)
                inner = inner_ref[half].astype(jnp.bfloat16) - dot_row * sign
                score_grads_list.append(positive * inner)
                if not masked:
                    start_half(number + 1, half)
            signed = jnp.concatenate(signed_list, axis=1)
            score_grads = jnp.concatenate(score_grads_list, axis=1)
            sums[0:64, span] += nn(keys_t[:, key_span], score_grads)
            sums[64:128, key_span] += nt(queries[:, span], score_grads)
            sums[128:192, key_span] += nt(grads[:, span], signed)

        for half in range(2):
            start_half(0, half)

        @pl.loop(0, place)
        def _(number):
            step(number, False)

        step(place, True)

    width = sends[0].shape[1]
    for part in range(parts):
        span = slice(part * width, (part + 1) * width)
        for rows, factor in ((slice(0, 128), scale), (slice(128, 192), 1.0)):
            done = (sums[rows, span] * factor).astype(jnp.bfloat16)
            whole_ref[rows, span] = done
            sends[part][rows, :] = done


def join_kernel(*refs):
    pieces, weight_ref, out_ref, joined = refs[:-3], refs[-3], refs[-2], refs[-1]
    rows = pieces[0].shape[0]
    for number, piece in enumerate(pieces):
        joined[number * rows : (number + 1) * rows, :] = piece[...]

    @pl.loop(0, weight_ref.shape[0] // HALF)
    def _(tile):
        span = pl.ds(pl.multiple_of(tile * HALF, HALF), HALF)
        out_ref[:, span] = nn(weight_ref[span, : joined.shape[0]], joined[...]).T


def join_product(pieces, weight):
    rows, span = pieces[0].shape
    width = weight.shape[0]
    total = len(pieces) * rows
    return pl.pallas_call(
        join_kernel,
        out_shape=jax.ShapeDtypeStruct((span, width), jnp.float32),
        scratch_shapes=[pltpu.VMEM((total, span), jnp.bfloat16)],
        compiler_params=pltpu.CompilerParams(vmem_limit_bytes=48 << 20),
        cost_estimate=pl.CostEstimate(
            flops=2 * span * width * total, bytes_accessed=12_000_000, transcendentals=0
        ),
        name="join_product",
    )(*pieces, weight)


def make_table(block_order, length, ctx_index, ctx):
    here = block_order.shape[0] // ctx
    order = (ctx_index - jnp.arange(ctx)) % ctx
    places = block_order.reshape(ctx, here)[order].reshape(-1)
    return jnp.concatenate([jnp.argsort(places).astype(jnp.int32), length[None]])


def head_specs(parts, span, row):
    return [pl.BlockSpec((HEAD_DIM, span), lambda i, t, row=row: (row, 0)) for _ in range(parts)]


def pair_tables(block_order, length, ctx_index, ctx):
    here = block_order.shape[0] // ctx
    order = (ctx_index - jnp.arange(ctx)) % ctx
    places = block_order.reshape(ctx, here)[order].reshape(-1)
    blocks = places.shape[0]
    part = jnp.arange(blocks) // here
    query, key = places[:, None], places[None, :]
    seen = ((key <= query) & (key * BLK < length)).reshape(-1)
    masked = ((key == query) | ((key + 1) * BLK > length)).reshape(-1)
    newest = jnp.maximum(part[:, None], part[None, :]).reshape(-1)
    phase = jnp.maximum(newest, 1)
    pairs = jnp.arange(blocks * blocks, dtype=jnp.int32)
    tables = []
    for number in range(1, ctx):
        mine = seen & (phase == number)
        plain = mine & ~masked
        rank = jnp.where(plain, 0, jnp.where(mine, 1, 2)) * pairs.shape[0] + pairs
        slot = jnp.sum((rank[None, :] < rank[:, None]).astype(jnp.int32), axis=1)
        codes = jnp.sum(jnp.where(slot[:, None] == pairs[None, :], pairs[:, None], 0), axis=0)
        counts = jnp.stack([jnp.sum(plain.astype(jnp.int32)), jnp.sum(mine.astype(jnp.int32)), length])
        tables.append(jnp.concatenate([counts, places, codes]).astype(jnp.int32))
    return tables


def attend_early(table, heads, ctx, packed_list, state):
    parts, span = len(packed_list), packed_list[0].shape[1]
    slots = ctx * span
    shapes = [(heads, 1, slots), (heads, 1, slots), (heads, HEAD_DIM, slots)]
    whole = lambda shape: pl.BlockSpec(shape, lambda i, t: (0,) * len(shape))
    return pl.pallas_call(
        functools.partial(early_kernel, parts, heads, state is None),
        grid_spec=pltpu.PrefetchScalarGridSpec(
            num_scalar_prefetch=1,
            grid=(1,),
            in_specs=[whole(packed_list[0].shape)] * parts
            + ([] if state is None else [whole(shape) for shape in shapes]),
            out_specs=[whole(shape) for shape in shapes],
            scratch_shapes=[
                pltpu.VMEM((128, slots), jnp.bfloat16),
                pltpu.VMEM((slots, 128), jnp.bfloat16),
                pltpu.VMEM((HEAD_DIM, slots), jnp.bfloat16),
            ],
        ),
        out_shape=[jax.ShapeDtypeStruct(shape, jnp.float32) for shape in shapes],
        compiler_params=pltpu.CompilerParams(vmem_limit_bytes=48 << 20),
        cost_estimate=pl.CostEstimate(flops=20_000_000_000, bytes_accessed=4_000_000, transcendentals=0),
        name="attend_early",
    )(table, *packed_list, *([] if state is None else state))


def attend_last(table, head, packed_list, state):
    parts, span = len(packed_list), packed_list[0].shape[1]
    slots = parts * span
    whole = lambda shape: pl.BlockSpec(shape, lambda i, t: (0,) * len(shape))
    piece = lambda rows: pl.BlockSpec((1, rows, slots), lambda i, t: (head, 0, 0))
    return pl.pallas_call(
        functools.partial(last_kernel, parts),
        grid_spec=pltpu.PrefetchScalarGridSpec(
            num_scalar_prefetch=1,
            grid=(1,),
            in_specs=head_specs(parts, span, 3 * head)
            + head_specs(parts, span, 3 * head + 1)
            + head_specs(parts, span, 3 * head + 2)
            + [piece(1), piece(1), piece(HEAD_DIM)],
            out_specs=[whole((HEAD_DIM, span))] * parts + [whole((HEAD_DIM, slots)), whole((1, slots))],
            scratch_shapes=[
                pltpu.VMEM((128, slots), jnp.bfloat16),
                pltpu.VMEM((slots, 128), jnp.bfloat16),
                pltpu.VMEM((HEAD_DIM, slots), jnp.bfloat16),
                pltpu.VMEM((1, slots), jnp.float32),
                pltpu.VMEM((1, slots), jnp.float32),
            ],
        ),
        out_shape=[jax.ShapeDtypeStruct((HEAD_DIM, span), jnp.bfloat16)] * parts
        + [
            jax.ShapeDtypeStruct((HEAD_DIM, slots), jnp.float32),
            jax.ShapeDtypeStruct((1, slots), jnp.float32),
        ],
        compiler_params=pltpu.CompilerParams(vmem_limit_bytes=40 << 20),
        cost_estimate=pl.CostEstimate(flops=10_000_000_000, bytes_accessed=4_000_000, transcendentals=0),
        name="attend_last",
    )(table, *packed_list, *packed_list, *packed_list, *state)


def attend_backward(table, head, packed_list, grad_list, exact, logs):
    parts, span = len(packed_list), packed_list[0].shape[1]
    slots = parts * span
    whole = lambda shape: pl.BlockSpec(shape, lambda i, t: (0, 0))
    three = 3 * HEAD_DIM
    return pl.pallas_call(
        functools.partial(backward_kernel, parts),
        grid_spec=pltpu.PrefetchScalarGridSpec(
            num_scalar_prefetch=1,
            grid=(1,),
            in_specs=head_specs(parts, span, 3 * head)
            + head_specs(parts, span, 3 * head + 1)
            + head_specs(parts, span, 3 * head + 2)
            + head_specs(parts, span, max(head - 1, 0))
            + [whole((HEAD_DIM, slots)), whole((1, slots))],
            out_specs=[whole((three, span))] * parts + [whole((three, slots))],
            scratch_shapes=[pltpu.VMEM((HEAD_DIM, slots), jnp.bfloat16)] * 4
            + [pltpu.VMEM((slots, 128), jnp.bfloat16)] * 2
            + [
                pltpu.VMEM((three, slots), jnp.float32),
                pltpu.VMEM((128, BLK), jnp.bfloat16),
                pltpu.VMEM((128, BLK), jnp.bfloat16),
                pltpu.VMEM((1, BLK), jnp.float32),
                pltpu.VMEM((2, BLK, HALF), jnp.float32),
                pltpu.VMEM((2, BLK, HALF), jnp.float32),
            ],
        ),
        out_shape=[jax.ShapeDtypeStruct((three, span), jnp.bfloat16)] * parts
        + [jax.ShapeDtypeStruct((three, slots), jnp.bfloat16)],
        compiler_params=pltpu.CompilerParams(vmem_limit_bytes=40 << 20),
        cost_estimate=pl.CostEstimate(flops=40_000_000_000, bytes_accessed=6_000_000, transcendentals=0),
        name="attend_backward",
    )(table, *packed_list, *packed_list, *packed_list, *grad_list, exact, logs)


def layer_norm(values, gain):
    centre = jnp.mean(values, axis=-1, keepdims=True)
    centred = values - centre
    spread = jnp.mean(centred * centred, axis=-1, keepdims=True)
    return centred * lax.rsqrt(spread + 1e-05) * gain


def gelu_tanh(values):
    return jax.nn.gelu(values, approximate=True)


def product(equation, left, right):
    return jnp.einsum(equation, left, right, preferred_element_type=jnp.float32)


def shift(array, ctx, by):
    if by % ctx == 0:
        return array
    return lax.ppermute(array, "ctx", [(i, (i + by) % ctx) for i in range(ctx)])


def turned(array, axis, by):
    return lax.dynamic_slice_in_dim(
        jnp.concatenate([array, array], axis=axis), by, array.shape[axis], axis
    )


def gather_rows(array):
    return lax.all_gather(array, "fsdp", axis=0, tiled=True)


def scatter_rows(array):
    return lax.psum_scatter(
        array.astype(jnp.bfloat16), "fsdp", scatter_dimension=0, tiled=True
    )


def scatter_pairs(array, fsdp):
    me = lax.axis_index("fsdp")
    core, chip = me % 2, me // 2
    parts = array.reshape(fsdp // 2, 2, array.shape[0] // fsdp, array.shape[1])
    kept = lax.dynamic_index_in_dim(parts, core, 1, keepdims=False)
    sent = lax.dynamic_index_in_dim(parts, 1 - core, 1, keepdims=False).astype(jnp.bfloat16)
    got = lax.ppermute(sent, "fsdp", [(i, i ^ 1) for i in range(fsdp)])
    kept = kept.astype(jnp.float32) + got.astype(jnp.float32)
    total = lax.dynamic_index_in_dim(kept, chip, 0, keepdims=False)
    narrow = kept.astype(jnp.bfloat16)
    for other in range(1, fsdp // 2):
        sent = lax.dynamic_index_in_dim(narrow, chip ^ other, 0, keepdims=False)
        got = lax.ppermute(sent, "fsdp", [(i, i ^ (2 * other)) for i in range(fsdp)])
        total += got.astype(jnp.float32)
    return total


def per_device(
    ctx, fsdp, tokens_in, out_grad, gain_attn, gain_mlp, w_qkv, w_out, w_up, w_down, lengths, block_order
):
    local_rows, width = tokens_in.shape[1:]
    tokens_in, out_grad, length, block_order = tokens_in[0], out_grad[0], lengths[0], block_order[0]
    ctx_index = lax.axis_index("ctx")
    heads_here = width // HEAD_DIM // ctx
    own = heads_here * HEAD_DIM
    table = make_table(block_order, length, ctx_index, ctx)

    gains = jnp.stack([gain_attn, gain_mlp], axis=1)
    gains = jnp.pad(gains, ((0, 0), (0, 126)))
    ordered = w_qkv.reshape(-1, 3, ctx, heads_here, HEAD_DIM).transpose(0, 2, 3, 1, 4)
    ordered = turned(ordered.reshape(-1, ctx, 3 * own), 1, ctx_index).reshape(w_qkv.shape)
    first = gather_rows(jnp.concatenate([ordered, gains], axis=1))
    gain_one = first[:, 3 * width].astype(jnp.float32)
    gain_two = first[:, 3 * width + 1].astype(jnp.float32)
    w_out_all = gather_rows(w_out)
    w_up_all = gather_rows(w_up)
    w_down_all = gather_rows(w_down)
    w_own = first[:, : 3 * own]
    w_out_turned = turned(w_out_all.reshape(ctx, heads_here, HEAD_DIM, width), 0, ctx_index)
    w_out_turned = w_out_turned.transpose(1, 0, 2, 3).reshape(width, width)

    here = local_rows // BLK
    places = lax.dynamic_slice_in_dim(block_order, ctx_index * here, here)
    places = (places[:, None] * BLK + jnp.arange(BLK, dtype=jnp.int32)[None]).reshape(-1)
    grad_z = out_grad * (places < length).astype(jnp.bfloat16)[:, None]

    tables = pair_tables(block_order, length, ctx_index, ctx)
    normed_list, packed_list = [], []
    tokens, state = tokens_in, None
    for part in range(ctx):
        here_tokens, gain_here, state = lax.optimization_barrier((tokens, gain_one, state))
        normed = layer_norm(here_tokens.astype(jnp.float32), gain_here).astype(jnp.bfloat16)
        normed_list.append(normed)
        packed_list.append(product("jn,uj->nu", w_own, normed).astype(jnp.bfloat16))
        if 0 < part < ctx - 1:
            state = attend_early(tables[part - 1], heads_here, ctx, packed_list, state)
        if part == 1:
            tokens, grad_z, tables = lax.optimization_barrier((tokens, grad_z, tables))
        if part < ctx - 1:
            tokens = shift(tokens, ctx, 1)
    kept, mixed_parts = [], []
    for head in range(heads_here):
        results = attend_last(tables[-1], head, packed_list, state)
        kept.append((results[ctx], results[ctx + 1]))
        mixed_parts += [shift(results[part], ctx, -part) for part in range(ctx)]
    mixed_t = jnp.concatenate(mixed_parts, axis=0)

    tokens_f = tokens_in.astype(jnp.float32)
    middle = tokens_f + product("nu,nj->uj", mixed_t, w_out_turned)
    normed_two, norm_two_back = jax.vjp(lambda v: layer_norm(v, gain_two), middle)
    normed_two = normed_two.astype(jnp.bfloat16)
    pre_act = product("uj,jn->un", normed_two, w_up_all)
    activation, gelu_back = jax.vjp(gelu_tanh, pre_act)
    activation = activation.astype(jnp.bfloat16)
    result = (middle + product("un,nj->uj", activation, w_down_all)).astype(jnp.bfloat16)

    grad_act = product("uj,nj->un", grad_z, w_down_all)
    grad_pre = gelu_back(grad_act)[0].astype(jnp.bfloat16)
    grad_normed_two = product("un,jn->uj", grad_pre, w_up_all)
    grad_middle = grad_z.astype(jnp.float32) + norm_two_back(grad_normed_two)[0]
    grad_branch = grad_middle.astype(jnp.bfloat16)
    grad_mixed_t = product("nj,uj->nu", w_out_turned, grad_branch).astype(jnp.bfloat16)
    count = ctx * HEAD_DIM
    grads_by_head = [[] for _ in range(heads_here)]
    for part in range(ctx):
        rows = [head * count + part * HEAD_DIM for head in range(heads_here)]
        pieces = [grad_mixed_t[row : row + HEAD_DIM] for row in rows]
        grads_by_head[0].append(shift(pieces[0], ctx, part))
        others = shift(jnp.concatenate(pieces[1:], axis=0), ctx, part)
        for head in range(1, heads_here):
            grads_by_head[head].append(others)

    grad_w_down = product("un,uj->nj", activation, grad_z).astype(jnp.bfloat16)
    grad_w_up = product("uj,un->jn", normed_two, grad_pre).astype(jnp.bfloat16)
    grad_w_out = product("nu,uj->nj", mixed_t, grad_branch).astype(jnp.bfloat16)
    grad_w_out = turned(
        grad_w_out.reshape(heads_here, ctx, HEAD_DIM, width).transpose(1, 0, 2, 3), 0, (ctx - ctx_index) % ctx
    )
    grad_w_down = scatter_rows(grad_w_down)
    grad_up_out = scatter_rows(
        jnp.concatenate([grad_w_up, grad_w_out.reshape(width, width)], axis=1)
    )

    grad_parts, grad_whole = [], []
    for head in range(heads_here):
        if head == max(heads_here - 2, 0):
            grad_up_out, grad_w_down, table = lax.optimization_barrier(
                (grad_up_out, grad_w_down, table)
            )
            grad_up_out, grad_w_down = lax.psum((grad_up_out, grad_w_down), "ctx")
        results = attend_backward(table, head, packed_list, grads_by_head[head], *kept[head])
        grad_parts.append([shift(results[part], ctx, -part) for part in range(ctx)])
        grad_whole.append(results[ctx])
    normed_all = jnp.concatenate(normed_list, axis=0)
    grad_qkv_own = product("uj,nu->jn", normed_all, jnp.concatenate(grad_whole, axis=0))
    grad_qkv_own = scatter_pairs(grad_qkv_own, fsdp).astype(jnp.bfloat16)
    grad_qkv = [shift(grad_qkv_own, ctx, -part) for part in range(ctx)]
    grad_qkv = turned(jnp.stack(grad_qkv), 0, (ctx - ctx_index) % ctx)
    rows_here = grad_qkv.shape[1]
    grad_qkv = grad_qkv.reshape(ctx, rows_here, heads_here, 3, HEAD_DIM)
    grad_w_qkv = grad_qkv.transpose(1, 3, 0, 2, 4).reshape(rows_here, 3 * width).astype(jnp.float32)

    grad_normed_one = join_product([grad_parts[head][part] for part in range(ctx) for head in range(heads_here)], first)
    norm_one_back = jax.vjp(lambda v: layer_norm(v, gain_one), tokens_f)[1]
    grad_tokens = (grad_middle + norm_one_back(grad_normed_one)[0]).astype(jnp.bfloat16)

    grad_w_down = grad_w_down.astype(jnp.float32)
    grad_w_up = grad_up_out[:, : w_up.shape[1]].astype(jnp.float32)
    grad_w_out = grad_up_out[:, w_up.shape[1] :].astype(jnp.float32)

    def gain_grad(grad_weight, weight, gain):
        total = jnp.sum(grad_weight * weight.astype(jnp.float32), axis=1)
        return total / gain.astype(jnp.float32)

    return (
        result[None],
        grad_tokens[None],
        gain_grad(grad_w_qkv, w_qkv, gain_attn),
        gain_grad(grad_w_up, w_up, gain_mlp),
        grad_w_qkv,
        grad_w_out,
        grad_w_up,
        grad_w_down,
    )


def solution(mesh):
    rows = P("fsdp", None)
    whole = P("fsdp", "ctx", None)
    ctx, fsdp = mesh.shape["ctx"], mesh.shape["fsdp"]

    def layer(*arrays):
        return per_device(ctx, fsdp, *arrays)

    return jax.shard_map(
        layer,
        mesh=mesh,
        in_specs=(whole, whole, P("fsdp"), P("fsdp"), rows, rows, rows, rows, P("fsdp"), rows),
        out_specs=(whole, whole, P("fsdp"), P("fsdp"), rows, rows, rows, rows),
        check_vma=False,
    )
```
